32 devices in a mesh: gx: 4 (over y, x), gy: 8 (over z, core).
Axes of the slice: x: 2, y: 2, z: 4, core: 2. Of those that a mesh axis runs over, the one named last changes fastest.
Arguments:
- velocity: float32 [3, 128, 64, 128], P(None, 'gx', 'gy'), may hold values from -6 to 6
- stress: float32 [6, 128, 64, 128], P(None, 'gx', 'gy'), may hold values from -6 to 6
- lame_first: float32 [128, 64, 128], P('gx', 'gy'), may hold values from 0.5 to 2
- modulus: float32 [128, 64, 128], P('gx', 'gy'), may hold values from 0.5 to 2
- buoyancy: float32 [128, 64, 128], P('gx', 'gy'), may hold values from 0.5 to 2
- zone: int32 [128, 64, 128], P('gx', 'gy'), may hold values from 0 to 7
- eligible: int32 [128, 64, 128], P('gx', 'gy'), may hold values 0 or 1
- cohesion: float32 [8], replicated, may hold values from 0.2 to 2
- friction: float32 [8], replicated, may hold values from 0.1 to 0.6
- source_cell: int32 [16], replicated, may hold values from 0 to 1048575
- source_moment: float32 [6, 16], replicated, may hold values from -15 to 15
Outputs:
- velocity_out: float32 [3, 128, 64, 128], P(None, 'gx', 'gy')
- stress_out: float32 [6, 128, 64, 128], P(None, 'gx', 'gy')
The draws below stay inside these ranges and needn't reach their ends.
All inputs are finite; a program needn't handle non-finite values. No bound on the sum of `eligible` on one device may be relied on, other than what follows from the above.
Results may differ from the reference program's by a relative error of at most 0.00011.
Values sent between devices are 32-bit elements; how exact they have to be, the bound alone decides.
A program may use at most 64 MiB of HBM per device.

```python
import math
import jax
import jax.numpy as jnp
from jax import lax

NZ = 128
STEPS = 2
NZONES = 8
NSRC = 16
NX = 128
NY = 64


def with_ends(values, stream_key, low, largest):
    longest = values.shape.index(max(values.shape))
    spots = []
    for shift in (0, 1):
        where = [jax.random.randint(jax.random.fold_in(stream_key, axis), (), 0, length) for axis, length in enumerate(values.shape)]
        where[longest] = (where[longest] + shift) % values.shape[longest]
        spots.append(tuple(where))
    return values.at[spots[0]].set(low).at[spots[1]].set(largest)


def levels(stream_key, shape, cuts, smallest, high):
    def one(position, parts):
        steps = jax.random.uniform(jax.random.fold_in(jax.random.fold_in(stream_key, 6), position), (parts,), jnp.float32, smallest / len(cuts), high / len(cuts))
        return jnp.repeat(jnp.exp(steps), shape[position] // parts).reshape((-1,) + (1,) * (len(shape) - position - 1))

    level = one(*cuts[0])
    for cut in cuts[1:]:
        level = level * one(*cut)
    return level


def centred(key, extent, deviation, most, pieces=(), dtype=jnp.bfloat16):
    array = jax.random.normal(key, extent, jnp.float32) * deviation
    if len(pieces) > 0:
        array = levels(key, extent, pieces, -0.22, 0.18) * array
    return jnp.clip(array, min=-most, max=most).astype(dtype)


def setup_inputs(seed: int = 0) -> dict:
    seeds = jax.random.split(jax.random.key(seed), 12)
    return {
        "velocity": centred(seeds[0], (3, NX, NY, NZ), 1.0, 6.0, ((1, 4), (2, 8)), jnp.float32),
        "stress": centred(seeds[1], (6, NX, NY, NZ), 1.0, 6.0, ((1, 4), (2, 8)), jnp.float32),
        "lame_first": jnp.clip(jnp.exp(math.log(2.0) - 1.3862944 * jax.random.uniform(seeds[2], (NX, NY, NZ), jnp.float32) ** levels(seeds[2], (NX, NY, NZ), ((0, 4), (1, 8)), -0.2, 0.2)), 0.5, 2.0),
        "modulus": jnp.clip(jnp.exp(math.log(2.0) - 1.3862944 * jax.random.uniform(seeds[3], (NX, NY, NZ), jnp.float32) ** levels(seeds[3], (NX, NY, NZ), ((0, 4), (1, 8)), -0.2, 0.2)), 0.5, 2.0),
        "buoyancy": jnp.clip(jnp.exp(math.log(2.0) - 1.3862944 * jax.random.uniform(seeds[4], (NX, NY, NZ), jnp.float32) ** levels(seeds[4], (NX, NY, NZ), ((0, 4), (1, 8)), -0.2, 0.2)), 0.5, 2.0),
        "zone": with_ends(jax.random.randint(seeds[5], (NX, NY, NZ), 0, NZONES), jax.random.fold_in(seeds[5], 1), 0, NZONES - 1).astype(jnp.int32),
        "eligible": with_ends((jax.random.randint(seeds[6], (NX, NY, NZ), 0, 2) < 1).astype(jnp.int32), jax.random.fold_in(seeds[6], 1), 0, 1),
        "cohesion": jnp.clip(jnp.exp(jax.random.uniform(seeds[7], (NZONES,), jnp.float32, math.log(0.2), math.log(2.0))), 0.2, 2.0),
        "friction": jnp.clip(jax.random.uniform(seeds[8], (NZONES,), jnp.float32, 0.1, 0.6), 0.1, 0.6),
        "source_cell": with_ends(jax.random.randint(seeds[9], (NSRC,), 0, NX * NY * NZ), jax.random.fold_in(seeds[9], 1), 0, (NX * NY * NZ) - 1).astype(jnp.int32),
        "source_moment": centred(seeds[10], (6, NSRC), 3.0, 15.0, (), jnp.float32),
    }


time_step = 0.1
near_weight = 9.0 / 8.0
far_weight = 1.0 / 24.0
shear_floor = 0.25

def crop(padded, axis, offset):
    result = padded
    for dim in range(3):
        begin = offset if dim == axis else 2
        length = padded.shape[dim] - 4
        result = lax.slice_in_dim(result, begin, begin + length, axis=dim)
    return result

def derivative(padded, axis, forward):
    if forward:
        return near_weight * (crop(padded, axis, 3) - crop(padded, axis, 2)) - far_weight * (crop(padded, axis, 4) - crop(padded, axis, 1))
    return near_weight * (crop(padded, axis, 2) - crop(padded, axis, 1)) - far_weight * (crop(padded, axis, 3) - crop(padded, axis, 0))

def velocity_update(stress_pad, velocity, buoyancy):
    force_x = derivative(stress_pad[0], 0, True) + derivative(stress_pad[3], 1, False) + derivative(stress_pad[4], 2, False)
    force_y = derivative(stress_pad[3], 0, False) + derivative(stress_pad[1], 1, True) + derivative(stress_pad[5], 2, False)
    force_z = derivative(stress_pad[4], 0, False) + derivative(stress_pad[5], 1, False) + derivative(stress_pad[2], 2, True)
    forces = jnp.stack([force_x, force_y, force_z])
    return velocity + time_step * buoyancy[None] * forces

def stress_update(flow_pad, stress, lame_first, modulus):
    strain_x = derivative(flow_pad[0], 0, False)
    strain_y = derivative(flow_pad[1], 1, False)
    strain_z = derivative(flow_pad[2], 2, False)
    dilation = strain_x + strain_y + strain_z
    shear_xy = derivative(flow_pad[0], 1, True) + derivative(flow_pad[1], 0, True)
    shear_xz = derivative(flow_pad[0], 2, True) + derivative(flow_pad[2], 0, True)
    shear_yz = derivative(flow_pad[1], 2, True) + derivative(flow_pad[2], 1, True)
    rates = jnp.stack([lame_first * dilation + 2.0 * modulus * strain_x, lame_first * dilation + 2.0 * modulus * strain_y, lame_first * dilation + 2.0 * modulus * strain_z, modulus * shear_xy, modulus * shear_xz, modulus * shear_yz])
    return stress + time_step * rates

def plastic(stress, cell_cohesion, cell_friction, eligible):
    pressure = (stress[0] + stress[1] + stress[2]) / 3.0
    dev_x = stress[0] - pressure
    dev_y = stress[1] - pressure
    dev_z = stress[2] - pressure
    second = 0.5 * (dev_x * dev_x + dev_y * dev_y + dev_z * dev_z) + stress[3] * stress[3] + stress[4] * stress[4] + stress[5] * stress[5]
    strength = jnp.maximum(cell_cohesion * jnp.sqrt(1.0 - cell_friction * cell_friction) - pressure * cell_friction, 0.0)
    ratio = jnp.minimum(1.0, strength / jnp.maximum(jnp.sqrt(second), shear_floor))
    factor = jnp.where(eligible == 1, ratio, 1.0)
    return jnp.stack([pressure + factor * dev_x, pressure + factor * dev_y, pressure + factor * dev_z, factor * stress[3], factor * stress[4], factor * stress[5]])

def pad_space(field, width):
    return jnp.pad(field, ((0, 0), (width, width), (width, width), (width, width)))

def reference(velocity, stress, lame_first, modulus, buoyancy, zone, eligible, cohesion, friction, source_cell, source_moment):
    cell_cohesion = cohesion[zone]
    cell_friction = friction[zone]
    plane = NY * NZ
    src_x = (source_cell // plane).astype(jnp.int32)
    src_y = (source_cell // NZ % NY).astype(jnp.int32)
    src_z = (source_cell % NZ).astype(jnp.int32)
    injection = jnp.zeros_like(stress).at[:, src_x, src_y, src_z].add(time_step * source_moment)
    for step in range(STEPS):
        velocity = velocity_update(pad_space(stress, 2), velocity, buoyancy)
        stress = stress_update(pad_space(velocity, 2), stress, lame_first, modulus)
        stress = stress + injection
        stress = plastic(stress, cell_cohesion, cell_friction, eligible)
    return (velocity, stress)
```

```python
import functools

import jax
import jax.numpy as jnp
from jax import lax
from jax.experimental import pallas as pl
from jax.experimental.pallas import tpu as pltpu
from jax.sharding import PartitionSpec as P

STEPS = 2
time_step = 0.1
shear_floor = 0.25
MESH = pl.DeviceIdType.MESH
CH = 8
R = 16

BACK = {"F": 1, "B": 2}
AHEAD = {"F": 2, "B": 1}
FORCE_X = ((0, "F"), (3, "B"), (4, "B"))
FORCE_Y = ((3, "B"), (1, "F"), (5, "B"))
FLOW_X = ("B", "F", "F")
FLOW_Y = ("F", "B", "F")
SLOT_X = {0: 0, 3: 1, 4: 2}
SLOT_Y = {3: 0, 1: 1, 5: 2}


def edge(kind, up, n):
    return list(range(n - BACK[kind], n)) if up else list(range(AHEAD[kind]))


def spread(kind, up, n, get):
    if up and kind == "B":
        return [(0, get(0) - 27.0 * get(1)), (1, get(1))]
    if up:
        return [(0, get(0))]
    if kind == "B":
        return [(n - 1, -get(0))]
    return [(n - 1, 27.0 * get(0) - get(1)), (n - 2, -get(0))]


def raw_list(force, up, n):
    return [(comp, i) for comp, kind in force for i in edge(kind, up, n)]


def flow_list(flow, up, n):
    return [(slot, i) for slot, kind in enumerate(flow) for i in edge(kind, up, n)]


def corner_list(sx, sy, nx, ny):
    found = []
    for k in range(3):
        comp, kind = FORCE_Y[k]
        found += [(comp, x, y) for x in edge(FLOW_X[k], sx, nx) for y in edge(kind, sy, ny)]
        comp, kind = FORCE_X[k]
        found += [(comp, x, y) for x in edge(kind, sx, nx) for y in edge(FLOW_Y[k], sy, ny)]
    return list(dict.fromkeys(found))


CORNERS = [(True, True), (True, False), (False, True), (False, False)]


def kernel(
    nx,
    ny,
    vel_hbm, str_hbm, lam_hbm, mod_hbm, buo_hbm, zone_hbm, elig_hbm,
    coh_ref, fri_ref, cell_ref, moment_ref,
    vout_ref, sout_ref,
    stage, vel, lam, mod, buo, zone, elig, inj, cc, cf,
    sx, sy, zb, vb, xs, rx, ys, ry, ds, rd, xf, yf,
    load_sem, xsend, xrecv, ysend, yrecv, dsend, drecv,
):
    rows_x = lam.shape[0]
    rows_y = lam.shape[1]
    depth = lam.shape[2]
    chunks = rows_x // CH
    ix = lax.axis_index("gx")
    iy = lax.axis_index("gy")
    x_lo, x_hi, y_lo, y_hi = ix > 0, ix < nx - 1, iy > 0, iy < ny - 1

    def to_x(up):
        return (x_hi, (ix + 1, iy)) if up else (x_lo, (ix - 1, iy))

    def to_y(up):
        return (y_hi, (ix, iy + 1)) if up else (y_lo, (ix, iy - 1))

    def to_corner(cx, cy):
        there = jnp.logical_and(to_x(cx)[0], to_y(cy)[0])
        return there, (to_x(cx)[1][0], to_y(cy)[1][1])

    sides = [to_x(True), to_x(False), to_y(True), to_y(False)] + [to_corner(*c) for c in CORNERS]
    barrier = pltpu.get_barrier_semaphore()
    for there, target in sides:

        @pl.when(there)
        def _():
            pl.semaphore_signal(barrier, inc=1, device_id=target, device_id_type=MESH)

    raw_x = {up: raw_list(FORCE_X, up, rows_x) for up in (True, False)}
    raw_y = {up: raw_list(FORCE_Y, up, rows_y) for up in (True, False)}
    flow_x = {up: flow_list(FLOW_X, up, rows_x) for up in (True, False)}
    flow_y = {up: flow_list(FLOW_Y, up, rows_y) for up in (True, False)}
    buo_x = {True: [rows_x - 2, rows_x - 1], False: [0, 1]}
    buo_y = {True: [rows_y - 2, rows_y - 1], False: [0, 1]}
    corner = {c: corner_list(c[0], c[1], rows_x, rows_y) for c in CORNERS}

    loads = []

    def load(src, dst):
        copy = pltpu.make_async_copy(src, dst, load_sem.at[len(loads)])
        copy.start()
        loads.append(copy)

    def sx_row(step, comp, x):
        return ((step * 3 + SLOT_X[comp]) * (rows_x + 4) + x + 2) * rows_y

    def sy_row(step, comp, x):
        return (step * 3 + SLOT_Y[comp]) * R * (rows_x + 1) + R * (x + 1)

    def vb_row(step, slot, x):
        return ((step * 3 + slot) * (rows_x + 5) + x + 3) * R

    plane = rows_x * rows_y
    load(str_hbm.at[pl.ds(3 * plane, plane)], sx.at[pl.ds(sx_row(0, 3, 0), plane)])
    load(str_hbm.at[pl.ds(1 * plane, plane)], stage.at[0])
    load(str_hbm.at[pl.ds(5 * plane, plane)], stage.at[1])
    load(buo_hbm, buo)
    load(str_hbm.at[pl.ds(0 * plane, plane)], sx.at[pl.ds(sx_row(0, 0, 0), plane)])
    load(str_hbm.at[pl.ds(4 * plane, plane)], sx.at[pl.ds(sx_row(0, 4, 0), plane)])
    first = len(loads)
    load(str_hbm.at[pl.ds(2 * plane, plane)], zb.at[pl.ds(0, plane)])
    load(vel_hbm, vel)
    second = len(loads)
    load(zone_hbm, zone)
    load(elig_hbm, elig)
    third = len(loads)
    load(lam_hbm, lam)
    load(mod_hbm, mod)

    tile = jnp.zeros((rows_y, depth), jnp.float32)

    for step in range(STEPS):
        for comp in SLOT_X:
            for layer in (-2, -1, rows_x, rows_x + 1):
                sx[pl.ds(sx_row(step, comp, layer), rows_y), :] = tile
    for ref in (xf, yf):
        for i in range(ref.shape[0] // rows_y):
            ref[pl.ds(i * rows_y, rows_y), :] = tile

    def clear(i, carry):
        sy[pl.ds(pl.multiple_of(i * R + rows_y, 8), R - rows_y), :] = jnp.zeros((R - rows_y, depth), jnp.float32)
        return carry

    lax.fori_loop(0, sy.shape[0] // R, clear, 0, unroll=8)

    for up in (True, False):

        @pl.when(jnp.logical_not(to_x(not up)[0]))
        def _():
            for step in range(STEPS):
                for i in range(rx.shape[2]):
                    rx[step, int(up), i] = tile

        @pl.when(jnp.logical_not(to_y(not up)[0]))
        def _():
            for step in range(STEPS):

                def wipe(c, carry):
                    for i in range(ry.shape[3] // 8):
                        ry[step, int(up), c, pl.ds(i * 8, 8), :] = tile
                    return carry

                lax.fori_loop(0, chunks, wipe, 0)

    for d, (cx, cy) in enumerate(CORNERS):

        @pl.when(jnp.logical_not(to_corner(not cx, not cy)[0]))
        def _():
            for step in range(STEPS):
                for i in range(rd.shape[2] // 8):
                    rd[step, d, pl.ds(i * 8, 8), :] = tile

    def n_raw(raw, step):
        return len(raw) + (2 if step == 0 else 0)

    def x_copy(step, up, part):
        start, count = (0, n_raw(raw_x[up], step)) if part == 0 else (len(raw_x[up]) + 2, len(flow_x[up]))
        return pltpu.make_async_remote_copy(
            src_ref=xs.at[step, int(up), pl.ds(start, count)],
            dst_ref=rx.at[step, int(up), pl.ds(start, count)],
            send_sem=xsend.at[step, int(up), part],
            recv_sem=xrecv.at[step, int(up), part],
            device_id=to_x(up)[1],
            device_id_type=MESH,
        )

    def y_copy(step, up, c, part):
        start, count = (0, n_raw(raw_y[up], step)) if part == 0 else (len(raw_y[up]) + 2, len(flow_y[up]))
        return pltpu.make_async_remote_copy(
            src_ref=ys.at[step, int(up), c, pl.ds(start * 8, count * 8)],
            dst_ref=ry.at[step, int(up), c, pl.ds(start * 8, count * 8)],
            send_sem=ysend.at[step, int(up), c, part],
            recv_sem=yrecv.at[step, int(up), c, part],
            device_id=to_y(up)[1],
            device_id_type=MESH,
        )

    def d_copy(step, d):
        return pltpu.make_async_remote_copy(
            src_ref=ds.at[step, d],
            dst_ref=rd.at[step, d],
            send_sem=dsend.at[step, d],
            recv_sem=drecv.at[step, d],
            device_id=to_corner(*CORNERS[d])[1],
            device_id_type=MESH,
        )

    def sx_tile(step, comp, x):
        return sx[pl.ds(sx_row(step, comp, x), rows_y), :]

    def sy_pack(step, comp, c, row):
        return sy[pl.ds(sy_row(step, comp, c * CH) + row, CH, stride=R), :]

    def vb_pack(step, slot, c, row):
        return pl.ds(vb_row(step, slot, c * CH) + row, CH, stride=R)

    def pack_x_raw(step, up):
        for i, (comp, x) in enumerate(raw_x[up]):
            xs[step, int(up), i] = sx_tile(step, comp, x)
        if step == 0:
            for i, x in enumerate(buo_x[up]):
                xs[step, int(up), len(raw_x[up]) + i] = buo[pl.ds(x * rows_y, rows_y), :]

    def pack_y_raw(step, c):
        for up in (True, False):
            for i, (comp, row) in enumerate(raw_y[up]):
                ys[step, int(up), c, pl.ds(i * 8, 8), :] = sy_pack(step, comp, c, row)
            if step == 0:
                for i, row in enumerate(buo_y[up]):
                    value = buo[pl.ds(c * CH * rows_y + row, CH, stride=rows_y), :]
                    ys[step, int(up), c, pl.ds((len(raw_y[up]) + i) * 8, 8), :] = value

    def pack_x_flow(step, up):
        for i, (slot, x) in enumerate(flow_x[up]):
            xs[step, int(up), len(raw_x[up]) + 2 + i] = vb[pl.ds(vb_row(step, slot, x), rows_y), :]

    def pack_y_flow(step, c):
        for up in (True, False):
            for i, (slot, row) in enumerate(flow_y[up]):
                ys[step, int(up), c, pl.ds((len(raw_y[up]) + 2 + i) * 8, 8), :] = vb[vb_pack(step, slot, c, row), :]

    def pack_corners(step, cxs):
        for d, (cx, cy) in enumerate(CORNERS):
            if cx in cxs:
                for i, (comp, x, y) in enumerate(corner[(cx, cy)]):
                    if comp in SLOT_X:
                        value = sx[pl.ds(sx_row(step, comp, x) + y, 1), :]
                    else:
                        value = sy[pl.ds(sy_row(step, comp, x) + y, 1), :]
                    ds[step, d, pl.ds(i, 1), :] = value

    def send_x(step, up, parts):
        @pl.when(to_x(up)[0])
        def _():
            for part in parts:
                x_copy(step, up, part).start()

    def send_y(step, cs, parts):
        for up in (True, False):

            @pl.when(to_y(up)[0])
            def _():
                for c in cs:
                    for part in parts:
                        y_copy(step, up, c, part).start()

    def send_corners(step, cxs):
        for d, (cx, cy) in enumerate(CORNERS):
            if cx in cxs:

                @pl.when(to_corner(cx, cy)[0])
                def _():
                    d_copy(step, d).start()

    lane = lax.broadcasted_iota(jnp.int32, (rows_y, depth), 1)
    keep = {
        1: lane < depth - 1,
        2: lane < depth - 2,
        -1: lane >= 1,
        -2: lane >= 2,
    }

    def along_z(value, offset):
        if offset == 0:
            return value
        return jnp.where(keep[offset], pltpu.roll(value, (-offset) % depth, 1), 0.0)

    def derivative(get, forward):
        a, b, c, d = (get(1), get(0), get(2), get(-1)) if forward else (get(0), get(-1), get(1), get(-2))
        return 27.0 * (a - b) - (c - d)

    def s_dx(step, comp, x, forward):
        return derivative(lambda o: sx_tile(step, comp, x + o), forward)

    def s_dy(step, comp, x, forward):
        return derivative(lambda o: sy[pl.ds(sy_row(step, comp, x) + o, rows_y), :], forward)

    def v_dx(step, slot, x, forward):
        return derivative(lambda o: vb[pl.ds(vb_row(step, slot, x + o), rows_y), :], forward)

    def v_dy(step, slot, x, forward):
        return derivative(lambda o: vb[pl.ds(vb_row(step, slot, x) + o, rows_y), :], forward)

    def dz(value, forward):
        return derivative(lambda o: along_z(value, o), forward)

    def own_sy(step, comp, x):
        return sy[pl.ds(sy_row(step, comp, x), rows_y), :]

    def own_zb(step, x):
        return zb[pl.ds((step * rows_x + x) * rows_y, rows_y), :]

    def own_v(step, slot, x):
        return vb[pl.ds(vb_row(step, slot, x), rows_y), :]

    def of_cell(ref, x):
        return ref[pl.ds(x * rows_y, rows_y), :]

    weight = time_step / 24.0

    def flow_layer(step, x):
        scale = weight * of_cell(buo, x)
        xz = sx_tile(step, 4, x)
        yz = own_sy(step, 5, x)
        zz = own_zb(step, x)
        force_x = s_dx(step, 0, x, True) + s_dy(step, 3, x, False) + dz(xz, False)
        force_y = s_dx(step, 3, x, False) + s_dy(step, 1, x, True) + dz(yz, False)
        force_z = s_dx(step, 4, x, False) + s_dy(step, 5, x, False) + dz(zz, True)
        for slot, force in enumerate((force_x, force_y, force_z)):
            old = vel[pl.ds((slot * rows_x + x) * rows_y, rows_y), :] if step == 0 else own_v(step - 1, slot, x)
            vb[pl.ds(vb_row(step, slot, x), rows_y), :] = old + scale * force

    def wait_x(step):
        for up in (True, False):

            @pl.when(to_x(not up)[0])
            def _():
                for part in (0, 1):
                    x_copy(step, up, part).wait_recv()

    def wait_y(step):
        for up in (True, False):

            @pl.when(to_y(not up)[0])
            def _():
                for c in range(chunks):
                    for part in (0, 1):
                        y_copy(step, up, c, part).wait_recv()

    def wait_corners(step):
        for d, (cx, cy) in enumerate(CORNERS):

            @pl.when(to_corner(not cx, not cy)[0])
            def _():
                d_copy(step, d).wait_recv()

    def place(items, what):
        return [i for i, item in enumerate(items) if item == what][0]

    def take_corners(step):
        for d, (cx, cy) in enumerate(CORNERS):

            def raw(comp, x, y):
                return rd[step, d, pl.ds(place(corner[(cx, cy)], (comp, x, y)), 1), :]

            for k in range(3):
                comp, kind = FORCE_Y[k]
                ys_ = edge(kind, cy, rows_y)
                for x in edge(FLOW_X[k], cx, rows_x):
                    base = (int(cx) * 5 + place(flow_x[cx], (k, x))) * rows_y
                    for row, value in spread(kind, cy, rows_y, lambda i: raw(comp, x, ys_[i])):
                        xf[pl.ds(base + row, 1), :] = value
                comp, kind = FORCE_X[k]
                xs_ = edge(kind, cx, rows_x)
                for y in edge(FLOW_Y[k], cy, rows_y):
                    base = ((int(cy) * 5 + place(flow_y[cy], (k, y))) * 2 + int(cx)) * 8
                    for layer, value in spread(kind, cx, CH, lambda i: raw(comp, xs_[i], y)):
                        yf[pl.ds(base + layer, 1), :] = value

    def finish_x(step):
        for up in (True, False):
            side = int(up)
            for k, (comp, kind) in enumerate(FORCE_X):
                places = [place(raw_x[up], (comp, x)) for x in edge(kind, up, rows_x)]
                for x, value in spread(kind, up, rows_x, lambda i: rx[step, side, places[i]]):
                    where = pl.ds(vb_row(step, k, x), rows_y)
                    vb[where, :] = vb[where, :] + weight * of_cell(buo, x) * value
            for k, (comp, kind) in enumerate(FORCE_X):
                mine = edge(kind, not up, rows_x)
                adds = dict(spread(kind, not up, rows_x, lambda i: sx_tile(step, comp, mine[i])))
                for x in edge(FLOW_X[k], up, rows_x):
                    i = place(flow_x[up], (k, x))
                    add = adds[x] + xf[pl.ds((side * 5 + i) * rows_y, rows_y), :]
                    scale = weight * rx[0, side, len(raw_x[up]) + place(buo_x[up], x)]
                    new = rx[step, side, len(raw_x[up]) + 2 + i] + scale * add
                    at = x - rows_x if up else x + rows_x
                    vb[pl.ds(vb_row(step, k, at), rows_y), :] = new

    def finish_y(step, c):
        for up in (True, False):
            side = int(up)

            def got(i):
                return ry[step, side, c, pl.ds(i * 8, 8), :]

            for k, (comp, kind) in enumerate(FORCE_Y):
                places = [place(raw_y[up], (comp, y)) for y in edge(kind, up, rows_y)]
                for y, value in spread(kind, up, rows_y, lambda i: got(places[i])):
                    where = vb_pack(step, k, c, y)
                    scale = weight * buo[pl.ds(c * CH * rows_y + y, CH, stride=rows_y), :]
                    vb[where, :] = vb[where, :] + scale * value
            for k, (comp, kind) in enumerate(FORCE_Y):
                mine = edge(kind, not up, rows_y)
                adds = dict(spread(kind, not up, rows_y, lambda i: sy_pack(step, comp, c, mine[i])))
                for y in edge(FLOW_Y[k], up, rows_y):
                    i = place(flow_y[up], (k, y))
                    add = adds[y]
                    for end, at_end in ((1, 0), (0, chunks - 1)):
                        if c == at_end:
                            add = add + yf[pl.ds(((side * 5 + i) * 2 + end) * 8, 8), :]
                    scale = weight * ry[0, side, c, pl.ds((len(raw_y[up]) + place(buo_y[up], y)) * 8, 8), :]
                    new = got(len(raw_y[up]) + 2 + i) + scale * add
                    at = y - rows_y if up else y + rows_y
                    vb[vb_pack(step, k, c, at), :] = new

    def stress_layer(step, x):
        last = step == STEPS - 1
        vx, vy, vz = (own_v(step, slot, x) for slot in range(3))
        if last:
            for slot, value in enumerate((vx, vy, vz)):
                vout_ref[slot, x] = value
        ex = v_dx(step, 0, x, False)
        ey = v_dy(step, 1, x, False)
        ez = dz(vz, False)
        xy = v_dy(step, 0, x, True) + v_dx(step, 1, x, True)
        xz = dz(vx, True) + v_dx(step, 2, x, True)
        yz = dz(vy, True) + v_dy(step, 2, x, True)
        m = weight * mod[x]
        grow = weight * lam[x] * (ex + ey + ez)
        m2 = m + m
        s0, s3, s4 = (sx_tile(step, comp, x) for comp in (0, 3, 4))
        s1, s5 = own_sy(step, 1, x), own_sy(step, 5, x)
        s2 = own_zb(step, x)
        s0 = s0 + (grow + m2 * ex) + inj[0, x]
        s1 = s1 + (grow + m2 * ey) + inj[1, x]
        s2 = s2 + (grow + m2 * ez) + inj[2, x]
        s3 = s3 + m * xy + inj[3, x]
        s4 = s4 + m * xz + inj[4, x]
        s5 = s5 + m * yz + inj[5, x]
        pressure = (s0 + s1 + s2) * (1.0 / 3.0)
        d0, d1, d2 = s0 - pressure, s1 - pressure, s2 - pressure
        second = 0.5 * (d0 * d0 + d1 * d1 + d2 * d2) + (s3 * s3 + s4 * s4 + s5 * s5)
        strength = jnp.maximum(cc[x] - pressure * cf[x], 0.0)
        factor = jnp.minimum(1.0, strength * lax.rsqrt(jnp.maximum(second, shear_floor * shear_floor)))
        s0, s1, s2 = pressure + factor * d0, pressure + factor * d1, pressure + factor * d2
        s3, s4, s5 = factor * s3, factor * s4, factor * s5
        if last:
            for comp, value in enumerate((s0, s1, s2, s3, s4, s5)):
                sout_ref[comp, x] = value
            return
        for comp, value in ((0, s0), (3, s3), (4, s4)):
            sx[pl.ds(sx_row(step + 1, comp, x), rows_y), :] = value
        for comp, value in ((3, s3), (1, s1), (5, s5)):
            sy[pl.ds(sy_row(step + 1, comp, x), rows_y), :] = value
        zb[pl.ds(((step + 1) * rows_x + x) * rows_y, rows_y), :] = s2

    for copy in loads[:first]:
        copy.wait()

    def fill_y(i, carry):
        at = pl.multiple_of(i * rows_y, 8)
        for comp, value in (
            (3, sx[pl.ds(sx_row(0, 3, 0) + at, rows_y), :]),
            (1, stage[0, pl.ds(at, rows_y), :]),
            (5, stage[1, pl.ds(at, rows_y), :]),
        ):
            sy[pl.ds(pl.multiple_of(sy_row(0, comp, 0) + i * R, 8), rows_y), :] = value
        return carry

    lax.fori_loop(0, rows_x, fill_y, 0, unroll=8)
    for up in (True, False):
        pack_x_raw(0, up)
    pack_corners(0, (True, False))
    for c in range(chunks):
        pack_y_raw(0, c)
    heard = sum(there.astype(jnp.int32) for there, _ in sides)
    pl.semaphore_wait(barrier, heard)
    for up in (True, False):
        send_x(0, up, (0,))
    send_corners(0, (True, False))
    send_y(0, range(chunks), (0,))
    for copy in loads[first:second]:
        copy.wait()
    order = [0] + ([chunks - 1] if chunks > 1 else []) + list(range(1, chunks - 1))
    for c in order:
        for i in range(CH):
            flow_layer(0, c * CH + i)
        if c == 0:
            pack_x_flow(0, False)
            send_x(0, False, (1,))
        if c == chunks - 1:
            pack_x_flow(0, True)
            send_x(0, True, (1,))
        pack_y_flow(0, c)
        send_y(0, (c,), (1,))

    cell = cell_ref[...]
    bits = depth.bit_length() - 1
    assert depth == 1 << bits
    plane_row = cell >> bits
    cell_z = cell & (depth - 1)
    row = lax.broadcasted_iota(jnp.int32, (rows_x * rows_y, cell.shape[1]), 0)
    row_bits = rows_y.bit_length() - 1
    assert rows_y == 1 << row_bits
    row = (ix * rows_x + (row >> row_bits)) * (ny * rows_y) + iy * rows_y + (row & (rows_y - 1))
    match = row == plane_row
    at_z = (lax.broadcasted_iota(jnp.int32, (depth, cell.shape[1]), 0) == cell_z).astype(jnp.float32)
    for comp in range(6):
        moment = time_step * moment_ref[pl.ds(comp, 1), :]
        value = lax.dot_general(
            jnp.where(match, moment, 0.0),
            at_z,
            (((1,), (1,)), ((), ())),
            precision=lax.Precision.HIGHEST,
            preferred_element_type=jnp.float32,
        )
        inj[comp] = value.reshape(rows_x, rows_y, depth)

    for copy in loads[second:third]:
        copy.wait()
    frictions, cohesions = [], []
    for which in range(coh_ref.shape[0]):
        f = jnp.full((rows_y, depth), fri_ref[which], jnp.float32)
        frictions.append(f)
        cohesions.append(coh_ref[which] * jnp.sqrt(1.0 - f * f))

    def table(x, carry):
        z = jnp.where(elig[x] == 1, zone[x], -1)
        c = jnp.full((rows_y, depth), 1e30, jnp.float32)
        f = jnp.zeros((rows_y, depth), jnp.float32)
        for which in range(coh_ref.shape[0]):
            hit = z == which
            c = jnp.where(hit, cohesions[which], c)
            f = jnp.where(hit, frictions[which], f)
        cc[x] = c
        cf[x] = f
        return carry

    lax.fori_loop(0, rows_x, table, 0, unroll=2)

    for copy in loads[third:]:
        copy.wait()

    for step in range(STEPS):
        wait_corners(step)
        take_corners(step)
        wait_x(step)
        finish_x(step)
        wait_y(step)
        for c in range(chunks):
            finish_y(step, c)
        last = step == STEPS - 1
        done = 0
        stressed = set()
        flowed = set()
        sent = set()
        for c in order:
            for i in range(CH):
                stress_layer(step, c * CH + i)
            if last:
                continue
            nxt = step + 1
            stressed.update(range(c * CH, (c + 1) * CH))
            pack_y_raw(nxt, c)
            send_y(nxt, (c,), (0,))
            if c == 0:
                pack_corners(nxt, (False,))
                send_corners(nxt, (False,))
                pack_x_raw(nxt, False)
            if c == chunks - 1:
                pack_corners(nxt, (True,))
                send_corners(nxt, (True,))
                pack_x_raw(nxt, True)
            for x in range(rows_x):
                near = range(max(x - 2, 0), min(x + 3, rows_x))
                if x not in flowed and all(n in stressed for n in near):
                    flow_layer(nxt, x)
                    flowed.add(x)
            if c == 0:
                pack_x_flow(nxt, False)
                send_x(nxt, False, (0, 1))
            if c == chunks - 1:
                pack_x_flow(nxt, True)
                send_x(nxt, True, (0, 1))
            for other in order:
                if other not in sent and all(x in flowed for x in range(other * CH, (other + 1) * CH)):
                    pack_y_flow(nxt, other)
                    send_y(nxt, (other,), (1,))
                    sent.add(other)

    for step in range(STEPS):
        for up in (True, False):

            @pl.when(to_x(up)[0])
            def _():
                for part in (0, 1):
                    x_copy(step, up, part).wait_send()

            @pl.when(to_y(up)[0])
            def _():
                for c in range(chunks):
                    for part in (0, 1):
                        y_copy(step, up, c, part).wait_send()

        for d, (cx, cy) in enumerate(CORNERS):

            @pl.when(to_corner(cx, cy)[0])
            def _():
                d_copy(step, d).wait_send()


def on_device(nx, ny, velocity, stress, lame_first, modulus, buoyancy, zone, eligible, cohesion, friction, source_cell, source_moment):
    rows_x, rows_y, depth = zone.shape
    assert rows_y == 8 and rows_x % CH == 0
    chunks = rows_x // CH
    f32 = jnp.float32
    grid = (rows_x, rows_y, depth)
    plane = rows_x * rows_y
    any_spec = pl.BlockSpec(memory_space=pltpu.HBM)
    smem = pl.BlockSpec(memory_space=pltpu.SMEM)
    vmem = pl.BlockSpec(memory_space=pltpu.VMEM)
    dma = pltpu.SemaphoreType.DMA
    return pl.pallas_call(
        functools.partial(kernel, nx, ny),
        out_shape=(pltpu.VMEM((3,) + grid, f32), pltpu.VMEM((6,) + grid, f32)),
        in_specs=[any_spec] * 7 + [smem, smem, vmem, vmem],
        out_specs=(vmem, vmem),
        scratch_shapes=[
            pltpu.VMEM((2, plane, depth), f32),
            pltpu.VMEM((3 * plane, depth), f32),
            pltpu.VMEM(grid, f32),
            pltpu.VMEM(grid, f32),
            pltpu.VMEM((plane, depth), f32),
            pltpu.VMEM(grid, jnp.int32),
            pltpu.VMEM(grid, jnp.int32),
            pltpu.VMEM((6,) + grid, f32),
            pltpu.VMEM(grid, f32),
            pltpu.VMEM(grid, f32),
            pltpu.VMEM((STEPS * 3 * (rows_x + 4) * rows_y, depth), f32),
            pltpu.VMEM((STEPS * 3 * R * (rows_x + 1) + R, depth), f32),
            pltpu.VMEM((STEPS * plane, depth), f32),
            pltpu.VMEM((STEPS * 3 * (rows_x + 5) * R, depth), f32),
            pltpu.VMEM((STEPS, 2, 11, rows_y, depth), f32),
            pltpu.VMEM((STEPS, 2, 11, rows_y, depth), f32),
            pltpu.VMEM((STEPS, 2, chunks, 11 * 8, depth), f32),
            pltpu.VMEM((STEPS, 2, chunks, 11 * 8, depth), f32),
            pltpu.VMEM((STEPS, 4, 16, depth), f32),
            pltpu.VMEM((STEPS, 4, 16, depth), f32),
            pltpu.VMEM((2 * 5 * rows_y, depth), f32),
            pltpu.VMEM((2 * 5 * 2 * 8, depth), f32),
            dma((12,)),
            dma((STEPS, 2, 2)),
            dma((STEPS, 2, 2)),
            dma((STEPS, 2, chunks, 2)),
            dma((STEPS, 2, chunks, 2)),
            dma((STEPS, 4)),
            dma((STEPS, 4)),
        ],
        compiler_params=pltpu.CompilerParams(collective_id=0, has_side_effects=True),
    )(
        velocity.reshape(3 * plane, depth), stress.reshape(6 * plane, depth), lame_first, modulus,
        buoyancy.reshape(plane, depth), zone, eligible,
        cohesion, friction, source_cell.reshape(1, -1), source_moment,
    )


def solution(mesh):
    field = P(None, "gx", "gy", None)
    cells = P("gx", "gy", None)
    return jax.shard_map(
        functools.partial(on_device, mesh.shape["gx"], mesh.shape["gy"]),
        mesh=mesh,
        in_specs=(field, field, cells, cells, cells, cells, cells, P(), P(), P(), P()),
        out_specs=(field, field),
        check_vma=False,
    )
```

```python
import functools

import jax
import jax.numpy as jnp
from jax import lax
from jax.experimental import pallas as pl
from jax.experimental.pallas import tpu as pltpu
from jax.sharding import PartitionSpec as P

STEPS = 2
time_step = 0.1
shear_floor = 0.25
MESH = pl.DeviceIdType.MESH
CH = 8
R = 16

BACK = {"F": 1, "B": 2}
AHEAD = {"F": 2, "B": 1}
FORCE_X = ((0, "F"), (3, "B"), (4, "B"))
FORCE_Y = ((3, "B"), (1, "F"), (5, "B"))
FLOW_X = ("B", "F", "F")
FLOW_Y = ("F", "B", "F")
SLOT_X = {0: 0, 3: 1, 4: 2}
SLOT_Y = {3: 0, 1: 1, 5: 2}


def edge(kind, up, n):
    return list(range(n - BACK[kind], n)) if up else list(range(AHEAD[kind]))


def spread(kind, up, n, get):
    if up and kind == "B":
        return [(0, get(0) - 27.0 * get(1)), (1, get(1))]
    if up:
        return [(0, get(0))]
    if kind == "B":
        return [(n - 1, -get(0))]
    return [(n - 1, 27.0 * get(0) - get(1)), (n - 2, -get(0))]


def raw_list(force, up, n):
    return [(comp, i) for comp, kind in force for i in edge(kind, up, n)]


def flow_list(flow, up, n):
    return [(slot, i) for slot, kind in enumerate(flow) for i in edge(kind, up, n)]


def corner_list(sx, sy, nx, ny):
    found = []
    for k in range(3):
        comp, kind = FORCE_Y[k]
        found += [(comp, x, y) for x in edge(FLOW_X[k], sx, nx) for y in edge(kind, sy, ny)]
        comp, kind = FORCE_X[k]
        found += [(comp, x, y) for x in edge(kind, sx, nx) for y in edge(FLOW_Y[k], sy, ny)]
    return list(dict.fromkeys(found))


CORNERS = [(True, True), (True, False), (False, True), (False, False)]


def kernel(
    nx,
    ny,
    vel_hbm, str_hbm, lam_hbm, mod_hbm, buo_hbm, zone_hbm, elig_hbm,
    coh_ref, fri_ref, cell_ref, moment_ref,
    vout_ref, sout_ref,
    stage, vel, lam, mod, buo, zone, elig, inj, cc, cf,
    sx, sy, zb, vb, xs, rx, ys, ry, ds, rd, xf, yf,
    load_sem, xsend, xrecv, ysend, yrecv, dsend, drecv,
):
    rows_x = lam.shape[0]
    rows_y = lam.shape[1]
    depth = lam.shape[2]
    chunks = rows_x // CH
    ix = lax.axis_index("gx")
    iy = lax.axis_index("gy")
    x_lo, x_hi, y_lo, y_hi = ix > 0, ix < nx - 1, iy > 0, iy < ny - 1

    def to_x(up):
        return (x_hi, (ix + 1, iy)) if up else (x_lo, (ix - 1, iy))

    def to_y(up):
        return (y_hi, (ix, iy + 1)) if up else (y_lo, (ix, iy - 1))

    def to_corner(cx, cy):
        there = jnp.logical_and(to_x(cx)[0], to_y(cy)[0])
        return there, (to_x(cx)[1][0], to_y(cy)[1][1])

    sides = [to_x(True), to_x(False), to_y(True), to_y(False)] + [to_corner(*c) for c in CORNERS]
    barrier = pltpu.get_barrier_semaphore()
    for there, target in sides:

        @pl.when(there)
        def _():
            pl.semaphore_signal(barrier, inc=1, device_id=target, device_id_type=MESH)

    raw_x = {up: raw_list(FORCE_X, up, rows_x) for up in (True, False)}
    raw_y = {up: raw_list(FORCE_Y, up, rows_y) for up in (True, False)}
    flow_x = {up: flow_list(FLOW_X, up, rows_x) for up in (True, False)}
    flow_y = {up: flow_list(FLOW_Y, up, rows_y) for up in (True, False)}
    buo_x = {True: [rows_x - 2, rows_x - 1], False: [0, 1]}
    buo_y = {True: [rows_y - 2, rows_y - 1], False: [0, 1]}
    corner = {c: corner_list(c[0], c[1], rows_x, rows_y) for c in CORNERS}

    loads = []

    def load(src, dst):
        copy = pltpu.make_async_copy(src, dst, load_sem.at[len(loads)])
        copy.start()
        loads.append(copy)

    def sx_row(step, comp, x):
        return ((step * 3 + SLOT_X[comp]) * (rows_x + 4) + x + 2) * rows_y

    def sy_row(step, comp, x):
        return (step * 3 + SLOT_Y[comp]) * R * (rows_x + 1) + R * (x + 1)

    def vb_row(step, slot, x):
        return ((step * 3 + slot) * (rows_x + 5) + x + 3) * R

    plane = rows_x * rows_y
    load(str_hbm.at[pl.ds(3 * plane, plane)], sx.at[pl.ds(sx_row(0, 3, 0), plane)])
    load(str_hbm.at[pl.ds(1 * plane, plane)], stage.at[0])
    load(str_hbm.at[pl.ds(5 * plane, plane)], stage.at[1])
    load(buo_hbm, buo)
    load(str_hbm.at[pl.ds(0 * plane, plane)], sx.at[pl.ds(sx_row(0, 0, 0), plane)])
    load(str_hbm.at[pl.ds(4 * plane, plane)], sx.at[pl.ds(sx_row(0, 4, 0), plane)])
    first = len(loads)
    load(str_hbm.at[pl.ds(2 * plane, plane)], zb.at[pl.ds(0, plane)])
    load(vel_hbm, vel)
    second = len(loads)
    load(zone_hbm, zone)
    load(elig_hbm, elig)
    third = len(loads)
    load(lam_hbm, lam)
    load(mod_hbm, mod)

    tile = jnp.zeros((rows_y, depth), jnp.float32)

    for step in range(STEPS):
        for comp in SLOT_X:
            for layer in (-2, -1, rows_x, rows_x + 1):
                sx[pl.ds(sx_row(step, comp, layer), rows_y), :] = tile
    for ref in (xf, yf):
        for i in range(ref.shape[0] // rows_y):
            ref[pl.ds(i * rows_y, rows_y), :] = tile

    def clear(i, carry):
        sy[pl.ds(pl.multiple_of(i * R + rows_y, 8), R - rows_y), :] = jnp.zeros((R - rows_y, depth), jnp.float32)
        return carry

    lax.fori_loop(0, sy.shape[0] // R, clear, 0, unroll=8)

    for up in (True, False):

        @pl.when(jnp.logical_not(to_x(not up)[0]))
        def _():
            for step in range(STEPS):
                for i in range(rx.shape[2]):
                    rx[step, int(up), i] = tile

        @pl.when(jnp.logical_not(to_y(not up)[0]))
        def _():
            for step in range(STEPS):

                def wipe(c, carry):
                    for i in range(ry.shape[3] // 8):
                        ry[step, int(up), c, pl.ds(i * 8, 8), :] = tile
                    return carry

                lax.fori_loop(0, chunks, wipe, 0)

    for d, (cx, cy) in enumerate(CORNERS):

        @pl.when(jnp.logical_not(to_corner(not cx, not cy)[0]))
        def _():
            for step in range(STEPS):
                for i in range(rd.shape[2] // 8):
                    rd[step, d, pl.ds(i * 8, 8), :] = tile

    def x_copy(step, up):
        count = len(raw_x[up]) + len(flow_x[up]) + (2 if step == 0 else 0)
        return pltpu.make_async_remote_copy(
            src_ref=xs.at[step, int(up), pl.ds(0, count)],
            dst_ref=rx.at[step, int(up), pl.ds(0, count)],
            send_sem=xsend.at[step, int(up)],
            recv_sem=xrecv.at[step, int(up)],
            device_id=to_x(up)[1],
            device_id_type=MESH,
        )

    def y_parts(step):
        return (0,) if step == 0 else (0, 1)

    def y_copy(step, up, c, part):
        raw, flow = len(raw_y[up]), len(flow_y[up])
        start, count = (0, raw + flow + 2) if step == 0 else ((0, raw), (raw, flow))[part]
        return pltpu.make_async_remote_copy(
            src_ref=ys.at[step, int(up), c, pl.ds(start * 8, count * 8)],
            dst_ref=ry.at[step, int(up), c, pl.ds(start * 8, count * 8)],
            send_sem=ysend.at[step, int(up), c, part],
            recv_sem=yrecv.at[step, int(up), c, part],
            device_id=to_y(up)[1],
            device_id_type=MESH,
        )

    def d_copy(step, d):
        return pltpu.make_async_remote_copy(
            src_ref=ds.at[step, d, pl.ds(0, len(corner[CORNERS[d]]))],
            dst_ref=rd.at[step, d, pl.ds(0, len(corner[CORNERS[d]]))],
            send_sem=dsend.at[step, d],
            recv_sem=drecv.at[step, d],
            device_id=to_corner(*CORNERS[d])[1],
            device_id_type=MESH,
        )

    def sx_tile(step, comp, x):
        return sx[pl.ds(sx_row(step, comp, x), rows_y), :]

    def sy_pack(step, comp, c, row):
        return sy[pl.ds(sy_row(step, comp, c * CH) + row, CH, stride=R), :]

    def vb_pack(step, slot, c, row):
        return pl.ds(vb_row(step, slot, c * CH) + row, CH, stride=R)

    def pack_x_raw(step, up):
        for i, (comp, x) in enumerate(raw_x[up]):
            xs[step, int(up), i] = sx_tile(step, comp, x)
        if step == 0:
            for i, x in enumerate(buo_x[up]):
                xs[step, int(up), len(raw_x[up]) + len(flow_x[up]) + i] = buo[pl.ds(x * rows_y, rows_y), :]

    def pack_y_raw(step, c):
        for up in (True, False):
            for i, (comp, row) in enumerate(raw_y[up]):
                ys[step, int(up), c, pl.ds(i * 8, 8), :] = sy_pack(step, comp, c, row)
            if step == 0:
                for i, row in enumerate(buo_y[up]):
                    value = buo[pl.ds(c * CH * rows_y + row, CH, stride=rows_y), :]
                    ys[step, int(up), c, pl.ds((len(raw_y[up]) + len(flow_y[up]) + i) * 8, 8), :] = value

    def pack_x_flow(step, up):
        for i, (slot, x) in enumerate(flow_x[up]):
            xs[step, int(up), len(raw_x[up]) + i] = vb[pl.ds(vb_row(step, slot, x), rows_y), :]

    def pack_y_flow(step, c):
        for up in (True, False):
            for i, (slot, row) in enumerate(flow_y[up]):
                ys[step, int(up), c, pl.ds((len(raw_y[up]) + i) * 8, 8), :] = vb[vb_pack(step, slot, c, row), :]

    def pack_corners(step, cxs):
        for d, (cx, cy) in enumerate(CORNERS):
            if cx in cxs:
                for i, (comp, x, y) in enumerate(corner[(cx, cy)]):
                    if comp in SLOT_X:
                        value = sx[pl.ds(sx_row(step, comp, x) + y, 1), :]
                    else:
                        value = sy[pl.ds(sy_row(step, comp, x) + y, 1), :]
                    ds[step, d, pl.ds(i, 1), :] = value

    def send_x(step, core):
        mine = iy % 2 == core
        odd = ix % 2 == 1
        for up, when in ((True, odd), (False, True), (True, jnp.logical_not(odd))):

            @pl.when(jnp.logical_and(jnp.logical_and(to_x(up)[0], mine), when))
            def _():
                x_copy(step, up).start()

    def send_y(step, cs, parts):
        for up in (True, False):

            @pl.when(to_y(up)[0])
            def _():
                for c in cs:
                    for part in parts:
                        y_copy(step, up, c, part).start()

    def send_corners(step, cxs):
        for d, (cx, cy) in enumerate(CORNERS):
            if cx in cxs:

                @pl.when(to_corner(cx, cy)[0])
                def _():
                    d_copy(step, d).start()

    lane = lax.broadcasted_iota(jnp.int32, (rows_y, depth), 1)
    keep = {
        1: lane < depth - 1,
        2: lane < depth - 2,
        -1: lane >= 1,
        -2: lane >= 2,
    }

    def along_z(value, offset):
        if offset == 0:
            return value
        return jnp.where(keep[offset], pltpu.roll(value, (-offset) % depth, 1), 0.0)

    def derivative(get, forward):
        a, b, c, d = (get(1), get(0), get(2), get(-1)) if forward else (get(0), get(-1), get(1), get(-2))
        return 27.0 * (a - b) - (c - d)

    def s_dx(step, comp, x, forward):
        return derivative(lambda o: sx_tile(step, comp, x + o), forward)

    def s_dy(step, comp, x, forward):
        return derivative(lambda o: sy[pl.ds(sy_row(step, comp, x) + o, rows_y), :], forward)

    def v_dx(step, slot, x, forward):
        return derivative(lambda o: vb[pl.ds(vb_row(step, slot, x + o), rows_y), :], forward)

    def v_dy(step, slot, x, forward):
        return derivative(lambda o: vb[pl.ds(vb_row(step, slot, x) + o, rows_y), :], forward)

    def dz(value, forward):
        return derivative(lambda o: along_z(value, o), forward)

    def own_sy(step, comp, x):
        return sy[pl.ds(sy_row(step, comp, x), rows_y), :]

    def own_zb(step, x):
        return zb[pl.ds((step * rows_x + x) * rows_y, rows_y), :]

    def own_v(step, slot, x):
        return vb[pl.ds(vb_row(step, slot, x), rows_y), :]

    def of_cell(ref, x):
        return ref[pl.ds(x * rows_y, rows_y), :]

    weight = time_step / 24.0

    def flow_layer(step, x):
        scale = weight * of_cell(buo, x)
        xz = sx_tile(step, 4, x)
        yz = own_sy(step, 5, x)
        zz = own_zb(step, x)
        force_x = s_dx(step, 0, x, True) + s_dy(step, 3, x, False) + dz(xz, False)
        force_y = s_dx(step, 3, x, False) + s_dy(step, 1, x, True) + dz(yz, False)
        force_z = s_dx(step, 4, x, False) + s_dy(step, 5, x, False) + dz(zz, True)
        for slot, force in enumerate((force_x, force_y, force_z)):
            old = vel[pl.ds((slot * rows_x + x) * rows_y, rows_y), :] if step == 0 else own_v(step - 1, slot, x)
            vb[pl.ds(vb_row(step, slot, x), rows_y), :] = old + scale * force

    def wait_x(step):
        for up in (True, False):

            @pl.when(to_x(not up)[0])
            def _():
                x_copy(step, up).wait_recv()

    def wait_y(step, cs):
        for up in (True, False):

            @pl.when(to_y(not up)[0])
            def _():
                for c in cs:
                    for part in y_parts(step):
                        y_copy(step, up, c, part).wait_recv()

    def wait_corners(step):
        for d, (cx, cy) in enumerate(CORNERS):

            @pl.when(to_corner(not cx, not cy)[0])
            def _():
                d_copy(step, d).wait_recv()

    def place(items, what):
        return [i for i, item in enumerate(items) if item == what][0]

    def take_corners(step):
        for d, (cx, cy) in enumerate(CORNERS):

            def raw(comp, x, y):
                return rd[step, d, pl.ds(place(corner[(cx, cy)], (comp, x, y)), 1), :]

            for k in range(3):
                comp, kind = FORCE_Y[k]
                ys_ = edge(kind, cy, rows_y)
                for x in edge(FLOW_X[k], cx, rows_x):
                    base = (int(cx) * 5 + place(flow_x[cx], (k, x))) * rows_y
                    for row, value in spread(kind, cy, rows_y, lambda i: raw(comp, x, ys_[i])):
                        xf[pl.ds(base + row, 1), :] = value
                comp, kind = FORCE_X[k]
                xs_ = edge(kind, cx, rows_x)
                for y in edge(FLOW_Y[k], cy, rows_y):
                    base = ((int(cy) * 5 + place(flow_y[cy], (k, y))) * 2 + int(cx)) * 8
                    for layer, value in spread(kind, cx, CH, lambda i: raw(comp, xs_[i], y)):
                        yf[pl.ds(base + layer, 1), :] = value

    def finish_x(step):
        for up in (True, False):
            side = int(up)
            for k, (comp, kind) in enumerate(FORCE_X):
                places = [place(raw_x[up], (comp, x)) for x in edge(kind, up, rows_x)]
                for x, value in spread(kind, up, rows_x, lambda i: rx[step, side, places[i]]):
                    where = pl.ds(vb_row(step, k, x), rows_y)
                    vb[where, :] = vb[where, :] + weight * of_cell(buo, x) * value
            for k, (comp, kind) in enumerate(FORCE_X):
                mine = edge(kind, not up, rows_x)
                adds = dict(spread(kind, not up, rows_x, lambda i: sx_tile(step, comp, mine[i])))
                for x in edge(FLOW_X[k], up, rows_x):
                    i = place(flow_x[up], (k, x))
                    add = adds[x] + xf[pl.ds((side * 5 + i) * rows_y, rows_y), :]
                    scale = weight * rx[0, side, len(raw_x[up]) + len(flow_x[up]) + place(buo_x[up], x)]
                    new = rx[step, side, len(raw_x[up]) + i] + scale * add
                    at = x - rows_x if up else x + rows_x
                    vb[pl.ds(vb_row(step, k, at), rows_y), :] = new

    def buo_halo_y(up, c, y):
        i = len(raw_y[up]) + len(flow_y[up]) + place(buo_y[up], y)
        return ry[0, int(up), c, pl.ds(i * 8, 8), :]

    def finish_y(step, c):
        for up in (True, False):
            side = int(up)

            def got(i):
                return ry[step, side, c, pl.ds(i * 8, 8), :]

            for k, (comp, kind) in enumerate(FORCE_Y):
                places = [place(raw_y[up], (comp, y)) for y in edge(kind, up, rows_y)]
                for y, value in spread(kind, up, rows_y, lambda i: got(places[i])):
                    where = vb_pack(step, k, c, y)
                    scale = weight * buo[pl.ds(c * CH * rows_y + y, CH, stride=rows_y), :]
                    vb[where, :] = vb[where, :] + scale * value
            for k, (comp, kind) in enumerate(FORCE_Y):
                mine = edge(kind, not up, rows_y)
                adds = dict(spread(kind, not up, rows_y, lambda i: sy_pack(step, comp, c, mine[i])))
                for y in edge(FLOW_Y[k], up, rows_y):
                    i = place(flow_y[up], (k, y))
                    scale = weight * buo_halo_y(up, c, y)
                    new = got(len(raw_y[up]) + i) + scale * adds[y]
                    at = y - rows_y if up else y + rows_y
                    vb[vb_pack(step, k, c, at), :] = new

    def finish_corners_y(step):
        for up in (True, False):
            for i, (k, y) in enumerate(flow_y[up]):
                at = y - rows_y if up else y + rows_y
                for end, c in ((1, 0), (0, chunks - 1)):
                    add = yf[pl.ds(((int(up) * 5 + i) * 2 + end) * 8, 8), :]
                    where = vb_pack(step, k, c, at)
                    vb[where, :] = vb[where, :] + weight * buo_halo_y(up, c, y) * add

    def stress_layer(step, x):
        last = step == STEPS - 1
        vx, vy, vz = (own_v(step, slot, x) for slot in range(3))
        if last:
            for slot, value in enumerate((vx, vy, vz)):
                vout_ref[slot, x] = value
        ex = v_dx(step, 0, x, False)
        ey = v_dy(step, 1, x, False)
        ez = dz(vz, False)
        xy = v_dy(step, 0, x, True) + v_dx(step, 1, x, True)
        xz = dz(vx, True) + v_dx(step, 2, x, True)
        yz = dz(vy, True) + v_dy(step, 2, x, True)
        m = weight * mod[x]
        grow = weight * lam[x] * (ex + ey + ez)
        m2 = m + m
        s0, s3, s4 = (sx_tile(step, comp, x) for comp in (0, 3, 4))
        s1, s5 = own_sy(step, 1, x), own_sy(step, 5, x)
        s2 = own_zb(step, x)
        s0 = s0 + (grow + m2 * ex) + inj[0, x]
        s1 = s1 + (grow + m2 * ey) + inj[1, x]
        s2 = s2 + (grow + m2 * ez) + inj[2, x]
        s3 = s3 + m * xy + inj[3, x]
        s4 = s4 + m * xz + inj[4, x]
        s5 = s5 + m * yz + inj[5, x]
        pressure = (s0 + s1 + s2) * (1.0 / 3.0)
        d0, d1, d2 = s0 - pressure, s1 - pressure, s2 - pressure
        second = 0.5 * (d0 * d0 + d1 * d1 + d2 * d2) + (s3 * s3 + s4 * s4 + s5 * s5)
        strength = jnp.maximum(cc[x] - pressure * cf[x], 0.0)
        factor = jnp.minimum(1.0, strength * lax.rsqrt(jnp.maximum(second, shear_floor * shear_floor)))
        s0, s1, s2 = pressure + factor * d0, pressure + factor * d1, pressure + factor * d2
        s3, s4, s5 = factor * s3, factor * s4, factor * s5
        if last:
            for comp, value in enumerate((s0, s1, s2, s3, s4, s5)):
                sout_ref[comp, x] = value
            return
        for comp, value in ((0, s0), (3, s3), (4, s4)):
            sx[pl.ds(sx_row(step + 1, comp, x), rows_y), :] = value
        for comp, value in ((3, s3), (1, s1), (5, s5)):
            sy[pl.ds(sy_row(step + 1, comp, x), rows_y), :] = value
        zb[pl.ds(((step + 1) * rows_x + x) * rows_y, rows_y), :] = s2

    for copy in loads[:first]:
        copy.wait()

    def fill_y(i, carry):
        at = pl.multiple_of(i * rows_y, 8)
        for comp, value in (
            (3, sx[pl.ds(sx_row(0, 3, 0) + at, rows_y), :]),
            (1, stage[0, pl.ds(at, rows_y), :]),
            (5, stage[1, pl.ds(at, rows_y), :]),
        ):
            sy[pl.ds(pl.multiple_of(sy_row(0, comp, 0) + i * R, 8), rows_y), :] = value
        return carry

    lax.fori_loop(0, rows_x, fill_y, 0, unroll=8)
    for copy in loads[first:second]:
        copy.wait()
    ends = [0] + ([chunks - 1] if chunks > 1 else [])
    middle = list(range(1, chunks - 1))
    for up in (True, False):
        pack_x_raw(0, up)
    pack_corners(0, (True, False))
    for c in ends + middle:
        pack_y_raw(0, c)
        for i in range(CH):
            flow_layer(0, c * CH + i)
        pack_y_flow(0, c)
    for up in (True, False):
        pack_x_flow(0, up)
    heard = sum(there.astype(jnp.int32) for there, _ in sides)
    pl.semaphore_wait(barrier, heard)
    send_corners(0, (True, False))
    send_x(0, 0)
    send_y(0, ends + middle, (0,))

    cell = cell_ref[...]
    bits = depth.bit_length() - 1
    assert depth == 1 << bits
    plane_row = cell >> bits
    cell_z = cell & (depth - 1)
    row = lax.broadcasted_iota(jnp.int32, (rows_x * rows_y, cell.shape[1]), 0)
    row_bits = rows_y.bit_length() - 1
    assert rows_y == 1 << row_bits
    row = (ix * rows_x + (row >> row_bits)) * (ny * rows_y) + iy * rows_y + (row & (rows_y - 1))
    match = row == plane_row
    at_z = (lax.broadcasted_iota(jnp.int32, (depth, cell.shape[1]), 0) == cell_z).astype(jnp.float32)
    for comp in range(6):
        moment = time_step * moment_ref[pl.ds(comp, 1), :]
        value = lax.dot_general(
            jnp.where(match, moment, 0.0),
            at_z,
            (((1,), (1,)), ((), ())),
            precision=lax.Precision.HIGHEST,
            preferred_element_type=jnp.float32,
        )
        inj[comp] = value.reshape(rows_x, rows_y, depth)

    send_x(0, 1)
    for copy in loads[second:third]:
        copy.wait()
    frictions, cohesions = [], []
    for which in range(coh_ref.shape[0]):
        f = jnp.full((rows_y, depth), fri_ref[which], jnp.float32)
        frictions.append(f)
        cohesions.append(coh_ref[which] * jnp.sqrt(1.0 - f * f))

    def table(x, carry):
        z = jnp.where(elig[x] == 1, zone[x], -1)
        c = jnp.full((rows_y, depth), 1e30, jnp.float32)
        f = jnp.zeros((rows_y, depth), jnp.float32)
        for which in range(coh_ref.shape[0]):
            hit = z == which
            c = jnp.where(hit, cohesions[which], c)
            f = jnp.where(hit, frictions[which], f)
        cc[x] = c
        cf[x] = f
        return carry

    lax.fori_loop(0, rows_x, table, 0, unroll=2)

    for copy in loads[third:]:
        copy.wait()

    rim = [x for x in range(rows_x) if x < 4 or x >= rows_x - 4]
    near = [x for x in range(rows_x) if x not in rim and (x < CH + 2 or x >= rows_x - CH - 2)]
    inner = [x for x in range(rows_x) if x not in rim and x not in near]
    for step in range(STEPS):
        nxt = step + 1
        last = nxt == STEPS
        wait_y(step, ends)
        for c in ends:
            finish_y(step, c)
        wait_corners(step)
        take_corners(step)
        finish_corners_y(step)
        wait_x(step)
        finish_x(step)
        for x in rim:
            stress_layer(step, x)
        flowed = set()
        if not last:
            pack_corners(nxt, (True, False))
            send_corners(nxt, (True, False))
            for x in (0, 1, rows_x - 2, rows_x - 1):
                flow_layer(nxt, x)
                flowed.add(x)
            for up in (True, False):
                pack_x_raw(nxt, up)
                pack_x_flow(nxt, up)
            send_x(nxt, 0)
        wait_y(step, middle)
        for c in middle:
            finish_y(step, c)
        for x in near:
            stress_layer(step, x)
        if not last:
            for c in ends:
                pack_y_raw(nxt, c)
            send_y(nxt, ends, (0,))
            for c in ends:
                for x in range(c * CH, (c + 1) * CH):
                    if x not in flowed:
                        flow_layer(nxt, x)
                pack_y_flow(nxt, c)
            send_y(nxt, ends, (1,))
            send_x(nxt, 1)
        for x in inner:
            stress_layer(step, x)
        if not last:
            for c in middle:
                pack_y_raw(nxt, c)
            send_y(nxt, middle, (0,))
            for c in middle:
                for x in range(c * CH, (c + 1) * CH):
                    flow_layer(nxt, x)
                pack_y_flow(nxt, c)
                send_y(nxt, (c,), (1,))

    for step in range(STEPS):
        for up in (True, False):

            @pl.when(to_x(up)[0])
            def _():
                x_copy(step, up).wait_send()

            @pl.when(to_y(up)[0])
            def _():
                for c in range(chunks):
                    for part in y_parts(step):
                        y_copy(step, up, c, part).wait_send()

        for d, (cx, cy) in enumerate(CORNERS):

            @pl.when(to_corner(cx, cy)[0])
            def _():
                d_copy(step, d).wait_send()


def on_device(nx, ny, velocity, stress, lame_first, modulus, buoyancy, zone, eligible, cohesion, friction, source_cell, source_moment):
    rows_x, rows_y, depth = zone.shape
    assert rows_y == 8 and rows_x % CH == 0 and rows_x >= 3 * CH
    chunks = rows_x // CH
    f32 = jnp.float32
    grid = (rows_x, rows_y, depth)
    plane = rows_x * rows_y
    any_spec = pl.BlockSpec(memory_space=pltpu.HBM)
    smem = pl.BlockSpec(memory_space=pltpu.SMEM)
    vmem = pl.BlockSpec(memory_space=pltpu.VMEM)
    dma = pltpu.SemaphoreType.DMA
    return pl.pallas_call(
        functools.partial(kernel, nx, ny),
        out_shape=(pltpu.VMEM((3,) + grid, f32), pltpu.VMEM((6,) + grid, f32)),
        in_specs=[any_spec] * 7 + [smem, smem, vmem, vmem],
        out_specs=(vmem, vmem),
        scratch_shapes=[
            pltpu.VMEM((2, plane, depth), f32),
            pltpu.VMEM((3 * plane, depth), f32),
            pltpu.VMEM(grid, f32),
            pltpu.VMEM(grid, f32),
            pltpu.VMEM((plane, depth), f32),
            pltpu.VMEM(grid, jnp.int32),
            pltpu.VMEM(grid, jnp.int32),
            pltpu.VMEM((6,) + grid, f32),
            pltpu.VMEM(grid, f32),
            pltpu.VMEM(grid, f32),
            pltpu.VMEM((STEPS * 3 * (rows_x + 4) * rows_y, depth), f32),
            pltpu.VMEM((STEPS * 3 * R * (rows_x + 1) + R, depth), f32),
            pltpu.VMEM((STEPS * plane, depth), f32),
            pltpu.VMEM((STEPS * 3 * (rows_x + 5) * R, depth), f32),
            pltpu.VMEM((STEPS, 2, 11, rows_y, depth), f32),
            pltpu.VMEM((STEPS, 2, 11, rows_y, depth), f32),
            pltpu.VMEM((STEPS, 2, chunks, 11 * 8, depth), f32),
            pltpu.VMEM((STEPS, 2, chunks, 11 * 8, depth), f32),
            pltpu.VMEM((STEPS, 4, 16, depth), f32),
            pltpu.VMEM((STEPS, 4, 16, depth), f32),
            pltpu.VMEM((2 * 5 * rows_y, depth), f32),
            pltpu.VMEM((2 * 5 * 2 * 8, depth), f32),
            dma((12,)),
            dma((STEPS, 2)),
            dma((STEPS, 2)),
            dma((STEPS, 2, chunks, 2)),
            dma((STEPS, 2, chunks, 2)),
            dma((STEPS, 4)),
            dma((STEPS, 4)),
        ],
        compiler_params=pltpu.CompilerParams(collective_id=0, has_side_effects=True),
    )(
        velocity.reshape(3 * plane, depth), stress.reshape(6 * plane, depth), lame_first, modulus,
        buoyancy.reshape(plane, depth), zone, eligible,
        cohesion, friction, source_cell.reshape(1, -1), source_moment,
    )


def solution(mesh):
    field = P(None, "gx", "gy", None)
    cells = P("gx", "gy", None)
    return jax.shard_map(
        functools.partial(on_device, mesh.shape["gx"], mesh.shape["gy"]),
        mesh=mesh,
        in_specs=(field, field, cells, cells, cells, cells, cells, P(), P(), P(), P()),
        out_specs=(field, field),
        check_vma=False,
    )
```

```python
import functools

import jax
import jax.numpy as jnp
from jax import lax
from jax.experimental import pallas as pl
from jax.experimental.pallas import tpu as pltpu
from jax.sharding import PartitionSpec as P

STEPS = 2
time_step = 0.1
shear_floor = 0.25
MESH = pl.DeviceIdType.MESH
CH = 8
R = 16

BACK = {"F": 1, "B": 2}
AHEAD = {"F": 2, "B": 1}
FORCE_X = ((0, "F"), (3, "B"), (4, "B"))
FORCE_Y = ((3, "B"), (1, "F"), (5, "B"))
FLOW_X = ("B", "F", "F")
FLOW_Y = ("F", "B", "F")
SLOT_X = {0: 0, 3: 1, 4: 2}
SLOT_Y = {3: 0, 1: 1, 5: 2}


def edge(kind, up, n):
    return list(range(n - BACK[kind], n)) if up else list(range(AHEAD[kind]))


def spread(kind, up, n, get):
    if up and kind == "B":
        return [(0, get(0) - 27.0 * get(1)), (1, get(1))]
    if up:
        return [(0, get(0))]
    if kind == "B":
        return [(n - 1, -get(0))]
    return [(n - 1, 27.0 * get(0) - get(1)), (n - 2, -get(0))]


def raw_list(force, up, n):
    return [(comp, i) for comp, kind in force for i in edge(kind, up, n)]


def flow_list(flow, up, n):
    return [(slot, i) for slot, kind in enumerate(flow) for i in edge(kind, up, n)]


def corner_list(sx, sy, nx, ny):
    found = []
    for k in range(3):
        comp, kind = FORCE_Y[k]
        found += [(comp, x, y) for x in edge(FLOW_X[k], sx, nx) for y in edge(kind, sy, ny)]
        comp, kind = FORCE_X[k]
        found += [(comp, x, y) for x in edge(kind, sx, nx) for y in edge(FLOW_Y[k], sy, ny)]
    return list(dict.fromkeys(found))


CORNERS = [(False, True), (False, False), (True, True), (True, False)]


class Fields:
    def __init__(self, sx, sy, zb, vb, lam, mod, inj, cc, cf):
        self.sx, self.sy, self.zb, self.vb = sx, sy, zb, vb
        self.lam, self.mod, self.inj, self.cc, self.cf = lam, mod, inj, cc, cf
        self.rows_x, self.rows_y, self.depth = lam.shape
        lane = lax.broadcasted_iota(jnp.int32, (self.rows_y, self.depth), 1)
        self.keep = {1: lane < self.depth - 1, 2: lane < self.depth - 2, -1: lane >= 1, -2: lane >= 2}

    def sx_row(self, comp, x):
        return (SLOT_X[comp] * (self.rows_x + 4) + x + 2) * self.rows_y

    def sy_row(self, comp, x):
        return SLOT_Y[comp] * R * (self.rows_x + 1) + R * (x + 1)

    def vb_row(self, slot, x):
        return (slot * (self.rows_x + 5) + x + 3) * R

    def sx_tile(self, step, comp, x):
        return self.sx[step][pl.ds(self.sx_row(comp, x), self.rows_y), :]

    def own_sy(self, step, comp, x):
        return self.sy[step][pl.ds(self.sy_row(comp, x), self.rows_y), :]

    def own_zb(self, step, x):
        return self.zb[step][pl.ds(x * self.rows_y, self.rows_y), :]

    def own_v(self, step, slot, x):
        return self.vb[step][pl.ds(self.vb_row(slot, x), self.rows_y), :]

    def along_z(self, value, offset):
        if offset == 0:
            return value
        return jnp.where(self.keep[offset], pltpu.roll(value, (-offset) % self.depth, 1), 0.0)

    def derivative(self, get, forward):
        a, b, c, d = (get(1), get(0), get(2), get(-1)) if forward else (get(0), get(-1), get(1), get(-2))
        return 27.0 * (a - b) - (c - d)

    def s_dx(self, step, comp, x, forward):
        return self.derivative(lambda o: self.sx_tile(step, comp, x + o), forward)

    def s_dy(self, step, comp, x, forward):
        row = self.sy_row(comp, x)
        return self.derivative(lambda o: self.sy[step][pl.ds(row + o, self.rows_y), :], forward)

    def v_dx(self, step, slot, x, forward):
        return self.derivative(lambda o: self.own_v(step, slot, x + o), forward)

    def v_dy(self, step, slot, x, forward):
        row = self.vb_row(slot, x)
        return self.derivative(lambda o: self.vb[step][pl.ds(row + o, self.rows_y), :], forward)

    def dz(self, value, forward):
        return self.derivative(lambda o: self.along_z(value, o), forward)

    def forces(self, step, x):
        xz, yz, zz = self.sx_tile(step, 4, x), self.own_sy(step, 5, x), self.own_zb(step, x)
        return (
            self.s_dx(step, 0, x, True) + self.s_dy(step, 3, x, False) + self.dz(xz, False),
            self.s_dx(step, 3, x, False) + self.s_dy(step, 1, x, True) + self.dz(yz, False),
            self.s_dx(step, 4, x, False) + self.s_dy(step, 5, x, False) + self.dz(zz, True),
        )

    def stress(self, step, x):
        vx, vy, vz = (self.own_v(step, slot, x) for slot in range(3))
        ex = self.v_dx(step, 0, x, False)
        ey = self.v_dy(step, 1, x, False)
        ez = self.dz(vz, False)
        xy = self.v_dy(step, 0, x, True) + self.v_dx(step, 1, x, True)
        xz = self.dz(vx, True) + self.v_dx(step, 2, x, True)
        yz = self.dz(vy, True) + self.v_dy(step, 2, x, True)
        weight = time_step / 24.0
        inj = self.inj
        m = weight * self.mod[x]
        grow = weight * self.lam[x] * (ex + ey + ez)
        m2 = m + m
        s0, s3, s4 = (self.sx_tile(step, comp, x) for comp in (0, 3, 4))
        s1, s5 = self.own_sy(step, 1, x), self.own_sy(step, 5, x)
        s2 = self.own_zb(step, x)
        s0 = s0 + (grow + m2 * ex) + inj[0, x]
        s1 = s1 + (grow + m2 * ey) + inj[1, x]
        s2 = s2 + (grow + m2 * ez) + inj[2, x]
        s3 = s3 + m * xy + inj[3, x]
        s4 = s4 + m * xz + inj[4, x]
        s5 = s5 + m * yz + inj[5, x]
        pressure = (s0 + s1 + s2) * (1.0 / 3.0)
        d0, d1, d2 = s0 - pressure, s1 - pressure, s2 - pressure
        second = 0.5 * (d0 * d0 + d1 * d1 + d2 * d2) + (s3 * s3 + s4 * s4 + s5 * s5)
        strength = jnp.maximum(self.cc[x] - pressure * self.cf[x], 0.0)
        factor = jnp.minimum(1.0, strength * lax.rsqrt(jnp.maximum(second, shear_floor * shear_floor)))
        s0, s1, s2 = pressure + factor * d0, pressure + factor * d1, pressure + factor * d2
        return s0, s1, s2, factor * s3, factor * s4, factor * s5


def finish_kernel(sx, sy, zb, vb, lam, mod, inj, cc, cf, vout_hbm, sout_hbm, vout, sout, sem):
    at = Fields((None, sx), (None, sy), (None, zb), (None, vb), lam, mod, inj, cc, cf)
    copies = []
    for c in range(at.rows_x // CH):
        for x in range(c * CH, (c + 1) * CH):
            for slot in range(3):
                vout[slot, x] = at.own_v(STEPS - 1, slot, x)
            for comp, value in enumerate(at.stress(STEPS - 1, x)):
                sout[comp, x] = value
        for i, (src, dst) in enumerate(((vout, vout_hbm), (sout, sout_hbm))):
            layers = pl.ds(c * CH, CH)
            copy = pltpu.make_async_copy(src.at[:, layers], dst.at[:, layers], sem.at[c, i])
            copy.start()
            copies.append(copy)
    for copy in copies:
        copy.wait()


def kernel(
    nx,
    ny,
    vel_hbm, str_hbm, lam_hbm, mod_hbm, buo_hbm, zone_hbm, elig_hbm,
    coh_ref, fri_ref, cell_ref, moment_ref,
    sx1, sy1, zb1, vb1, lam, mod, inj, cc, cf,
    sx0, sy0, zb0, vb0, stage, vel, buo, zone, elig,
    xs, rx, ys, ry, ds, rd, xf, yf,
    load_sem, xsend, xrecv, ysend, yrecv, dsend, drecv,
):
    rows_x = lam.shape[0]
    rows_y = lam.shape[1]
    depth = lam.shape[2]
    chunks = rows_x // CH
    sx, sy, zb, vb = (sx0, sx1), (sy0, sy1), (zb0, zb1), (vb0, vb1)
    at = Fields(sx, sy, zb, vb, lam, mod, inj, cc, cf)
    sx_row, sy_row, vb_row, sx_tile = at.sx_row, at.sy_row, at.vb_row, at.sx_tile
    ix = lax.axis_index("gx")
    iy = lax.axis_index("gy")
    x_lo, x_hi, y_lo, y_hi = ix > 0, ix < nx - 1, iy > 0, iy < ny - 1

    def to_x(up):
        return (x_hi, (ix + 1, iy)) if up else (x_lo, (ix - 1, iy))

    def to_y(up):
        return (y_hi, (ix, iy + 1)) if up else (y_lo, (ix, iy - 1))

    def to_corner(cx, cy):
        there = jnp.logical_and(to_x(cx)[0], to_y(cy)[0])
        return there, (to_x(cx)[1][0], to_y(cy)[1][1])

    sides = [to_x(True), to_x(False), to_y(True), to_y(False)] + [to_corner(*c) for c in CORNERS]
    barrier = pltpu.get_barrier_semaphore()
    for there, target in sides:

        @pl.when(there)
        def _():
            pl.semaphore_signal(barrier, inc=1, device_id=target, device_id_type=MESH)

    raw_x = {up: raw_list(FORCE_X, up, rows_x) for up in (True, False)}
    raw_y = {up: raw_list(FORCE_Y, up, rows_y) for up in (True, False)}
    flow_x = {up: flow_list(FLOW_X, up, rows_x) for up in (True, False)}
    flow_y = {up: flow_list(FLOW_Y, up, rows_y) for up in (True, False)}
    buo_x = {True: [rows_x - 2, rows_x - 1], False: [0, 1]}
    buo_y = {True: [rows_y - 2, rows_y - 1], False: [0, 1]}
    corner = {c: corner_list(c[0], c[1], rows_x, rows_y) for c in CORNERS}

    loads = []

    def load(src, dst):
        copy = pltpu.make_async_copy(src, dst, load_sem.at[len(loads)])
        copy.start()
        loads.append(copy)

    plane = rows_x * rows_y
    load(str_hbm.at[pl.ds(3 * plane, plane)], sx0.at[pl.ds(sx_row(3, 0), plane)])
    load(str_hbm.at[pl.ds(1 * plane, plane)], stage.at[0])
    load(str_hbm.at[pl.ds(5 * plane, plane)], stage.at[1])
    load(buo_hbm, buo)
    load(str_hbm.at[pl.ds(0 * plane, plane)], sx0.at[pl.ds(sx_row(0, 0), plane)])
    load(str_hbm.at[pl.ds(4 * plane, plane)], sx0.at[pl.ds(sx_row(4, 0), plane)])
    first = len(loads)
    load(str_hbm.at[pl.ds(2 * plane, plane)], zb0)
    load(vel_hbm, vel)
    second = len(loads)
    load(zone_hbm, zone)
    load(elig_hbm, elig)
    third = len(loads)
    load(lam_hbm, lam)
    load(mod_hbm, mod)

    tile = jnp.zeros((rows_y, depth), jnp.float32)

    for step in range(STEPS):
        for comp in SLOT_X:
            for layer in (-2, -1, rows_x, rows_x + 1):
                sx[step][pl.ds(sx_row(comp, layer), rows_y), :] = tile
    for ref in (xf, yf):
        for i in range(ref.shape[0] // rows_y):
            ref[pl.ds(i * rows_y, rows_y), :] = tile

    def clear(i, carry):
        for ref in sy:
            ref[pl.ds(pl.multiple_of(i * R + rows_y, 8), R - rows_y), :] = jnp.zeros((R - rows_y, depth), jnp.float32)
        return carry

    lax.fori_loop(0, sy0.shape[0] // R, clear, 0, unroll=4)

    for up in (True, False):

        @pl.when(jnp.logical_not(to_x(not up)[0]))
        def _():
            for step in range(STEPS):
                for i in range(rx.shape[2]):
                    rx[step, int(up), i] = tile

        @pl.when(jnp.logical_not(to_y(not up)[0]))
        def _():
            for step in range(STEPS):

                def wipe(c, carry):
                    for i in range(ry.shape[3] // 8):
                        ry[step, int(up), c, pl.ds(i * 8, 8), :] = tile
                    return carry

                lax.fori_loop(0, chunks, wipe, 0)

    for d, (cx, cy) in enumerate(CORNERS):

        @pl.when(jnp.logical_not(to_corner(not cx, not cy)[0]))
        def _():
            for step in range(STEPS):
                for i in range(rd.shape[2] // 8):
                    rd[step, d, pl.ds(i * 8, 8), :] = tile

    def x_copy(step, up):
        count = len(raw_x[up]) + len(flow_x[up]) + (2 if step == 0 else 0)
        return pltpu.make_async_remote_copy(
            src_ref=xs.at[step, int(up), pl.ds(0, count)],
            dst_ref=rx.at[step, int(up), pl.ds(0, count)],
            send_sem=xsend.at[step, int(up)],
            recv_sem=xrecv.at[step, int(up)],
            device_id=to_x(up)[1],
            device_id_type=MESH,
        )

    def y_parts(step):
        return (0,) if step == 0 else (0, 1)

    def y_copy(step, up, c, part):
        raw, flow = len(raw_y[up]), len(flow_y[up])
        start, count = (0, raw + flow + 2) if step == 0 else ((0, raw), (raw, flow))[part]
        return pltpu.make_async_remote_copy(
            src_ref=ys.at[step, int(up), c, pl.ds(start * 8, count * 8)],
            dst_ref=ry.at[step, int(up), c, pl.ds(start * 8, count * 8)],
            send_sem=ysend.at[step, int(up), c, part],
            recv_sem=yrecv.at[step, int(up), c, part],
            device_id=to_y(up)[1],
            device_id_type=MESH,
        )

    def d_copy(step, d):
        return pltpu.make_async_remote_copy(
            src_ref=ds.at[step, d, pl.ds(0, len(corner[CORNERS[d]]))],
            dst_ref=rd.at[step, d, pl.ds(0, len(corner[CORNERS[d]]))],
            send_sem=dsend.at[step, d],
            recv_sem=drecv.at[step, d],
            device_id=to_corner(*CORNERS[d])[1],
            device_id_type=MESH,
        )

    def sy_pack(step, comp, c, row):
        return sy[step][pl.ds(sy_row(comp, c * CH) + row, CH, stride=R), :]

    def vb_pack(slot, c, row):
        return pl.ds(vb_row(slot, c * CH) + row, CH, stride=R)

    def pack_x_raw(step, up):
        for i, (comp, x) in enumerate(raw_x[up]):
            xs[step, int(up), i] = sx_tile(step, comp, x)
        if step == 0:
            for i, x in enumerate(buo_x[up]):
                xs[step, int(up), len(raw_x[up]) + len(flow_x[up]) + i] = buo[pl.ds(x * rows_y, rows_y), :]

    def pack_y_raw(step, c):
        for up in (True, False):
            for i, (comp, row) in enumerate(raw_y[up]):
                ys[step, int(up), c, pl.ds(i * 8, 8), :] = sy_pack(step, comp, c, row)
            if step == 0:
                for i, row in enumerate(buo_y[up]):
                    value = buo[pl.ds(c * CH * rows_y + row, CH, stride=rows_y), :]
                    ys[step, int(up), c, pl.ds((len(raw_y[up]) + len(flow_y[up]) + i) * 8, 8), :] = value

    def pack_x_flow(step, up):
        for i, (slot, x) in enumerate(flow_x[up]):
            xs[step, int(up), len(raw_x[up]) + i] = vb[step][pl.ds(vb_row(slot, x), rows_y), :]

    def pack_y_flow(step, c):
        for up in (True, False):
            for i, (slot, row) in enumerate(flow_y[up]):
                ys[step, int(up), c, pl.ds((len(raw_y[up]) + i) * 8, 8), :] = vb[step][vb_pack(slot, c, row), :]

    def pack_corners(step, cxs):
        for d, (cx, cy) in enumerate(CORNERS):
            if cx in cxs:
                for i, (comp, x, y) in enumerate(corner[(cx, cy)]):
                    if comp in SLOT_X:
                        value = sx[step][pl.ds(sx_row(comp, x) + y, 1), :]
                    else:
                        value = sy[step][pl.ds(sy_row(comp, x) + y, 1), :]
                    ds[step, d, pl.ds(i, 1), :] = value

    def send_x(step, cores):
        mine = iy % 2 == cores[0]
        for up in (False, True):

            @pl.when(to_x(up)[0] if len(cores) == 2 else jnp.logical_and(to_x(up)[0], mine))
            def _():
                x_copy(step, up).start()

    def send_y(step, cs, parts):
        for up in (True, False):

            @pl.when(to_y(up)[0])
            def _():
                for c in cs:
                    for part in parts:
                        y_copy(step, up, c, part).start()

    def send_corners(step, cxs):
        for d, (cx, cy) in enumerate(CORNERS):
            if cx in cxs:

                @pl.when(to_corner(cx, cy)[0])
                def _():
                    d_copy(step, d).start()

    weight = time_step / 24.0

    def flow_layer(step, x):
        scale = weight * of_cell(buo, x)
        for slot, force in enumerate(at.forces(step, x)):
            old = vel[pl.ds((slot * rows_x + x) * rows_y, rows_y), :] if step == 0 else at.own_v(step - 1, slot, x)
            vb[step][pl.ds(vb_row(slot, x), rows_y), :] = old + scale * force

    def stress_layer(step, x):
        s = at.stress(step, x)
        for comp in SLOT_X:
            sx[step + 1][pl.ds(sx_row(comp, x), rows_y), :] = s[comp]
        for comp in SLOT_Y:
            sy[step + 1][pl.ds(sy_row(comp, x), rows_y), :] = s[comp]
        zb[step + 1][pl.ds(x * rows_y, rows_y), :] = s[2]

    def of_cell(ref, x):
        return ref[pl.ds(x * rows_y, rows_y), :]

    def wait_x(step):
        for up in (True, False):

            @pl.when(to_x(not up)[0])
            def _():
                x_copy(step, up).wait_recv()

    def wait_y(step, cs):
        for up in (True, False):

            @pl.when(to_y(not up)[0])
            def _():
                for c in cs:
                    for part in y_parts(step):
                        y_copy(step, up, c, part).wait_recv()

    def wait_corners(step):
        for d, (cx, cy) in enumerate(CORNERS):

            @pl.when(to_corner(not cx, not cy)[0])
            def _():
                d_copy(step, d).wait_recv()

    def place(items, what):
        return [i for i, item in enumerate(items) if item == what][0]

    def take_corners(step):
        for d, (cx, cy) in enumerate(CORNERS):

            def raw(comp, x, y):
                return rd[step, d, pl.ds(place(corner[(cx, cy)], (comp, x, y)), 1), :]

            for k in range(3):
                comp, kind = FORCE_Y[k]
                ys_ = edge(kind, cy, rows_y)
                for x in edge(FLOW_X[k], cx, rows_x):
                    base = (int(cx) * 5 + place(flow_x[cx], (k, x))) * rows_y
                    for row, value in spread(kind, cy, rows_y, lambda i: raw(comp, x, ys_[i])):
                        xf[pl.ds(base + row, 1), :] = value
                comp, kind = FORCE_X[k]
                xs_ = edge(kind, cx, rows_x)
                for y in edge(FLOW_Y[k], cy, rows_y):
                    base = ((int(cy) * 5 + place(flow_y[cy], (k, y))) * 2 + int(cx)) * 8
                    for layer, value in spread(kind, cx, CH, lambda i: raw(comp, xs_[i], y)):
                        yf[pl.ds(base + layer, 1), :] = value

    def finish_x(step):
        for up in (True, False):
            side = int(up)
            for k, (comp, kind) in enumerate(FORCE_X):
                places = [place(raw_x[up], (comp, x)) for x in edge(kind, up, rows_x)]
                for x, value in spread(kind, up, rows_x, lambda i: rx[step, side, places[i]]):
                    where = pl.ds(vb_row(k, x), rows_y)
                    vb[step][where, :] = vb[step][where, :] + weight * of_cell(buo, x) * value
            for k, (comp, kind) in enumerate(FORCE_X):
                mine = edge(kind, not up, rows_x)
                adds = dict(spread(kind, not up, rows_x, lambda i: sx_tile(step, comp, mine[i])))
                for x in edge(FLOW_X[k], up, rows_x):
                    i = place(flow_x[up], (k, x))
                    add = adds[x] + xf[pl.ds((side * 5 + i) * rows_y, rows_y), :]
                    scale = weight * rx[0, side, len(raw_x[up]) + len(flow_x[up]) + place(buo_x[up], x)]
                    new = rx[step, side, len(raw_x[up]) + i] + scale * add
                    halo = x - rows_x if up else x + rows_x
                    vb[step][pl.ds(vb_row(k, halo), rows_y), :] = new

    def buo_halo_y(up, c, y):
        i = len(raw_y[up]) + len(flow_y[up]) + place(buo_y[up], y)
        return ry[0, int(up), c, pl.ds(i * 8, 8), :]

    def finish_y(step, c):
        for up in (True, False):
            side = int(up)

            def got(i):
                return ry[step, side, c, pl.ds(i * 8, 8), :]

            for k, (comp, kind) in enumerate(FORCE_Y):
                places = [place(raw_y[up], (comp, y)) for y in edge(kind, up, rows_y)]
                for y, value in spread(kind, up, rows_y, lambda i: got(places[i])):
                    where = vb_pack(k, c, y)
                    scale = weight * buo[pl.ds(c * CH * rows_y + y, CH, stride=rows_y), :]
                    vb[step][where, :] = vb[step][where, :] + scale * value
            for k, (comp, kind) in enumerate(FORCE_Y):
                mine = edge(kind, not up, rows_y)
                adds = dict(spread(kind, not up, rows_y, lambda i: sy_pack(step, comp, c, mine[i])))
                for y in edge(FLOW_Y[k], up, rows_y):
                    i = place(flow_y[up], (k, y))
                    scale = weight * buo_halo_y(up, c, y)
                    new = got(len(raw_y[up]) + i) + scale * adds[y]
                    halo = y - rows_y if up else y + rows_y
                    vb[step][vb_pack(k, c, halo), :] = new

    def finish_corners_y(step):
        for up in (True, False):
            for i, (k, y) in enumerate(flow_y[up]):
                halo = y - rows_y if up else y + rows_y
                for end, c in ((1, 0), (0, chunks - 1)):
                    add = yf[pl.ds(((int(up) * 5 + i) * 2 + end) * 8, 8), :]
                    where = vb_pack(k, c, halo)
                    vb[step][where, :] = vb[step][where, :] + weight * buo_halo_y(up, c, y) * add

    for copy in loads[:first]:
        copy.wait()

    def fill_y(i, carry):
        first_row = pl.multiple_of(i * rows_y, 8)
        for comp, value in (
            (3, sx0[pl.ds(sx_row(3, 0) + first_row, rows_y), :]),
            (1, stage[0, pl.ds(first_row, rows_y), :]),
            (5, stage[1, pl.ds(first_row, rows_y), :]),
        ):
            sy0[pl.ds(pl.multiple_of(sy_row(comp, 0) + i * R, 8), rows_y), :] = value
        return carry

    lax.fori_loop(0, rows_x, fill_y, 0, unroll=8)
    for copy in loads[first:second]:
        copy.wait()
    ends = [0] + ([chunks - 1] if chunks > 1 else [])
    middle = list(range(1, chunks - 1))
    for up in (True, False):
        pack_x_raw(0, up)
    pack_corners(0, (True, False))
    for c in ends + middle:
        pack_y_raw(0, c)
        for i in range(CH):
            flow_layer(0, c * CH + i)
        pack_y_flow(0, c)
    for up in (True, False):
        pack_x_flow(0, up)
    heard = sum(there.astype(jnp.int32) for there, _ in sides)
    pl.semaphore_wait(barrier, heard)
    send_corners(0, (True, False))
    send_x(0, (0,))
    send_y(0, ends + middle, (0,))

    cell = cell_ref[...]
    bits = depth.bit_length() - 1
    assert depth == 1 << bits
    plane_row = cell >> bits
    cell_z = cell & (depth - 1)
    row = lax.broadcasted_iota(jnp.int32, (rows_x * rows_y, cell.shape[1]), 0)
    row_bits = rows_y.bit_length() - 1
    assert rows_y == 1 << row_bits
    row = (ix * rows_x + (row >> row_bits)) * (ny * rows_y) + iy * rows_y + (row & (rows_y - 1))
    match = row == plane_row
    at_z = (lax.broadcasted_iota(jnp.int32, (depth, cell.shape[1]), 0) == cell_z).astype(jnp.float32)
    for comp in range(6):
        moment = time_step * moment_ref[pl.ds(comp, 1), :]
        value = lax.dot_general(
            jnp.where(match, moment, 0.0),
            at_z,
            (((1,), (1,)), ((), ())),
            precision=lax.Precision.HIGHEST,
            preferred_element_type=jnp.float32,
        )
        inj[comp] = value.reshape(rows_x, rows_y, depth)

    send_x(0, (1,))
    for copy in loads[second:third]:
        copy.wait()
    frictions, cohesions = [], []
    for which in range(coh_ref.shape[0]):
        f = jnp.full((rows_y, depth), fri_ref[which], jnp.float32)
        frictions.append(f)
        cohesions.append(coh_ref[which] * jnp.sqrt(1.0 - f * f))

    def table(x, carry):
        z = jnp.where(elig[x] == 1, zone[x], -1)
        c = jnp.full((rows_y, depth), 1e30, jnp.float32)
        f = jnp.zeros((rows_y, depth), jnp.float32)
        for which in range(coh_ref.shape[0]):
            hit = z == which
            c = jnp.where(hit, cohesions[which], c)
            f = jnp.where(hit, frictions[which], f)
        cc[x] = c
        cf[x] = f
        return carry

    lax.fori_loop(0, rows_x, table, 0, unroll=2)

    for copy in loads[third:]:
        copy.wait()

    rim = [x for x in range(rows_x) if x < 4 or x >= rows_x - 4]
    near = [x for x in range(rows_x) if x not in rim and (x < CH + 2 or x >= rows_x - CH - 2)]
    inner = [x for x in range(rows_x) if x not in rim and x not in near]
    for step in range(STEPS):
        nxt = step + 1
        last = nxt == STEPS
        wait_y(step, ends)
        for c in ends:
            finish_y(step, c)
        wait_corners(step)
        take_corners(step)
        finish_corners_y(step)
        wait_x(step)
        finish_x(step)
        if not last:
            for x in rim:
                stress_layer(step, x)
        flowed = set()
        if not last:
            pack_corners(nxt, (True, False))
            send_corners(nxt, (True, False))
            for x in (0, 1, rows_x - 2, rows_x - 1):
                flow_layer(nxt, x)
                flowed.add(x)
            for up in (True, False):
                pack_x_raw(nxt, up)
                pack_x_flow(nxt, up)
            send_x(nxt, (0,))
        wait_y(step, middle)
        for c in middle:
            finish_y(step, c)
        if not last:
            for x in near:
                stress_layer(step, x)
            for c in ends:
                pack_y_raw(nxt, c)
            send_y(nxt, ends, (0,))
            for c in ends:
                for x in range(c * CH, (c + 1) * CH):
                    if x not in flowed:
                        flow_layer(nxt, x)
                pack_y_flow(nxt, c)
            send_y(nxt, ends, (1,))
            send_x(nxt, (1,))
        if not last:
            for x in inner:
                stress_layer(step, x)
            for c in middle:
                pack_y_raw(nxt, c)
            send_y(nxt, middle, (0,))
            for c in middle:
                for x in range(c * CH, (c + 1) * CH):
                    flow_layer(nxt, x)
                pack_y_flow(nxt, c)
                send_y(nxt, (c,), (1,))

    for step in range(STEPS):
        for up in (True, False):

            @pl.when(to_x(up)[0])
            def _():
                x_copy(step, up).wait_send()

            @pl.when(to_y(up)[0])
            def _():
                for c in range(chunks):
                    for part in y_parts(step):
                        y_copy(step, up, c, part).wait_send()

        for d, (cx, cy) in enumerate(CORNERS):

            @pl.when(to_corner(cx, cy)[0])
            def _():
                d_copy(step, d).wait_send()


def on_device(nx, ny, velocity, stress, lame_first, modulus, buoyancy, zone, eligible, cohesion, friction, source_cell, source_moment):
    rows_x, rows_y, depth = zone.shape
    assert rows_y == 8 and rows_x % CH == 0 and rows_x >= 3 * CH
    chunks = rows_x // CH
    f32 = jnp.float32
    grid = (rows_x, rows_y, depth)
    plane = rows_x * rows_y
    any_spec = pl.BlockSpec(memory_space=pltpu.HBM)
    smem = pl.BlockSpec(memory_space=pltpu.SMEM)
    vmem = pl.BlockSpec(memory_space=pltpu.VMEM)
    dma = pltpu.SemaphoreType.DMA
    fields = [
        pltpu.VMEM((3 * (rows_x + 4) * rows_y, depth), f32),
        pltpu.VMEM((3 * R * (rows_x + 1) + R, depth), f32),
        pltpu.VMEM((plane, depth), f32),
        pltpu.VMEM((3 * (rows_x + 5) * R, depth), f32),
        pltpu.VMEM(grid, f32),
        pltpu.VMEM(grid, f32),
        pltpu.VMEM((6,) + grid, f32),
        pltpu.VMEM(grid, f32),
        pltpu.VMEM(grid, f32),
    ]
    held = pl.pallas_call(
        functools.partial(kernel, nx, ny),
        out_shape=fields,
        in_specs=[any_spec] * 7 + [smem, smem, vmem, vmem],
        out_specs=[vmem] * len(fields),
        scratch_shapes=fields[:4] + [
            pltpu.VMEM((2, plane, depth), f32),
            pltpu.VMEM((3 * plane, depth), f32),
            pltpu.VMEM((plane, depth), f32),
            pltpu.VMEM(grid, jnp.int32),
            pltpu.VMEM(grid, jnp.int32),
            pltpu.VMEM((STEPS, 2, 11, rows_y, depth), f32),
            pltpu.VMEM((STEPS, 2, 11, rows_y, depth), f32),
            pltpu.VMEM((STEPS, 2, chunks, 11 * 8, depth), f32),
            pltpu.VMEM((STEPS, 2, chunks, 11 * 8, depth), f32),
            pltpu.VMEM((STEPS, 4, 16, depth), f32),
            pltpu.VMEM((STEPS, 4, 16, depth), f32),
            pltpu.VMEM((2 * 5 * rows_y, depth), f32),
            pltpu.VMEM((2 * 5 * 2 * 8, depth), f32),
            dma((12,)),
            dma((STEPS, 2)),
            dma((STEPS, 2)),
            dma((STEPS, 2, chunks, 2)),
            dma((STEPS, 2, chunks, 2)),
            dma((STEPS, 4)),
            dma((STEPS, 4)),
        ],
        compiler_params=pltpu.CompilerParams(collective_id=0, has_side_effects=True, vmem_limit_bytes=63_000_000),
    )(
        velocity.reshape(3 * plane, depth), stress.reshape(6 * plane, depth), lame_first, modulus,
        buoyancy.reshape(plane, depth), zone, eligible,
        cohesion, friction, source_cell.reshape(1, -1), source_moment,
    )
    return pl.pallas_call(
        finish_kernel,
        out_shape=(jax.ShapeDtypeStruct((3,) + grid, f32), jax.ShapeDtypeStruct((6,) + grid, f32)),
        in_specs=[vmem] * len(fields),
        out_specs=(any_spec, any_spec),
        scratch_shapes=[pltpu.VMEM((3,) + grid, f32), pltpu.VMEM((6,) + grid, f32), dma((chunks, 2))],
        compiler_params=pltpu.CompilerParams(vmem_limit_bytes=24 * 2**20),
    )(*held)


def solution(mesh):
    field = P(None, "gx", "gy", None)
    cells = P("gx", "gy", None)
    return jax.shard_map(
        functools.partial(on_device, mesh.shape["gx"], mesh.shape["gy"]),
        mesh=mesh,
        in_specs=(field, field, cells, cells, cells, cells, cells, P(), P(), P(), P()),
        out_specs=(field, field),
        check_vma=False,
    )
```

```python
import functools

import jax
import jax.numpy as jnp
from jax import lax
from jax.experimental import pallas as pl
from jax.experimental.pallas import tpu as pltpu
from jax.sharding import PartitionSpec as P

STEPS = 2
time_step = 0.1
shear_floor = 0.25
MESH = pl.DeviceIdType.MESH
CH = 8
R = 16

BACK = {"F": 1, "B": 2}
AHEAD = {"F": 2, "B": 1}
FORCE_X = ((0, "F"), (3, "B"), (4, "B"))
FORCE_Y = ((3, "B"), (1, "F"), (5, "B"))
FLOW_X = ("B", "F", "F")
FLOW_Y = ("F", "B", "F")
SLOT_X = {0: 0, 3: 1, 4: 2}
SLOT_Y = {3: 0, 1: 1, 5: 2}


def edge(kind, up, n):
    return list(range(n - BACK[kind], n)) if up else list(range(AHEAD[kind]))


def spread(kind, up, n, get):
    if up and kind == "B":
        return [(0, get(0) - 27.0 * get(1)), (1, get(1))]
    if up:
        return [(0, get(0))]
    if kind == "B":
        return [(n - 1, -get(0))]
    return [(n - 1, 27.0 * get(0) - get(1)), (n - 2, -get(0))]


def raw_list(force, up, n):
    return [(comp, i) for comp, kind in force for i in edge(kind, up, n)]


def flow_list(flow, up, n):
    return [(slot, i) for slot, kind in enumerate(flow) for i in edge(kind, up, n)]


def corner_list(sx, sy, nx, ny):
    found = []
    for k in range(3):
        comp, kind = FORCE_Y[k]
        found += [(comp, x, y) for x in edge(FLOW_X[k], sx, nx) for y in edge(kind, sy, ny)]
        comp, kind = FORCE_X[k]
        found += [(comp, x, y) for x in edge(kind, sx, nx) for y in edge(FLOW_Y[k], sy, ny)]
    return list(dict.fromkeys(found))


CORNERS = [(False, True), (False, False), (True, True), (True, False)]


class Fields:
    def __init__(self, sx, sy, zb, vb, lam, mod, inj, cc, cf):
        self.sx, self.sy, self.zb, self.vb = sx, sy, zb, vb
        self.lam, self.mod, self.inj, self.cc, self.cf = lam, mod, inj, cc, cf
        self.rows_x, self.rows_y, self.depth = lam.shape
        lane = lax.broadcasted_iota(jnp.int32, (self.rows_y, self.depth), 1)
        self.keep = {1: lane < self.depth - 1, 2: lane < self.depth - 2, -1: lane >= 1, -2: lane >= 2}

    def sx_row(self, comp, x):
        return (SLOT_X[comp] * (self.rows_x + 4) + x + 2) * self.rows_y

    def sy_row(self, comp, x):
        return SLOT_Y[comp] * R * (self.rows_x + 1) + R * (x + 1)

    def vb_row(self, slot, x):
        return (slot * (self.rows_x + 5) + x + 3) * R

    def sx_tile(self, step, comp, x):
        return self.sx[step][pl.ds(self.sx_row(comp, x), self.rows_y), :]

    def own_sy(self, step, comp, x):
        return self.sy[step][pl.ds(self.sy_row(comp, x), self.rows_y), :]

    def own_zb(self, step, x):
        return self.zb[step][pl.ds(x * self.rows_y, self.rows_y), :]

    def own_v(self, step, slot, x):
        return self.vb[step][pl.ds(self.vb_row(slot, x), self.rows_y), :]

    def along_z(self, value, offset):
        if offset == 0:
            return value
        return jnp.where(self.keep[offset], pltpu.roll(value, (-offset) % self.depth, 1), 0.0)

    def derivative(self, get, forward):
        a, b, c, d = (get(1), get(0), get(2), get(-1)) if forward else (get(0), get(-1), get(1), get(-2))
        return 27.0 * (a - b) - (c - d)

    def s_dx(self, step, comp, x, forward):
        return self.derivative(lambda o: self.sx_tile(step, comp, x + o), forward)

    def s_dy(self, step, comp, x, forward):
        row = self.sy_row(comp, x)
        return self.derivative(lambda o: self.sy[step][pl.ds(row + o, self.rows_y), :], forward)

    def v_dx(self, step, slot, x, forward):
        return self.derivative(lambda o: self.own_v(step, slot, x + o), forward)

    def v_dy(self, step, slot, x, forward):
        row = self.vb_row(slot, x)
        return self.derivative(lambda o: self.vb[step][pl.ds(row + o, self.rows_y), :], forward)

    def dz(self, value, forward):
        return self.derivative(lambda o: self.along_z(value, o), forward)

    def forces(self, step, x):
        xz, yz, zz = self.sx_tile(step, 4, x), self.own_sy(step, 5, x), self.own_zb(step, x)
        return (
            self.s_dx(step, 0, x, True) + self.s_dy(step, 3, x, False) + self.dz(xz, False),
            self.s_dx(step, 3, x, False) + self.s_dy(step, 1, x, True) + self.dz(yz, False),
            self.s_dx(step, 4, x, False) + self.s_dy(step, 5, x, False) + self.dz(zz, True),
        )

    def stress(self, step, x):
        vx, vy, vz = (self.own_v(step, slot, x) for slot in range(3))
        ex = self.v_dx(step, 0, x, False)
        ey = self.v_dy(step, 1, x, False)
        ez = self.dz(vz, False)
        xy = self.v_dy(step, 0, x, True) + self.v_dx(step, 1, x, True)
        xz = self.dz(vx, True) + self.v_dx(step, 2, x, True)
        yz = self.dz(vy, True) + self.v_dy(step, 2, x, True)
        weight = time_step / 24.0
        inj = self.inj
        m = weight * self.mod[x]
        grow = weight * self.lam[x] * (ex + ey + ez)
        m2 = m + m
        s0, s3, s4 = (self.sx_tile(step, comp, x) for comp in (0, 3, 4))
        s1, s5 = self.own_sy(step, 1, x), self.own_sy(step, 5, x)
        s2 = self.own_zb(step, x)
        s0 = s0 + (grow + m2 * ex) + inj[0, x]
        s1 = s1 + (grow + m2 * ey) + inj[1, x]
        s2 = s2 + (grow + m2 * ez) + inj[2, x]
        s3 = s3 + m * xy + inj[3, x]
        s4 = s4 + m * xz + inj[4, x]
        s5 = s5 + m * yz + inj[5, x]
        pressure = (s0 + s1 + s2) * (1.0 / 3.0)
        d0, d1, d2 = s0 - pressure, s1 - pressure, s2 - pressure
        second = 0.5 * (d0 * d0 + d1 * d1 + d2 * d2) + (s3 * s3 + s4 * s4 + s5 * s5)
        strength = jnp.maximum(self.cc[x] - pressure * self.cf[x], 0.0)
        factor = jnp.minimum(1.0, strength * lax.rsqrt(jnp.maximum(second, shear_floor * shear_floor)))
        s0, s1, s2 = pressure + factor * d0, pressure + factor * d1, pressure + factor * d2
        return s0, s1, s2, factor * s3, factor * s4, factor * s5


def finish_kernel(sx, sy, zb, vb, lam, mod, inj, cc, cf, vout_hbm, sout_hbm, vout, sout, sem):
    at = Fields((None, sx), (None, sy), (None, zb), (None, vb), lam, mod, inj, cc, cf)
    copies = []
    for c in range(at.rows_x // CH):
        for x in range(c * CH, (c + 1) * CH):
            for slot in range(3):
                vout[slot, x] = at.own_v(STEPS - 1, slot, x)
            for comp, value in enumerate(at.stress(STEPS - 1, x)):
                sout[comp, x] = value
        for i, (src, dst) in enumerate(((vout, vout_hbm), (sout, sout_hbm))):
            layers = pl.ds(c * CH, CH)
            copy = pltpu.make_async_copy(src.at[:, layers], dst.at[:, layers], sem.at[c, i])
            copy.start()
            copies.append(copy)
    for copy in copies:
        copy.wait()


def kernel(
    nx,
    ny,
    vel_hbm, str_hbm, lam_hbm, mod_hbm, buo_hbm, zone_hbm, elig_hbm,
    coh_hbm, fri_hbm, cell_hbm, moment_hbm,
    sx1, sy1, zb1, vb1, lam, mod, inj, cc, cf,
    sx0, sy0, zb0, vb0, stage, vel, buo, zone, elig,
    xs, rx, ys, ry, ds, rd, xf, yf, coh_ref, fri_ref, cell_ref, moment_ref,
    load_sem, xsend, xrecv, ysend, yrecv, dsend, drecv,
):
    rows_x = lam.shape[0]
    rows_y = lam.shape[1]
    depth = lam.shape[2]
    chunks = rows_x // CH
    sx, sy, zb, vb = (sx0, sx1), (sy0, sy1), (zb0, zb1), (vb0, vb1)
    at = Fields(sx, sy, zb, vb, lam, mod, inj, cc, cf)
    sx_row, sy_row, vb_row, sx_tile = at.sx_row, at.sy_row, at.vb_row, at.sx_tile
    ix = lax.axis_index("gx")
    iy = lax.axis_index("gy")
    x_lo, x_hi, y_lo, y_hi = ix > 0, ix < nx - 1, iy > 0, iy < ny - 1

    def to_x(up):
        return (x_hi, (ix + 1, iy)) if up else (x_lo, (ix - 1, iy))

    def to_y(up):
        return (y_hi, (ix, iy + 1)) if up else (y_lo, (ix, iy - 1))

    def to_corner(cx, cy):
        there = jnp.logical_and(to_x(cx)[0], to_y(cy)[0])
        return there, (to_x(cx)[1][0], to_y(cy)[1][1])

    sides = [to_x(True), to_x(False), to_y(True), to_y(False)] + [to_corner(*c) for c in CORNERS]
    barrier = pltpu.get_barrier_semaphore()
    for there, target in sides:

        @pl.when(there)
        def _():
            pl.semaphore_signal(barrier, inc=1, device_id=target, device_id_type=MESH)

    raw_x = {up: raw_list(FORCE_X, up, rows_x) for up in (True, False)}
    raw_y = {up: raw_list(FORCE_Y, up, rows_y) for up in (True, False)}
    flow_x = {up: flow_list(FLOW_X, up, rows_x) for up in (True, False)}
    flow_y = {up: flow_list(FLOW_Y, up, rows_y) for up in (True, False)}
    buo_x = {True: [rows_x - 2, rows_x - 1], False: [0, 1]}
    buo_y = {True: [rows_y - 2, rows_y - 1], False: [0, 1]}
    corner = {c: corner_list(c[0], c[1], rows_x, rows_y) for c in CORNERS}

    loads = []

    def load(src, dst):
        copy = pltpu.make_async_copy(src, dst, load_sem.at[len(loads)])
        copy.start()
        loads.append(copy)

    plane = rows_x * rows_y
    load(str_hbm.at[pl.ds(3 * plane, plane)], sx0.at[pl.ds(sx_row(3, 0), plane)])
    load(str_hbm.at[pl.ds(1 * plane, plane)], stage.at[0])
    load(str_hbm.at[pl.ds(5 * plane, plane)], stage.at[1])
    load(buo_hbm, buo)
    load(str_hbm.at[pl.ds(0 * plane, plane)], sx0.at[pl.ds(sx_row(0, 0), plane)])
    load(str_hbm.at[pl.ds(4 * plane, plane)], sx0.at[pl.ds(sx_row(4, 0), plane)])
    first = len(loads)
    load(str_hbm.at[pl.ds(2 * plane, plane)], zb0)
    load(vel_hbm, vel)
    second = len(loads)
    load(cell_hbm, cell_ref)
    load(moment_hbm, moment_ref)
    sources = len(loads)
    load(coh_hbm, coh_ref)
    load(fri_hbm, fri_ref)
    load(zone_hbm, zone)
    load(elig_hbm, elig)
    third = len(loads)
    load(lam_hbm, lam)
    load(mod_hbm, mod)

    tile = jnp.zeros((rows_y, depth), jnp.float32)

    for step in range(STEPS):
        for comp in SLOT_X:
            for layer in (-2, -1, rows_x, rows_x + 1):
                sx[step][pl.ds(sx_row(comp, layer), rows_y), :] = tile
    for ref in (xf, yf):
        for i in range(ref.shape[0] // rows_y):
            ref[pl.ds(i * rows_y, rows_y), :] = tile

    def clear(i, carry):
        for ref in sy:
            ref[pl.ds(pl.multiple_of(i * R + rows_y, 8), R - rows_y), :] = jnp.zeros((R - rows_y, depth), jnp.float32)
        return carry

    lax.fori_loop(0, sy0.shape[0] // R, clear, 0, unroll=4)

    for up in (True, False):

        @pl.when(jnp.logical_not(to_x(not up)[0]))
        def _():
            for step in range(STEPS):
                for i in range(rx.shape[2]):
                    rx[step, int(up), i] = tile

        @pl.when(jnp.logical_not(to_y(not up)[0]))
        def _():
            for step in range(STEPS):

                def wipe(c, carry):
                    for i in range(ry.shape[3] // 8):
                        ry[step, int(up), c, pl.ds(i * 8, 8), :] = tile
                    return carry

                lax.fori_loop(0, chunks, wipe, 0)

    for d, (cx, cy) in enumerate(CORNERS):

        @pl.when(jnp.logical_not(to_corner(not cx, not cy)[0]))
        def _():
            for step in range(STEPS):
                for i in range(rd.shape[2] // 8):
                    rd[step, d, pl.ds(i * 8, 8), :] = tile

    def x_copy(step, up):
        count = len(raw_x[up]) + len(flow_x[up]) + (2 if step == 0 else 0)
        return pltpu.make_async_remote_copy(
            src_ref=xs.at[step, int(up), pl.ds(0, count)],
            dst_ref=rx.at[step, int(up), pl.ds(0, count)],
            send_sem=xsend.at[step, int(up)],
            recv_sem=xrecv.at[step, int(up)],
            device_id=to_x(up)[1],
            device_id_type=MESH,
        )

    def y_parts(step):
        return (0,) if step == 0 else (0, 1)

    def y_copy(step, up, c, part):
        raw, flow = len(raw_y[up]), len(flow_y[up])
        start, count = (0, raw + flow + 2) if step == 0 else ((0, raw), (raw, flow))[part]
        return pltpu.make_async_remote_copy(
            src_ref=ys.at[step, int(up), c, pl.ds(start * 8, count * 8)],
            dst_ref=ry.at[step, int(up), c, pl.ds(start * 8, count * 8)],
            send_sem=ysend.at[step, int(up), c, part],
            recv_sem=yrecv.at[step, int(up), c, part],
            device_id=to_y(up)[1],
            device_id_type=MESH,
        )

    def d_copy(step, d):
        return pltpu.make_async_remote_copy(
            src_ref=ds.at[step, d, pl.ds(0, len(corner[CORNERS[d]]))],
            dst_ref=rd.at[step, d, pl.ds(0, len(corner[CORNERS[d]]))],
            send_sem=dsend.at[step, d],
            recv_sem=drecv.at[step, d],
            device_id=to_corner(*CORNERS[d])[1],
            device_id_type=MESH,
        )

    def sy_pack(step, comp, c, row):
        return sy[step][pl.ds(sy_row(comp, c * CH) + row, CH, stride=R), :]

    def vb_pack(slot, c, row):
        return pl.ds(vb_row(slot, c * CH) + row, CH, stride=R)

    def pack_x_raw(step, up):
        for i, (comp, x) in enumerate(raw_x[up]):
            xs[step, int(up), i] = sx_tile(step, comp, x)
        if step == 0:
            for i, x in enumerate(buo_x[up]):
                xs[step, int(up), len(raw_x[up]) + len(flow_x[up]) + i] = buo[pl.ds(x * rows_y, rows_y), :]

    def pack_y_raw(step, c):
        for up in (True, False):
            for i, (comp, row) in enumerate(raw_y[up]):
                ys[step, int(up), c, pl.ds(i * 8, 8), :] = sy_pack(step, comp, c, row)
            if step == 0:
                for i, row in enumerate(buo_y[up]):
                    value = buo[pl.ds(c * CH * rows_y + row, CH, stride=rows_y), :]
                    ys[step, int(up), c, pl.ds((len(raw_y[up]) + len(flow_y[up]) + i) * 8, 8), :] = value

    def pack_x_flow(step, up):
        for i, (slot, x) in enumerate(flow_x[up]):
            xs[step, int(up), len(raw_x[up]) + i] = vb[step][pl.ds(vb_row(slot, x), rows_y), :]

    def pack_y_flow(step, c):
        for up in (True, False):
            for i, (slot, row) in enumerate(flow_y[up]):
                ys[step, int(up), c, pl.ds((len(raw_y[up]) + i) * 8, 8), :] = vb[step][vb_pack(slot, c, row), :]

    def pack_corners(step, cxs):
        for d, (cx, cy) in enumerate(CORNERS):
            if cx in cxs:
                for i, (comp, x, y) in enumerate(corner[(cx, cy)]):
                    if comp in SLOT_X:
                        value = sx[step][pl.ds(sx_row(comp, x) + y, 1), :]
                    else:
                        value = sy[step][pl.ds(sy_row(comp, x) + y, 1), :]
                    ds[step, d, pl.ds(i, 1), :] = value

    def send_x(step, cores):
        mine = iy % 2 == cores[0]
        for up in (False, True):

            @pl.when(to_x(up)[0] if len(cores) == 2 else jnp.logical_and(to_x(up)[0], mine))
            def _():
                x_copy(step, up).start()

    def send_y(step, cs, parts):
        for up in (True, False):

            @pl.when(to_y(up)[0])
            def _():
                for c in cs:
                    for part in parts:
                        y_copy(step, up, c, part).start()

    def send_corners(step, cxs):
        for d, (cx, cy) in enumerate(CORNERS):
            if cx in cxs:

                @pl.when(to_corner(cx, cy)[0])
                def _():
                    d_copy(step, d).start()

    weight = time_step / 24.0

    def flow_layer(step, x):
        scale = weight * of_cell(buo, x)
        for slot, force in enumerate(at.forces(step, x)):
            old = vel[pl.ds((slot * rows_x + x) * rows_y, rows_y), :] if step == 0 else at.own_v(step - 1, slot, x)
            vb[step][pl.ds(vb_row(slot, x), rows_y), :] = old + scale * force

    def stress_layer(step, x):
        s = at.stress(step, x)
        for comp in SLOT_X:
            sx[step + 1][pl.ds(sx_row(comp, x), rows_y), :] = s[comp]
        for comp in SLOT_Y:
            sy[step + 1][pl.ds(sy_row(comp, x), rows_y), :] = s[comp]
        zb[step + 1][pl.ds(x * rows_y, rows_y), :] = s[2]

    def of_cell(ref, x):
        return ref[pl.ds(x * rows_y, rows_y), :]

    def wait_x(step):
        for up in (True, False):

            @pl.when(to_x(not up)[0])
            def _():
                x_copy(step, up).wait_recv()

    def wait_y(step, cs):
        for up in (True, False):

            @pl.when(to_y(not up)[0])
            def _():
                for c in cs:
                    for part in y_parts(step):
                        y_copy(step, up, c, part).wait_recv()

    def wait_corners(step):
        for d, (cx, cy) in enumerate(CORNERS):

            @pl.when(to_corner(not cx, not cy)[0])
            def _():
                d_copy(step, d).wait_recv()

    def place(items, what):
        return [i for i, item in enumerate(items) if item == what][0]

    def take_corners(step):
        for d, (cx, cy) in enumerate(CORNERS):

            def raw(comp, x, y):
                return rd[step, d, pl.ds(place(corner[(cx, cy)], (comp, x, y)), 1), :]

            for k in range(3):
                comp, kind = FORCE_Y[k]
                ys_ = edge(kind, cy, rows_y)
                for x in edge(FLOW_X[k], cx, rows_x):
                    base = (int(cx) * 5 + place(flow_x[cx], (k, x))) * rows_y
                    for row, value in spread(kind, cy, rows_y, lambda i: raw(comp, x, ys_[i])):
                        xf[pl.ds(base + row, 1), :] = value
                comp, kind = FORCE_X[k]
                xs_ = edge(kind, cx, rows_x)
                for y in edge(FLOW_Y[k], cy, rows_y):
                    base = ((int(cy) * 5 + place(flow_y[cy], (k, y))) * 2 + int(cx)) * 8
                    for layer, value in spread(kind, cx, CH, lambda i: raw(comp, xs_[i], y)):
                        yf[pl.ds(base + layer, 1), :] = value

    def finish_x(step):
        for up in (True, False):
            side = int(up)
            for k, (comp, kind) in enumerate(FORCE_X):
                places = [place(raw_x[up], (comp, x)) for x in edge(kind, up, rows_x)]
                for x, value in spread(kind, up, rows_x, lambda i: rx[step, side, places[i]]):
                    where = pl.ds(vb_row(k, x), rows_y)
                    vb[step][where, :] = vb[step][where, :] + weight * of_cell(buo, x) * value
            for k, (comp, kind) in enumerate(FORCE_X):
                mine = edge(kind, not up, rows_x)
                adds = dict(spread(kind, not up, rows_x, lambda i: sx_tile(step, comp, mine[i])))
                for x in edge(FLOW_X[k], up, rows_x):
                    i = place(flow_x[up], (k, x))
                    add = adds[x] + xf[pl.ds((side * 5 + i) * rows_y, rows_y), :]
                    scale = weight * rx[0, side, len(raw_x[up]) + len(flow_x[up]) + place(buo_x[up], x)]
                    new = rx[step, side, len(raw_x[up]) + i] + scale * add
                    halo = x - rows_x if up else x + rows_x
                    vb[step][pl.ds(vb_row(k, halo), rows_y), :] = new

    def buo_halo_y(up, c, y):
        i = len(raw_y[up]) + len(flow_y[up]) + place(buo_y[up], y)
        return ry[0, int(up), c, pl.ds(i * 8, 8), :]

    def finish_y(step, c):
        for up in (True, False):
            side = int(up)

            def got(i):
                return ry[step, side, c, pl.ds(i * 8, 8), :]

            for k, (comp, kind) in enumerate(FORCE_Y):
                places = [place(raw_y[up], (comp, y)) for y in edge(kind, up, rows_y)]
                for y, value in spread(kind, up, rows_y, lambda i: got(places[i])):
                    where = vb_pack(k, c, y)
                    scale = weight * buo[pl.ds(c * CH * rows_y + y, CH, stride=rows_y), :]
                    vb[step][where, :] = vb[step][where, :] + scale * value
            for k, (comp, kind) in enumerate(FORCE_Y):
                mine = edge(kind, not up, rows_y)
                adds = dict(spread(kind, not up, rows_y, lambda i: sy_pack(step, comp, c, mine[i])))
                for y in edge(FLOW_Y[k], up, rows_y):
                    i = place(flow_y[up], (k, y))
                    scale = weight * buo_halo_y(up, c, y)
                    new = got(len(raw_y[up]) + i) + scale * adds[y]
                    halo = y - rows_y if up else y + rows_y
                    vb[step][vb_pack(k, c, halo), :] = new

    def finish_corners_y(step):
        for up in (True, False):
            for i, (k, y) in enumerate(flow_y[up]):
                halo = y - rows_y if up else y + rows_y
                for end, c in ((1, 0), (0, chunks - 1)):
                    add = yf[pl.ds(((int(up) * 5 + i) * 2 + end) * 8, 8), :]
                    where = vb_pack(k, c, halo)
                    vb[step][where, :] = vb[step][where, :] + weight * buo_halo_y(up, c, y) * add

    for copy in loads[:first]:
        copy.wait()

    def fill_y(i, carry):
        first_row = pl.multiple_of(i * rows_y, 8)
        for comp, value in (
            (3, sx0[pl.ds(sx_row(3, 0) + first_row, rows_y), :]),
            (1, stage[0, pl.ds(first_row, rows_y), :]),
            (5, stage[1, pl.ds(first_row, rows_y), :]),
        ):
            sy0[pl.ds(pl.multiple_of(sy_row(comp, 0) + i * R, 8), rows_y), :] = value
        return carry

    lax.fori_loop(0, rows_x, fill_y, 0, unroll=8)
    for copy in loads[first:second]:
        copy.wait()
    ends = [0] + ([chunks - 1] if chunks > 1 else [])
    middle = list(range(1, chunks - 1))
    for up in (True, False):
        pack_x_raw(0, up)
    pack_corners(0, (True, False))

    def flow_chunk(c):
        pack_y_raw(0, c)
        for i in range(CH):
            flow_layer(0, c * CH + i)
        pack_y_flow(0, c)

    for c in ends:
        flow_chunk(c)
    for up in (True, False):
        pack_x_flow(0, up)
    heard = sum(there.astype(jnp.int32) for there, _ in sides)
    pl.semaphore_wait(barrier, heard)
    send_corners(0, (True, False))
    send_x(0, (0,))
    send_y(0, ends, (0,))
    for c in middle:
        flow_chunk(c)
        send_y(0, (c,), (0,))

    for copy in loads[second:sources]:
        copy.wait()
    cell = cell_ref[...]
    bits = depth.bit_length() - 1
    assert depth == 1 << bits
    plane_row = cell >> bits
    cell_z = cell & (depth - 1)
    row = lax.broadcasted_iota(jnp.int32, (rows_x * rows_y, cell.shape[1]), 0)
    row_bits = rows_y.bit_length() - 1
    assert rows_y == 1 << row_bits
    row = (ix * rows_x + (row >> row_bits)) * (ny * rows_y) + iy * rows_y + (row & (rows_y - 1))
    match = row == plane_row
    at_z = (lax.broadcasted_iota(jnp.int32, (depth, cell.shape[1]), 0) == cell_z).astype(jnp.float32)
    for comp in range(6):
        moment = time_step * moment_ref[pl.ds(comp, 1), :]
        value = lax.dot_general(
            jnp.where(match, moment, 0.0),
            at_z,
            (((1,), (1,)), ((), ())),
            precision=lax.Precision.HIGHEST,
            preferred_element_type=jnp.float32,
        )
        inj[comp] = value.reshape(rows_x, rows_y, depth)

    send_x(0, (1,))
    for copy in loads[sources:third]:
        copy.wait()
    frictions, cohesions = [], []
    for which in range(coh_ref.shape[0]):
        f = jnp.full((rows_y, depth), fri_ref[which], jnp.float32)
        frictions.append(f)
        cohesions.append(coh_ref[which] * jnp.sqrt(1.0 - f * f))

    def table(x, carry):
        z = jnp.where(elig[x] == 1, zone[x], -1)
        c = jnp.full((rows_y, depth), 1e30, jnp.float32)
        f = jnp.zeros((rows_y, depth), jnp.float32)
        for which in range(coh_ref.shape[0]):
            hit = z == which
            c = jnp.where(hit, cohesions[which], c)
            f = jnp.where(hit, frictions[which], f)
        cc[x] = c
        cf[x] = f
        return carry

    lax.fori_loop(0, rows_x, table, 0, unroll=2)

    for copy in loads[third:]:
        copy.wait()

    rim = [x for x in range(rows_x) if x < 4 or x >= rows_x - 4]
    near = [x for x in range(rows_x) if x not in rim and (x < CH + 2 or x >= rows_x - CH - 2)]
    inner = [x for x in range(rows_x) if x not in rim and x not in near]
    for step in range(STEPS):
        nxt = step + 1
        last = nxt == STEPS
        wait_y(step, ends)
        for c in ends:
            finish_y(step, c)
        wait_corners(step)
        take_corners(step)
        finish_corners_y(step)
        wait_x(step)
        finish_x(step)
        if not last:
            for x in rim:
                stress_layer(step, x)
        flowed = set()
        if not last:
            pack_corners(nxt, (True, False))
            send_corners(nxt, (True, False))
            for x in (0, 1, rows_x - 2, rows_x - 1):
                flow_layer(nxt, x)
                flowed.add(x)
            for up in (True, False):
                pack_x_raw(nxt, up)
                pack_x_flow(nxt, up)
            send_x(nxt, (0,))
        wait_y(step, middle)
        for c in middle:
            finish_y(step, c)
        if not last:
            for x in near:
                stress_layer(step, x)
            for c in ends:
                pack_y_raw(nxt, c)
            send_y(nxt, ends, (0,))
            for c in ends:
                for x in range(c * CH, (c + 1) * CH):
                    if x not in flowed:
                        flow_layer(nxt, x)
                pack_y_flow(nxt, c)
            send_y(nxt, ends, (1,))
            send_x(nxt, (1,))
        if not last:
            for x in inner:
                stress_layer(step, x)
            for c in middle:
                pack_y_raw(nxt, c)
            send_y(nxt, middle, (0,))
            for c in middle:
                for x in range(c * CH, (c + 1) * CH):
                    flow_layer(nxt, x)
                pack_y_flow(nxt, c)
                send_y(nxt, (c,), (1,))

    for step in range(STEPS):
        for up in (True, False):

            @pl.when(to_x(up)[0])
            def _():
                x_copy(step, up).wait_send()

            @pl.when(to_y(up)[0])
            def _():
                for c in range(chunks):
                    for part in y_parts(step):
                        y_copy(step, up, c, part).wait_send()

        for d, (cx, cy) in enumerate(CORNERS):

            @pl.when(to_corner(cx, cy)[0])
            def _():
                d_copy(step, d).wait_send()


def on_device(nx, ny, velocity, stress, lame_first, modulus, buoyancy, zone, eligible, cohesion, friction, source_cell, source_moment):
    rows_x, rows_y, depth = zone.shape
    assert rows_y == 8 and rows_x % CH == 0 and rows_x >= 3 * CH
    chunks = rows_x // CH
    f32 = jnp.float32
    grid = (rows_x, rows_y, depth)
    plane = rows_x * rows_y
    any_spec = pl.BlockSpec(memory_space=pltpu.HBM)
    vmem = pl.BlockSpec(memory_space=pltpu.VMEM)
    dma = pltpu.SemaphoreType.DMA
    fields = [
        pltpu.VMEM((3 * (rows_x + 4) * rows_y, depth), f32),
        pltpu.VMEM((3 * R * (rows_x + 1) + R, depth), f32),
        pltpu.VMEM((plane, depth), f32),
        pltpu.VMEM((3 * (rows_x + 5) * R, depth), f32),
        pltpu.VMEM(grid, f32),
        pltpu.VMEM(grid, f32),
        pltpu.VMEM((6,) + grid, f32),
        pltpu.VMEM(grid, f32),
        pltpu.VMEM(grid, f32),
    ]
    held = pl.pallas_call(
        functools.partial(kernel, nx, ny),
        out_shape=fields,
        in_specs=[any_spec] * 11,
        out_specs=[vmem] * len(fields),
        scratch_shapes=fields[:4] + [
            pltpu.VMEM((2, plane, depth), f32),
            pltpu.VMEM((3 * plane, depth), f32),
            pltpu.VMEM((plane, depth), f32),
            pltpu.VMEM(grid, jnp.int32),
            pltpu.VMEM(grid, jnp.int32),
            pltpu.VMEM((STEPS, 2, 11, rows_y, depth), f32),
            pltpu.VMEM((STEPS, 2, 11, rows_y, depth), f32),
            pltpu.VMEM((STEPS, 2, chunks, 11 * 8, depth), f32),
            pltpu.VMEM((STEPS, 2, chunks, 11 * 8, depth), f32),
            pltpu.VMEM((STEPS, 4, 16, depth), f32),
            pltpu.VMEM((STEPS, 4, 16, depth), f32),
            pltpu.VMEM((2 * 5 * rows_y, depth), f32),
            pltpu.VMEM((2 * 5 * 2 * 8, depth), f32),
            pltpu.SMEM(cohesion.shape, f32),
            pltpu.SMEM(friction.shape, f32),
            pltpu.VMEM((1,) + source_cell.shape, jnp.int32),
            pltpu.VMEM(source_moment.shape, f32),
            dma((16,)),
            dma((STEPS, 2)),
            dma((STEPS, 2)),
            dma((STEPS, 2, chunks, 2)),
            dma((STEPS, 2, chunks, 2)),
            dma((STEPS, 4)),
            dma((STEPS, 4)),
        ],
        compiler_params=pltpu.CompilerParams(collective_id=0, has_side_effects=True, vmem_limit_bytes=63_000_000),
    )(
        velocity.reshape(3 * plane, depth), stress.reshape(6 * plane, depth), lame_first, modulus,
        buoyancy.reshape(plane, depth), zone, eligible,
        cohesion, friction, source_cell.reshape(1, -1), source_moment,
    )
    return pl.pallas_call(
        finish_kernel,
        out_shape=(jax.ShapeDtypeStruct((3,) + grid, f32), jax.ShapeDtypeStruct((6,) + grid, f32)),
        in_specs=[vmem] * len(fields),
        out_specs=(any_spec, any_spec),
        scratch_shapes=[pltpu.VMEM((3,) + grid, f32), pltpu.VMEM((6,) + grid, f32), dma((chunks, 2))],
        compiler_params=pltpu.CompilerParams(vmem_limit_bytes=24 * 2**20),
    )(*held)


def solution(mesh):
    field = P(None, "gx", "gy", None)
    cells = P("gx", "gy", None)
    return jax.shard_map(
        functools.partial(on_device, mesh.shape["gx"], mesh.shape["gy"]),
        mesh=mesh,
        in_specs=(field, field, cells, cells, cells, cells, cells, P(), P(), P(), P()),
        out_specs=(field, field),
        check_vma=False,
    )
```

```python
import functools

import jax
import jax.numpy as jnp
from jax import lax
from jax.experimental import pallas as pl
from jax.experimental.pallas import tpu as pltpu
from jax.sharding import PartitionSpec as P

STEPS = 2
time_step = 0.1
shear_floor = 0.25
MESH = pl.DeviceIdType.MESH
CH = 8
R = 16

BACK = {"F": 1, "B": 2}
AHEAD = {"F": 2, "B": 1}
FORCE_X = ((0, "F"), (3, "B"), (4, "B"))
FORCE_Y = ((3, "B"), (1, "F"), (5, "B"))
FLOW_X = ("B", "F", "F")
FLOW_Y = ("F", "B", "F")
SLOT_X = {0: 0, 3: 1, 4: 2}
SLOT_Y = {3: 0, 1: 1, 5: 2}


def edge(kind, up, n):
    return list(range(n - BACK[kind], n)) if up else list(range(AHEAD[kind]))


def spread(kind, up, n, get):
    if up and kind == "B":
        return [(0, get(0) - 27.0 * get(1)), (1, get(1))]
    if up:
        return [(0, get(0))]
    if kind == "B":
        return [(n - 1, -get(0))]
    return [(n - 1, 27.0 * get(0) - get(1)), (n - 2, -get(0))]


def raw_list(force, up, n):
    return [(comp, i) for comp, kind in force for i in edge(kind, up, n)]


def flow_list(flow, up, n):
    return [(slot, i) for slot, kind in enumerate(flow) for i in edge(kind, up, n)]


def corner_list(sx, sy, nx, ny):
    found = []
    for k in range(3):
        comp, kind = FORCE_Y[k]
        found += [(comp, x, y) for x in edge(FLOW_X[k], sx, nx) for y in edge(kind, sy, ny)]
        comp, kind = FORCE_X[k]
        found += [(comp, x, y) for x in edge(kind, sx, nx) for y in edge(FLOW_Y[k], sy, ny)]
    return list(dict.fromkeys(found))


CORNERS = [(False, True), (False, False), (True, True), (True, False)]


class Fields:
    def __init__(self, sx, sy, zb, vb, lam, mod, inj, cc, cf):
        self.sx, self.sy, self.zb, self.vb = sx, sy, zb, vb
        self.lam, self.mod, self.inj, self.cc, self.cf = lam, mod, inj, cc, cf
        self.rows_x, self.rows_y, self.depth = lam.shape
        lane = lax.broadcasted_iota(jnp.int32, (self.rows_y, self.depth), 1)
        self.keep = {1: lane < self.depth - 1, 2: lane < self.depth - 2, -1: lane >= 1, -2: lane >= 2}

    def sx_row(self, comp, x):
        return (SLOT_X[comp] * (self.rows_x + 4) + x + 2) * self.rows_y

    def sy_row(self, comp, x):
        return SLOT_Y[comp] * R * (self.rows_x + 1) + R * (x + 1)

    def vb_row(self, slot, x):
        return (slot * (self.rows_x + 5) + x + 3) * R

    def sx_tile(self, step, comp, x):
        return self.sx[step][pl.ds(self.sx_row(comp, x), self.rows_y), :]

    def own_sy(self, step, comp, x):
        return self.sy[step][pl.ds(self.sy_row(comp, x), self.rows_y), :]

    def own_zb(self, step, x):
        return self.zb[step][pl.ds(x * self.rows_y, self.rows_y), :]

    def own_v(self, step, slot, x):
        return self.vb[step][pl.ds(self.vb_row(slot, x), self.rows_y), :]

    def along_z(self, value, offset):
        if offset == 0:
            return value
        return jnp.where(self.keep[offset], pltpu.roll(value, (-offset) % self.depth, 1), 0.0)

    def derivative(self, get, forward):
        a, b, c, d = (get(1), get(0), get(2), get(-1)) if forward else (get(0), get(-1), get(1), get(-2))
        return 27.0 * (a - b) - (c - d)

    def s_dx(self, step, comp, x, forward):
        return self.derivative(lambda o: self.sx_tile(step, comp, x + o), forward)

    def s_dy(self, step, comp, x, forward):
        row = self.sy_row(comp, x)
        return self.derivative(lambda o: self.sy[step][pl.ds(row + o, self.rows_y), :], forward)

    def v_dx(self, step, slot, x, forward):
        return self.derivative(lambda o: self.own_v(step, slot, x + o), forward)

    def v_dy(self, step, slot, x, forward):
        row = self.vb_row(slot, x)
        return self.derivative(lambda o: self.vb[step][pl.ds(row + o, self.rows_y), :], forward)

    def dz(self, value, forward):
        return self.derivative(lambda o: self.along_z(value, o), forward)

    def forces(self, step, x):
        xz, yz, zz = self.sx_tile(step, 4, x), self.own_sy(step, 5, x), self.own_zb(step, x)
        return (
            self.s_dx(step, 0, x, True) + self.s_dy(step, 3, x, False) + self.dz(xz, False),
            self.s_dx(step, 3, x, False) + self.s_dy(step, 1, x, True) + self.dz(yz, False),
            self.s_dx(step, 4, x, False) + self.s_dy(step, 5, x, False) + self.dz(zz, True),
        )

    def stress(self, step, x):
        vx, vy, vz = (self.own_v(step, slot, x) for slot in range(3))
        ex = self.v_dx(step, 0, x, False)
        ey = self.v_dy(step, 1, x, False)
        ez = self.dz(vz, False)
        xy = self.v_dy(step, 0, x, True) + self.v_dx(step, 1, x, True)
        xz = self.dz(vx, True) + self.v_dx(step, 2, x, True)
        yz = self.dz(vy, True) + self.v_dy(step, 2, x, True)
        weight = time_step / 24.0
        inj = self.inj
        m = weight * self.mod[x]
        grow = weight * self.lam[x] * (ex + ey + ez)
        m2 = m + m
        s0, s3, s4 = (self.sx_tile(step, comp, x) for comp in (0, 3, 4))
        s1, s5 = self.own_sy(step, 1, x), self.own_sy(step, 5, x)
        s2 = self.own_zb(step, x)
        s0 = s0 + (grow + m2 * ex) + inj[0, x]
        s1 = s1 + (grow + m2 * ey) + inj[1, x]
        s2 = s2 + (grow + m2 * ez) + inj[2, x]
        s3 = s3 + m * xy + inj[3, x]
        s4 = s4 + m * xz + inj[4, x]
        s5 = s5 + m * yz + inj[5, x]
        pressure = (s0 + s1 + s2) * (1.0 / 3.0)
        d0, d1, d2 = s0 - pressure, s1 - pressure, s2 - pressure
        second = 0.5 * (d0 * d0 + d1 * d1 + d2 * d2) + (s3 * s3 + s4 * s4 + s5 * s5)
        strength = jnp.maximum(self.cc[x] - pressure * self.cf[x], 0.0)
        factor = jnp.minimum(1.0, strength * lax.rsqrt(jnp.maximum(second, shear_floor * shear_floor)))
        s0, s1, s2 = pressure + factor * d0, pressure + factor * d1, pressure + factor * d2
        return s0, s1, s2, factor * s3, factor * s4, factor * s5


def rim_of(rows_x):
    return [*range(4), *range(rows_x - 4, rows_x)]


def finish_kernel(sx, sy, zb, vb, lam, mod, inj, cc, cf, edge_out, vout_hbm, sout_hbm, vout, sout, sem):
    at = Fields((None, sx), (None, sy), (None, zb), (None, vb), lam, mod, inj, cc, cf)
    copies = []

    def put(src, dst):
        copy = pltpu.make_async_copy(src, dst, sem.at[len(copies)])
        copy.start()
        copies.append(copy)

    for i, x in ((0, 0), (4, at.rows_x - 4)):
        put(edge_out.at[:, pl.ds(i, 4)], sout_hbm.at[:, pl.ds(x, 4)])
    for start in range(4, at.rows_x - 4, CH):
        stop = min(start + CH, at.rows_x - 4)
        low, high = (0 if start == 4 else start), (at.rows_x if stop == at.rows_x - 4 else stop)
        for x in range(low, high):
            for slot in range(3):
                vout[slot, x] = at.own_v(STEPS - 1, slot, x)
        put(vout.at[:, pl.ds(low, high - low)], vout_hbm.at[:, pl.ds(low, high - low)])
        for x in range(start, stop):
            for comp, value in enumerate(at.stress(STEPS - 1, x)):
                sout[comp, x] = value
        put(sout.at[:, pl.ds(start, stop - start)], sout_hbm.at[:, pl.ds(start, stop - start)])
    for copy in copies:
        copy.wait()


def kernel(
    nx,
    ny,
    vel_hbm, str_hbm, lam_hbm, mod_hbm, buo_hbm, zone_hbm, elig_hbm,
    coh_hbm, fri_hbm, cell_hbm, moment_hbm,
    sx1, sy1, zb1, vb1, lam, mod, inj, cc, cf, edge_out,
    sx0, sy0, zb0, vb0, stage, vel, buo, zone, elig,
    xs, rx, ys, ry, ds, rd, xf, yf, coh_ref, fri_ref, cell_ref, moment_ref,
    load_sem, xsend, xrecv, ysend, yrecv, dsend, drecv,
):
    rows_x = lam.shape[0]
    rows_y = lam.shape[1]
    depth = lam.shape[2]
    chunks = rows_x // CH
    sx, sy, zb, vb = (sx0, sx1), (sy0, sy1), (zb0, zb1), (vb0, vb1)
    at = Fields(sx, sy, zb, vb, lam, mod, inj, cc, cf)
    sx_row, sy_row, vb_row, sx_tile = at.sx_row, at.sy_row, at.vb_row, at.sx_tile
    ix = lax.axis_index("gx")
    iy = lax.axis_index("gy")
    x_lo, x_hi, y_lo, y_hi = ix > 0, ix < nx - 1, iy > 0, iy < ny - 1

    def to_x(up):
        return (x_hi, (ix + 1, iy)) if up else (x_lo, (ix - 1, iy))

    def to_y(up):
        return (y_hi, (ix, iy + 1)) if up else (y_lo, (ix, iy - 1))

    def to_corner(cx, cy):
        there = jnp.logical_and(to_x(cx)[0], to_y(cy)[0])
        return there, (to_x(cx)[1][0], to_y(cy)[1][1])

    sides = [to_x(True), to_x(False), to_y(True), to_y(False)] + [to_corner(*c) for c in CORNERS]
    barrier = pltpu.get_barrier_semaphore()
    for there, target in sides:

        @pl.when(there)
        def _():
            pl.semaphore_signal(barrier, inc=1, device_id=target, device_id_type=MESH)

    raw_x = {up: raw_list(FORCE_X, up, rows_x) for up in (True, False)}
    raw_y = {up: raw_list(FORCE_Y, up, rows_y) for up in (True, False)}
    flow_x = {up: flow_list(FLOW_X, up, rows_x) for up in (True, False)}
    flow_y = {up: flow_list(FLOW_Y, up, rows_y) for up in (True, False)}
    buo_x = {True: [rows_x - 2, rows_x - 1], False: [0, 1]}
    buo_y = {True: [rows_y - 2, rows_y - 1], False: [0, 1]}
    corner = {c: corner_list(c[0], c[1], rows_x, rows_y) for c in CORNERS}

    loads = []

    def load(src, dst):
        copy = pltpu.make_async_copy(src, dst, load_sem.at[len(loads)])
        copy.start()
        loads.append(copy)

    plane = rows_x * rows_y
    load(str_hbm.at[pl.ds(3 * plane, plane)], sx0.at[pl.ds(sx_row(3, 0), plane)])
    load(str_hbm.at[pl.ds(1 * plane, plane)], stage.at[0])
    load(str_hbm.at[pl.ds(5 * plane, plane)], stage.at[1])
    load(buo_hbm, buo)
    load(str_hbm.at[pl.ds(0 * plane, plane)], sx0.at[pl.ds(sx_row(0, 0), plane)])
    load(str_hbm.at[pl.ds(4 * plane, plane)], sx0.at[pl.ds(sx_row(4, 0), plane)])
    first = len(loads)
    load(str_hbm.at[pl.ds(2 * plane, plane)], zb0)
    load(vel_hbm, vel)
    second = len(loads)
    load(cell_hbm, cell_ref)
    load(moment_hbm, moment_ref)
    sources = len(loads)
    load(coh_hbm, coh_ref)
    load(fri_hbm, fri_ref)
    load(zone_hbm, zone)
    load(elig_hbm, elig)
    third = len(loads)
    load(lam_hbm, lam)
    load(mod_hbm, mod)

    tile = jnp.zeros((rows_y, depth), jnp.float32)

    for step in range(STEPS):
        for comp in SLOT_X:
            for layer in (-2, -1, rows_x, rows_x + 1):
                sx[step][pl.ds(sx_row(comp, layer), rows_y), :] = tile
    for ref in (xf, yf):
        for i in range(ref.shape[0] // rows_y):
            ref[pl.ds(i * rows_y, rows_y), :] = tile

    def clear(i, carry):
        for ref in sy:
            ref[pl.ds(pl.multiple_of(i * R + rows_y, 8), R - rows_y), :] = jnp.zeros((R - rows_y, depth), jnp.float32)
        return carry

    lax.fori_loop(0, sy0.shape[0] // R, clear, 0, unroll=4)

    for up in (True, False):

        @pl.when(jnp.logical_not(to_x(not up)[0]))
        def _():
            for step in range(STEPS):
                for i in range(rx.shape[2]):
                    rx[step, int(up), i] = tile

        @pl.when(jnp.logical_not(to_y(not up)[0]))
        def _():
            for step in range(STEPS):

                def wipe(c, carry):
                    for i in range(ry.shape[3] // 8):
                        ry[step, int(up), c, pl.ds(i * 8, 8), :] = tile
                    return carry

                lax.fori_loop(0, chunks, wipe, 0)

    for d, (cx, cy) in enumerate(CORNERS):

        @pl.when(jnp.logical_not(to_corner(not cx, not cy)[0]))
        def _():
            for step in range(STEPS):
                for i in range(rd.shape[2] // 8):
                    rd[step, d, pl.ds(i * 8, 8), :] = tile

    def x_copy(step, up):
        count = len(raw_x[up]) + len(flow_x[up]) + (2 if step == 0 else 0)
        return pltpu.make_async_remote_copy(
            src_ref=xs.at[step, int(up), pl.ds(0, count)],
            dst_ref=rx.at[step, int(up), pl.ds(0, count)],
            send_sem=xsend.at[step, int(up)],
            recv_sem=xrecv.at[step, int(up)],
            device_id=to_x(up)[1],
            device_id_type=MESH,
        )

    def y_parts(step):
        return (0,) if step == 0 else (0, 1)

    def y_copy(step, up, c, part):
        raw, flow = len(raw_y[up]), len(flow_y[up])
        start, count = (0, raw + flow + 2) if step == 0 else ((0, raw), (raw, flow))[part]
        return pltpu.make_async_remote_copy(
            src_ref=ys.at[step, int(up), c, pl.ds(start * 8, count * 8)],
            dst_ref=ry.at[step, int(up), c, pl.ds(start * 8, count * 8)],
            send_sem=ysend.at[step, int(up), c, part],
            recv_sem=yrecv.at[step, int(up), c, part],
            device_id=to_y(up)[1],
            device_id_type=MESH,
        )

    def d_copy(step, d):
        return pltpu.make_async_remote_copy(
            src_ref=ds.at[step, d, pl.ds(0, len(corner[CORNERS[d]]))],
            dst_ref=rd.at[step, d, pl.ds(0, len(corner[CORNERS[d]]))],
            send_sem=dsend.at[step, d],
            recv_sem=drecv.at[step, d],
            device_id=to_corner(*CORNERS[d])[1],
            device_id_type=MESH,
        )

    def sy_pack(step, comp, c, row):
        return sy[step][pl.ds(sy_row(comp, c * CH) + row, CH, stride=R), :]

    def vb_pack(slot, c, row):
        return pl.ds(vb_row(slot, c * CH) + row, CH, stride=R)

    def pack_x_raw(step, up):
        for i, (comp, x) in enumerate(raw_x[up]):
            xs[step, int(up), i] = sx_tile(step, comp, x)
        if step == 0:
            for i, x in enumerate(buo_x[up]):
                xs[step, int(up), len(raw_x[up]) + len(flow_x[up]) + i] = buo[pl.ds(x * rows_y, rows_y), :]

    def pack_y_raw(step, c):
        for up in (True, False):
            for i, (comp, row) in enumerate(raw_y[up]):
                ys[step, int(up), c, pl.ds(i * 8, 8), :] = sy_pack(step, comp, c, row)
            if step == 0:
                for i, row in enumerate(buo_y[up]):
                    value = buo[pl.ds(c * CH * rows_y + row, CH, stride=rows_y), :]
                    ys[step, int(up), c, pl.ds((len(raw_y[up]) + len(flow_y[up]) + i) * 8, 8), :] = value

    def pack_x_flow(step, up):
        for i, (slot, x) in enumerate(flow_x[up]):
            xs[step, int(up), len(raw_x[up]) + i] = vb[step][pl.ds(vb_row(slot, x), rows_y), :]

    def pack_y_flow(step, c):
        for up in (True, False):
            for i, (slot, row) in enumerate(flow_y[up]):
                ys[step, int(up), c, pl.ds((len(raw_y[up]) + i) * 8, 8), :] = vb[step][vb_pack(slot, c, row), :]

    def pack_corners(step, cxs):
        for d, (cx, cy) in enumerate(CORNERS):
            if cx in cxs:
                for i, (comp, x, y) in enumerate(corner[(cx, cy)]):
                    if comp in SLOT_X:
                        value = sx[step][pl.ds(sx_row(comp, x) + y, 1), :]
                    else:
                        value = sy[step][pl.ds(sy_row(comp, x) + y, 1), :]
                    ds[step, d, pl.ds(i, 1), :] = value

    def send_x(step, cores, ways):
        mine = iy % 2 == cores[0]
        for up in ways:

            @pl.when(to_x(up)[0] if len(cores) == 2 else jnp.logical_and(to_x(up)[0], mine))
            def _():
                x_copy(step, up).start()

    def send_y(step, cs, parts):
        for up in (True, False):

            @pl.when(to_y(up)[0])
            def _():
                for c in cs:
                    for part in parts:
                        y_copy(step, up, c, part).start()

    def send_corners(step, cxs):
        for d, (cx, cy) in enumerate(CORNERS):
            if cx in cxs:

                @pl.when(to_corner(cx, cy)[0])
                def _():
                    d_copy(step, d).start()

    weight = time_step / 24.0

    def flow_layer(step, x):
        scale = weight * of_cell(buo, x)
        for slot, force in enumerate(at.forces(step, x)):
            old = vel[pl.ds((slot * rows_x + x) * rows_y, rows_y), :] if step == 0 else at.own_v(step - 1, slot, x)
            vb[step][pl.ds(vb_row(slot, x), rows_y), :] = old + scale * force

    def stress_layer(step, x):
        s = at.stress(step, x)
        for comp in SLOT_X:
            sx[step + 1][pl.ds(sx_row(comp, x), rows_y), :] = s[comp]
        for comp in SLOT_Y:
            sy[step + 1][pl.ds(sy_row(comp, x), rows_y), :] = s[comp]
        zb[step + 1][pl.ds(x * rows_y, rows_y), :] = s[2]

    def of_cell(ref, x):
        return ref[pl.ds(x * rows_y, rows_y), :]

    def wait_x(step):
        for up in (True, False):

            @pl.when(to_x(not up)[0])
            def _():
                x_copy(step, up).wait_recv()

    def wait_y(step, cs):
        for up in (True, False):

            @pl.when(to_y(not up)[0])
            def _():
                for c in cs:
                    for part in y_parts(step):
                        y_copy(step, up, c, part).wait_recv()

    def wait_corners(step):
        for d, (cx, cy) in enumerate(CORNERS):

            @pl.when(to_corner(not cx, not cy)[0])
            def _():
                d_copy(step, d).wait_recv()

    def place(items, what):
        return [i for i, item in enumerate(items) if item == what][0]

    def take_corners(step):
        for d, (cx, cy) in enumerate(CORNERS):

            def raw(comp, x, y):
                return rd[step, d, pl.ds(place(corner[(cx, cy)], (comp, x, y)), 1), :]

            for k in range(3):
                comp, kind = FORCE_Y[k]
                ys_ = edge(kind, cy, rows_y)
                for x in edge(FLOW_X[k], cx, rows_x):
                    base = (int(cx) * 5 + place(flow_x[cx], (k, x))) * rows_y
                    for row, value in spread(kind, cy, rows_y, lambda i: raw(comp, x, ys_[i])):
                        xf[pl.ds(base + row, 1), :] = value
                comp, kind = FORCE_X[k]
                xs_ = edge(kind, cx, rows_x)
                for y in edge(FLOW_Y[k], cy, rows_y):
                    base = ((int(cy) * 5 + place(flow_y[cy], (k, y))) * 2 + int(cx)) * 8
                    for layer, value in spread(kind, cx, CH, lambda i: raw(comp, xs_[i], y)):
                        yf[pl.ds(base + layer, 1), :] = value

    def finish_x(step):
        for up in (True, False):
            side = int(up)
            for k, (comp, kind) in enumerate(FORCE_X):
                places = [place(raw_x[up], (comp, x)) for x in edge(kind, up, rows_x)]
                for x, value in spread(kind, up, rows_x, lambda i: rx[step, side, places[i]]):
                    where = pl.ds(vb_row(k, x), rows_y)
                    vb[step][where, :] = vb[step][where, :] + weight * of_cell(buo, x) * value
            for k, (comp, kind) in enumerate(FORCE_X):
                mine = edge(kind, not up, rows_x)
                adds = dict(spread(kind, not up, rows_x, lambda i: sx_tile(step, comp, mine[i])))
                for x in edge(FLOW_X[k], up, rows_x):
                    i = place(flow_x[up], (k, x))
                    add = adds[x] + xf[pl.ds((side * 5 + i) * rows_y, rows_y), :]
                    scale = weight * rx[0, side, len(raw_x[up]) + len(flow_x[up]) + place(buo_x[up], x)]
                    new = rx[step, side, len(raw_x[up]) + i] + scale * add
                    halo = x - rows_x if up else x + rows_x
                    vb[step][pl.ds(vb_row(k, halo), rows_y), :] = new

    def buo_halo_y(up, c, y):
        i = len(raw_y[up]) + len(flow_y[up]) + place(buo_y[up], y)
        return ry[0, int(up), c, pl.ds(i * 8, 8), :]

    def finish_y(step, c):
        for up in (True, False):
            side = int(up)

            def got(i):
                return ry[step, side, c, pl.ds(i * 8, 8), :]

            for k, (comp, kind) in enumerate(FORCE_Y):
                places = [place(raw_y[up], (comp, y)) for y in edge(kind, up, rows_y)]
                for y, value in spread(kind, up, rows_y, lambda i: got(places[i])):
                    where = vb_pack(k, c, y)
                    scale = weight * buo[pl.ds(c * CH * rows_y + y, CH, stride=rows_y), :]
                    vb[step][where, :] = vb[step][where, :] + scale * value
            for k, (comp, kind) in enumerate(FORCE_Y):
                mine = edge(kind, not up, rows_y)
                adds = dict(spread(kind, not up, rows_y, lambda i: sy_pack(step, comp, c, mine[i])))
                for y in edge(FLOW_Y[k], up, rows_y):
                    i = place(flow_y[up], (k, y))
                    scale = weight * buo_halo_y(up, c, y)
                    new = got(len(raw_y[up]) + i) + scale * adds[y]
                    halo = y - rows_y if up else y + rows_y
                    vb[step][vb_pack(k, c, halo), :] = new

    def finish_corners_y(step):
        for up in (True, False):
            for i, (k, y) in enumerate(flow_y[up]):
                halo = y - rows_y if up else y + rows_y
                for end, c in ((1, 0), (0, chunks - 1)):
                    add = yf[pl.ds(((int(up) * 5 + i) * 2 + end) * 8, 8), :]
                    where = vb_pack(k, c, halo)
                    vb[step][where, :] = vb[step][where, :] + weight * buo_halo_y(up, c, y) * add

    for copy in loads[:first]:
        copy.wait()

    def fill_y(i, carry):
        first_row = pl.multiple_of(i * rows_y, 8)
        for comp, value in (
            (3, sx0[pl.ds(sx_row(3, 0) + first_row, rows_y), :]),
            (1, stage[0, pl.ds(first_row, rows_y), :]),
            (5, stage[1, pl.ds(first_row, rows_y), :]),
        ):
            sy0[pl.ds(pl.multiple_of(sy_row(comp, 0) + i * R, 8), rows_y), :] = value
        return carry

    lax.fori_loop(0, rows_x, fill_y, 0, unroll=8)
    for copy in loads[first:second]:
        copy.wait()
    ends = [0] + ([chunks - 1] if chunks > 1 else [])
    middle = list(range(1, chunks - 1))
    for up in (True, False):
        pack_x_raw(0, up)
    pack_corners(0, (True, False))

    def flow_chunk(c):
        pack_y_raw(0, c)
        for i in range(CH):
            flow_layer(0, c * CH + i)
        pack_y_flow(0, c)

    for c in ends:
        flow_chunk(c)
    for up in (True, False):
        pack_x_flow(0, up)
    heard = sum(there.astype(jnp.int32) for there, _ in sides)
    pl.semaphore_wait(barrier, heard)
    send_corners(0, (True, False))
    send_x(0, (0,), (False, True))
    send_y(0, ends, (0,))
    for c in middle:
        flow_chunk(c)
        send_y(0, (c,), (0,))

    for copy in loads[second:sources]:
        copy.wait()
    cell = cell_ref[...]
    bits = depth.bit_length() - 1
    assert depth == 1 << bits
    plane_row = cell >> bits
    cell_z = cell & (depth - 1)
    row = lax.broadcasted_iota(jnp.int32, (rows_x * rows_y, cell.shape[1]), 0)
    row_bits = rows_y.bit_length() - 1
    assert rows_y == 1 << row_bits
    row = (ix * rows_x + (row >> row_bits)) * (ny * rows_y) + iy * rows_y + (row & (rows_y - 1))
    match = row == plane_row
    at_z = (lax.broadcasted_iota(jnp.int32, (depth, cell.shape[1]), 0) == cell_z).astype(jnp.float32)
    for comp in range(6):
        moment = time_step * moment_ref[pl.ds(comp, 1), :]
        value = lax.dot_general(
            jnp.where(match, moment, 0.0),
            at_z,
            (((1,), (1,)), ((), ())),
            precision=lax.Precision.HIGHEST,
            preferred_element_type=jnp.float32,
        )
        inj[comp] = value.reshape(rows_x, rows_y, depth)

    send_x(0, (1,), (False, True))
    for copy in loads[sources:third]:
        copy.wait()
    frictions, cohesions = [], []
    for which in range(coh_ref.shape[0]):
        f = jnp.full((rows_y, depth), fri_ref[which], jnp.float32)
        frictions.append(f)
        cohesions.append(coh_ref[which] * jnp.sqrt(1.0 - f * f))

    def table(x, carry):
        z = jnp.where(elig[x] == 1, zone[x], -1)
        c = jnp.full((rows_y, depth), 1e30, jnp.float32)
        f = jnp.zeros((rows_y, depth), jnp.float32)
        for which in range(coh_ref.shape[0]):
            hit = z == which
            c = jnp.where(hit, cohesions[which], c)
            f = jnp.where(hit, frictions[which], f)
        cc[x] = c
        cf[x] = f
        return carry

    lax.fori_loop(0, rows_x, table, 0, unroll=2)

    for copy in loads[third:]:
        copy.wait()

    def finish_sends(step):
        for up in (True, False):

            @pl.when(to_x(up)[0])
            def _():
                x_copy(step, up).wait_send()

            @pl.when(to_y(up)[0])
            def _():
                for c in range(chunks):
                    for part in y_parts(step):
                        y_copy(step, up, c, part).wait_send()

        for d, (cx, cy) in enumerate(CORNERS):

            @pl.when(to_corner(cx, cy)[0])
            def _():
                d_copy(step, d).wait_send()

    def flow_rest(step, c, done):
        for x in range(c * CH, (c + 1) * CH):
            if x not in done:
                flow_layer(step, x)
        pack_y_flow(step, c)
        send_y(step, (c,), (1,))

    for step in range(STEPS):
        nxt = step + 1
        wait_y(step, ends)
        for c in ends:
            finish_y(step, c)
        wait_corners(step)
        take_corners(step)
        finish_corners_y(step)
        wait_x(step)
        finish_x(step)
        if nxt == STEPS:
            for i, x in enumerate(rim_of(rows_x)):
                for comp, value in enumerate(at.stress(step, x)):
                    edge_out[comp, i] = value
        wait_y(step, middle)
        for c in middle:
            finish_y(step, c)
        if nxt == STEPS:
            break
        sides_x = ((range(CH), 0, (0, 1), False), (range(rows_x - 4, rows_x), None, (rows_x - 2, rows_x - 1), True))
        flowed, stressed = set(), set()
        for layers, c, flows, up in sides_x:
            for x in layers:
                stress_layer(step, x)
                stressed.add(x)
            if c is not None:
                pack_y_raw(nxt, c)
                send_y(nxt, (c,), (0,))
            for x in flows:
                flow_layer(nxt, x)
                flowed.add(x)
            pack_corners(nxt, (up,))
            send_corners(nxt, (up,))
            pack_x_raw(nxt, up)
            pack_x_flow(nxt, up)
            send_x(nxt, (0,), (up,))
        for x in range(rows_x - CH, rows_x - 4):
            stress_layer(step, x)
            stressed.add(x)
        pack_y_raw(nxt, chunks - 1)
        send_y(nxt, (chunks - 1,), (0,))
        for x in (CH, CH + 1, rows_x - CH - 2, rows_x - CH - 1):
            stress_layer(step, x)
            stressed.add(x)
        for c in ends:
            flow_rest(nxt, c, flowed)
        send_x(nxt, (1,), (False, True))
        for c in middle:
            for x in range(c * CH, (c + 1) * CH):
                if x not in stressed:
                    stress_layer(step, x)
            pack_y_raw(nxt, c)
            send_y(nxt, (c,), (0,))
        for c in middle:
            flow_rest(nxt, c, ())
        for done in range(STEPS):
            finish_sends(done)


def on_device(nx, ny, velocity, stress, lame_first, modulus, buoyancy, zone, eligible, cohesion, friction, source_cell, source_moment):
    rows_x, rows_y, depth = zone.shape
    assert rows_y == 8 and rows_x % CH == 0 and rows_x >= 3 * CH
    chunks = rows_x // CH
    f32 = jnp.float32
    grid = (rows_x, rows_y, depth)
    plane = rows_x * rows_y
    any_spec = pl.BlockSpec(memory_space=pltpu.HBM)
    vmem = pl.BlockSpec(memory_space=pltpu.VMEM)
    dma = pltpu.SemaphoreType.DMA
    fields = [
        pltpu.VMEM((3 * (rows_x + 4) * rows_y, depth), f32),
        pltpu.VMEM((3 * R * (rows_x + 1) + R, depth), f32),
        pltpu.VMEM((plane, depth), f32),
        pltpu.VMEM((3 * (rows_x + 5) * R, depth), f32),
        pltpu.VMEM(grid, f32),
        pltpu.VMEM(grid, f32),
        pltpu.VMEM((6,) + grid, f32),
        pltpu.VMEM(grid, f32),
        pltpu.VMEM(grid, f32),
        pltpu.VMEM((6, len(rim_of(rows_x)), rows_y, depth), f32),
    ]
    held = pl.pallas_call(
        functools.partial(kernel, nx, ny),
        out_shape=fields,
        in_specs=[any_spec] * 11,
        out_specs=[vmem] * len(fields),
        scratch_shapes=fields[:4] + [
            pltpu.VMEM((2, plane, depth), f32),
            pltpu.VMEM((3 * plane, depth), f32),
            pltpu.VMEM((plane, depth), f32),
            pltpu.VMEM(grid, jnp.int32),
            pltpu.VMEM(grid, jnp.int32),
            pltpu.VMEM((STEPS, 2, 11, rows_y, depth), f32),
            pltpu.VMEM((STEPS, 2, 11, rows_y, depth), f32),
            pltpu.VMEM((STEPS, 2, chunks, 11 * 8, depth), f32),
            pltpu.VMEM((STEPS, 2, chunks, 11 * 8, depth), f32),
            pltpu.VMEM((STEPS, 4, 16, depth), f32),
            pltpu.VMEM((STEPS, 4, 16, depth), f32),
            pltpu.VMEM((2 * 5 * rows_y, depth), f32),
            pltpu.VMEM((2 * 5 * 2 * 8, depth), f32),
            pltpu.SMEM(cohesion.shape, f32),
            pltpu.SMEM(friction.shape, f32),
            pltpu.VMEM((1,) + source_cell.shape, jnp.int32),
            pltpu.VMEM(source_moment.shape, f32),
            dma((16,)),
            dma((STEPS, 2)),
            dma((STEPS, 2)),
            dma((STEPS, 2, chunks, 2)),
            dma((STEPS, 2, chunks, 2)),
            dma((STEPS, 4)),
            dma((STEPS, 4)),
        ],
        compiler_params=pltpu.CompilerParams(collective_id=0, has_side_effects=True, vmem_limit_bytes=63_000_000),
    )(
        velocity.reshape(3 * plane, depth), stress.reshape(6 * plane, depth), lame_first, modulus,
        buoyancy.reshape(plane, depth), zone, eligible,
        cohesion, friction, source_cell.reshape(1, -1), source_moment,
    )
    return pl.pallas_call(
        finish_kernel,
        out_shape=(jax.ShapeDtypeStruct((3,) + grid, f32), jax.ShapeDtypeStruct((6,) + grid, f32)),
        in_specs=[vmem] * len(fields),
        out_specs=(any_spec, any_spec),
        scratch_shapes=[pltpu.VMEM((3,) + grid, f32), pltpu.VMEM((6,) + grid, f32), dma((2 + 2 * chunks,))],
        compiler_params=pltpu.CompilerParams(vmem_limit_bytes=24 * 2**20),
    )(*held)


def solution(mesh):
    field = P(None, "gx", "gy", None)
    cells = P("gx", "gy", None)
    return jax.shard_map(
        functools.partial(on_device, mesh.shape["gx"], mesh.shape["gy"]),
        mesh=mesh,
        in_specs=(field, field, cells, cells, cells, cells, cells, P(), P(), P(), P()),
        out_specs=(field, field),
        check_vma=False,
    )
```

```python
import functools

import jax
import jax.numpy as jnp
from jax import lax
from jax.experimental import pallas as pl
from jax.experimental.pallas import tpu as pltpu
from jax.sharding import PartitionSpec as P

STEPS = 2
time_step = 0.1
shear_floor = 0.25
MESH = pl.DeviceIdType.MESH
CH = 8
R = 16

BACK = {"F": 1, "B": 2}
AHEAD = {"F": 2, "B": 1}
FORCE_X = ((0, "F"), (3, "B"), (4, "B"))
FORCE_Y = ((3, "B"), (1, "F"), (5, "B"))
FLOW_X = ("B", "F", "F")
FLOW_Y = ("F", "B", "F")
SLOT_X = {0: 0, 3: 1, 4: 2}
SLOT_Y = {3: 0, 1: 1, 5: 2}


def edge(kind, up, n):
    return list(range(n - BACK[kind], n)) if up else list(range(AHEAD[kind]))


def spread(kind, up, n, get):
    if up and kind == "B":
        return [(0, get(0) - 27.0 * get(1)), (1, get(1))]
    if up:
        return [(0, get(0))]
    if kind == "B":
        return [(n - 1, -get(0))]
    return [(n - 1, 27.0 * get(0) - get(1)), (n - 2, -get(0))]


def raw_list(force, up, n):
    return [(comp, i) for comp, kind in force for i in edge(kind, up, n)]


def flow_list(flow, up, n):
    return [(slot, i) for slot, kind in enumerate(flow) for i in edge(kind, up, n)]


def corner_list(sx, sy, nx, ny):
    found = []
    for k in range(3):
        comp, kind = FORCE_Y[k]
        found += [(comp, x, y) for x in edge(FLOW_X[k], sx, nx) for y in edge(kind, sy, ny)]
        comp, kind = FORCE_X[k]
        found += [(comp, x, y) for x in edge(kind, sx, nx) for y in edge(FLOW_Y[k], sy, ny)]
    return list(dict.fromkeys(found))


CORNERS = [(False, True), (False, False), (True, True), (True, False)]


class Fields:
    def __init__(self, sx, sy, zb, vb, lam, mod, inj, cc, cf):
        self.sx, self.sy, self.zb, self.vb = sx, sy, zb, vb
        self.lam, self.mod, self.inj, self.cc, self.cf = lam, mod, inj, cc, cf
        self.rows_x, self.rows_y, self.depth = lam.shape
        lane = lax.broadcasted_iota(jnp.int32, (self.rows_y, self.depth), 1)
        self.keep = {1: lane < self.depth - 1, 2: lane < self.depth - 2, -1: lane >= 1, -2: lane >= 2}

    def sx_row(self, comp, x):
        return (SLOT_X[comp] * (self.rows_x + 4) + x + 2) * self.rows_y

    def sy_row(self, comp, x):
        return SLOT_Y[comp] * R * (self.rows_x + 1) + R * (x + 1)

    def vb_row(self, slot, x):
        return (slot * (self.rows_x + 5) + x + 3) * R

    def sx_tile(self, step, comp, x):
        return self.sx[step][pl.ds(self.sx_row(comp, x), self.rows_y), :]

    def own_sy(self, step, comp, x):
        return self.sy[step][pl.ds(self.sy_row(comp, x), self.rows_y), :]

    def own_zb(self, step, x):
        return self.zb[step][pl.ds(x * self.rows_y, self.rows_y), :]

    def own_v(self, step, slot, x):
        return self.vb[step][pl.ds(self.vb_row(slot, x), self.rows_y), :]

    def along_z(self, value, offset):
        if offset == 0:
            return value
        return jnp.where(self.keep[offset], pltpu.roll(value, (-offset) % self.depth, 1), 0.0)

    def derivative(self, get, forward):
        a, b, c, d = (get(1), get(0), get(2), get(-1)) if forward else (get(0), get(-1), get(1), get(-2))
        return 27.0 * (a - b) - (c - d)

    def s_dx(self, step, comp, x, forward):
        return self.derivative(lambda o: self.sx_tile(step, comp, x + o), forward)

    def s_dy(self, step, comp, x, forward):
        row = self.sy_row(comp, x)
        return self.derivative(lambda o: self.sy[step][pl.ds(row + o, self.rows_y), :], forward)

    def v_dx(self, step, slot, x, forward):
        return self.derivative(lambda o: self.own_v(step, slot, x + o), forward)

    def v_dy(self, step, slot, x, forward):
        row = self.vb_row(slot, x)
        return self.derivative(lambda o: self.vb[step][pl.ds(row + o, self.rows_y), :], forward)

    def dz(self, value, forward):
        return self.derivative(lambda o: self.along_z(value, o), forward)

    def forces(self, step, x):
        xz, yz, zz = self.sx_tile(step, 4, x), self.own_sy(step, 5, x), self.own_zb(step, x)
        return (
            self.s_dx(step, 0, x, True) + self.s_dy(step, 3, x, False) + self.dz(xz, False),
            self.s_dx(step, 3, x, False) + self.s_dy(step, 1, x, True) + self.dz(yz, False),
            self.s_dx(step, 4, x, False) + self.s_dy(step, 5, x, False) + self.dz(zz, True),
        )

    def stress(self, step, x):
        vx, vy, vz = (self.own_v(step, slot, x) for slot in range(3))
        ex = self.v_dx(step, 0, x, False)
        ey = self.v_dy(step, 1, x, False)
        ez = self.dz(vz, False)
        xy = self.v_dy(step, 0, x, True) + self.v_dx(step, 1, x, True)
        xz = self.dz(vx, True) + self.v_dx(step, 2, x, True)
        yz = self.dz(vy, True) + self.v_dy(step, 2, x, True)
        weight = time_step / 24.0
        inj = self.inj
        m = weight * self.mod[x]
        grow = weight * self.lam[x] * (ex + ey + ez)
        m2 = m + m
        s0, s3, s4 = (self.sx_tile(step, comp, x) for comp in (0, 3, 4))
        s1, s5 = self.own_sy(step, 1, x), self.own_sy(step, 5, x)
        s2 = self.own_zb(step, x)
        s0 = s0 + (grow + m2 * ex) + inj[0, x]
        s1 = s1 + (grow + m2 * ey) + inj[1, x]
        s2 = s2 + (grow + m2 * ez) + inj[2, x]
        s3 = s3 + m * xy + inj[3, x]
        s4 = s4 + m * xz + inj[4, x]
        s5 = s5 + m * yz + inj[5, x]
        pressure = (s0 + s1 + s2) * (1.0 / 3.0)
        d0, d1, d2 = s0 - pressure, s1 - pressure, s2 - pressure
        second = 0.5 * (d0 * d0 + d1 * d1 + d2 * d2) + (s3 * s3 + s4 * s4 + s5 * s5)
        strength = jnp.maximum(self.cc[x] - pressure * self.cf[x], 0.0)
        factor = jnp.minimum(1.0, strength * lax.rsqrt(jnp.maximum(second, shear_floor * shear_floor)))
        s0, s1, s2 = pressure + factor * d0, pressure + factor * d1, pressure + factor * d2
        return s0, s1, s2, factor * s3, factor * s4, factor * s5


def rim_of(rows_x):
    return [*range(4), *range(rows_x - 4, rows_x)]


def finish_kernel(sx, sy, zb, vb, lam, mod, inj, cc, cf, edge_out, vout_hbm, sout_hbm, vout, sout, sem):
    at = Fields((None, sx), (None, sy), (None, zb), (None, vb), lam, mod, inj, cc, cf)
    copies = []

    def put(src, dst):
        copy = pltpu.make_async_copy(src, dst, sem.at[len(copies)])
        copy.start()
        copies.append(copy)

    for i, x in ((0, 0), (4, at.rows_x - 4)):
        put(edge_out.at[:, pl.ds(i, 4)], sout_hbm.at[:, pl.ds(x, 4)])
    for start in range(4, at.rows_x - 4, CH):
        stop = min(start + CH, at.rows_x - 4)
        low, high = (0 if start == 4 else start), (at.rows_x if stop == at.rows_x - 4 else stop)
        for x in range(low, high):
            for slot in range(3):
                vout[slot, x] = at.own_v(STEPS - 1, slot, x)
        put(vout.at[:, pl.ds(low, high - low)], vout_hbm.at[:, pl.ds(low, high - low)])
        for x in range(start, stop):
            for comp, value in enumerate(at.stress(STEPS - 1, x)):
                sout[comp, x] = value
        put(sout.at[:, pl.ds(start, stop - start)], sout_hbm.at[:, pl.ds(start, stop - start)])
    for copy in copies:
        copy.wait()


def kernel(
    nx,
    ny,
    vel_hbm, str_hbm, lam_hbm, mod_hbm, buo_hbm, zone_hbm, elig_hbm,
    coh_hbm, fri_hbm, cell_hbm, moment_hbm,
    sx1, sy1, zb1, vb1, lam, mod, inj, cc, cf, edge_out,
    sx0, sy0, zb0, vb0, stage, vel, buo, zone, elig,
    xs, rx, ys, ry, ds, rd, xf, yf, coh_ref, fri_ref, cell_ref, moment_ref,
    load_sem, xsend, xrecv, ysend, yrecv, dsend, drecv, ready,
):
    rows_x = lam.shape[0]
    rows_y = lam.shape[1]
    depth = lam.shape[2]
    chunks = rows_x // CH
    sx, sy, zb, vb = (sx0, sx1), (sy0, sy1), (zb0, zb1), (vb0, vb1)
    at = Fields(sx, sy, zb, vb, lam, mod, inj, cc, cf)
    sx_row, sy_row, vb_row, sx_tile = at.sx_row, at.sy_row, at.vb_row, at.sx_tile
    ix = lax.axis_index("gx")
    iy = lax.axis_index("gy")
    x_lo, x_hi, y_lo, y_hi = ix > 0, ix < nx - 1, iy > 0, iy < ny - 1

    def to_x(up):
        return (x_hi, (ix + 1, iy)) if up else (x_lo, (ix - 1, iy))

    def to_y(up):
        return (y_hi, (ix, iy + 1)) if up else (y_lo, (ix, iy - 1))

    def to_corner(cx, cy):
        there = jnp.logical_and(to_x(cx)[0], to_y(cy)[0])
        return there, (to_x(cx)[1][0], to_y(cy)[1][1])

    sides = [to_x(True), to_x(False), to_y(True), to_y(False)]
    barrier = pltpu.get_barrier_semaphore()
    for there, target in sides:

        @pl.when(there)
        def _():
            pl.semaphore_signal(barrier, inc=1, device_id=target, device_id_type=MESH)

    raw_x = {up: raw_list(FORCE_X, up, rows_x) for up in (True, False)}
    raw_y = {up: raw_list(FORCE_Y, up, rows_y) for up in (True, False)}
    flow_x = {up: flow_list(FLOW_X, up, rows_x) for up in (True, False)}
    flow_y = {up: flow_list(FLOW_Y, up, rows_y) for up in (True, False)}
    buo_x = {True: [rows_x - 2, rows_x - 1], False: [0, 1]}
    buo_y = {True: [rows_y - 2, rows_y - 1], False: [0, 1]}
    corner = {c: corner_list(c[0], c[1], rows_x, rows_y) for c in CORNERS}

    loads = []

    def load(src, dst):
        copy = pltpu.make_async_copy(src, dst, load_sem.at[len(loads)])
        copy.start()
        loads.append(copy)

    plane = rows_x * rows_y
    load(str_hbm.at[pl.ds(3 * plane, plane)], sx0.at[pl.ds(sx_row(3, 0), plane)])
    load(str_hbm.at[pl.ds(1 * plane, plane)], stage.at[0])
    load(str_hbm.at[pl.ds(5 * plane, plane)], stage.at[1])
    load(buo_hbm, buo)
    load(str_hbm.at[pl.ds(0 * plane, plane)], sx0.at[pl.ds(sx_row(0, 0), plane)])
    load(str_hbm.at[pl.ds(4 * plane, plane)], sx0.at[pl.ds(sx_row(4, 0), plane)])
    first = len(loads)
    load(str_hbm.at[pl.ds(2 * plane, plane)], zb0)
    load(vel_hbm, vel)
    second = len(loads)
    load(cell_hbm, cell_ref)
    load(moment_hbm, moment_ref)
    sources = len(loads)
    load(coh_hbm, coh_ref)
    load(fri_hbm, fri_ref)
    load(zone_hbm, zone)
    load(elig_hbm, elig)
    third = len(loads)
    load(lam_hbm, lam)
    load(mod_hbm, mod)

    tile = jnp.zeros((rows_y, depth), jnp.float32)

    for step in range(STEPS):
        for comp in SLOT_X:
            for layer in (-2, -1, rows_x, rows_x + 1):
                sx[step][pl.ds(sx_row(comp, layer), rows_y), :] = tile
    for ref in (xf, yf):
        for i in range(ref.shape[0] // rows_y):
            ref[pl.ds(i * rows_y, rows_y), :] = tile

    def clear(i, carry):
        for ref in sy:
            ref[pl.ds(pl.multiple_of(i * R + rows_y, 8), R - rows_y), :] = jnp.zeros((R - rows_y, depth), jnp.float32)
        return carry

    lax.fori_loop(0, sy0.shape[0] // R, clear, 0, unroll=4)

    for up in (True, False):

        @pl.when(jnp.logical_not(to_x(not up)[0]))
        def _():
            for step in range(STEPS):
                for i in range(rx.shape[2]):
                    rx[step, int(up), i] = tile

        @pl.when(jnp.logical_not(to_y(not up)[0]))
        def _():
            for step in range(STEPS):

                def wipe(c, carry):
                    for i in range(ry.shape[3] // 8):
                        ry[step, int(up), c, pl.ds(i * 8, 8), :] = tile
                    return carry

                lax.fori_loop(0, chunks, wipe, 0)

    for d, (cx, cy) in enumerate(CORNERS):

        @pl.when(jnp.logical_not(to_corner(not cx, not cy)[0]))
        def _():
            for step in range(STEPS):
                for i in range(rd.shape[2] // 8):
                    rd[step, d, pl.ds(i * 8, 8), :] = tile

    def x_copy(step, up):
        count = len(raw_x[up]) + len(flow_x[up]) + (2 if step == 0 else 0)
        return pltpu.make_async_remote_copy(
            src_ref=xs.at[step, int(up), pl.ds(0, count)],
            dst_ref=rx.at[step, int(up), pl.ds(0, count)],
            send_sem=xsend.at[step, int(up)],
            recv_sem=xrecv.at[step, int(up)],
            device_id=to_x(up)[1],
            device_id_type=MESH,
        )

    def y_parts(step):
        return (0,) if step == 0 else (0, 1)

    def y_copy(step, up, c, part):
        raw, flow = len(raw_y[up]), len(flow_y[up])
        start, count = (0, raw + flow + 2) if step == 0 else ((0, raw), (raw, flow))[part]
        return pltpu.make_async_remote_copy(
            src_ref=ys.at[step, int(up), c, pl.ds(start * 8, count * 8)],
            dst_ref=ry.at[step, int(up), c, pl.ds(start * 8, count * 8)],
            send_sem=ysend.at[step, int(up), c, part],
            recv_sem=yrecv.at[step, int(up), c, part],
            device_id=to_y(up)[1],
            device_id_type=MESH,
        )

    def d_copy(step, d):
        return pltpu.make_async_remote_copy(
            src_ref=ds.at[step, d, pl.ds(0, len(corner[CORNERS[d]]))],
            dst_ref=rd.at[step, d, pl.ds(0, len(corner[CORNERS[d]]))],
            send_sem=dsend.at[step, d],
            recv_sem=drecv.at[step, d],
            device_id=to_corner(*CORNERS[d])[1],
            device_id_type=MESH,
        )

    def sy_pack(step, comp, c, row):
        return sy[step][pl.ds(sy_row(comp, c * CH) + row, CH, stride=R), :]

    def vb_pack(slot, c, row):
        return pl.ds(vb_row(slot, c * CH) + row, CH, stride=R)

    def pack_x_raw(step, up):
        for i, (comp, x) in enumerate(raw_x[up]):
            xs[step, int(up), i] = sx_tile(step, comp, x)
        if step == 0:
            for i, x in enumerate(buo_x[up]):
                xs[step, int(up), len(raw_x[up]) + len(flow_x[up]) + i] = buo[pl.ds(x * rows_y, rows_y), :]

    def pack_y_raw(step, c):
        for up in (True, False):
            for i, (comp, row) in enumerate(raw_y[up]):
                ys[step, int(up), c, pl.ds(i * 8, 8), :] = sy_pack(step, comp, c, row)
            if step == 0:
                for i, row in enumerate(buo_y[up]):
                    value = buo[pl.ds(c * CH * rows_y + row, CH, stride=rows_y), :]
                    ys[step, int(up), c, pl.ds((len(raw_y[up]) + len(flow_y[up]) + i) * 8, 8), :] = value

    def pack_x_flow(step, up):
        for i, (slot, x) in enumerate(flow_x[up]):
            xs[step, int(up), len(raw_x[up]) + i] = vb[step][pl.ds(vb_row(slot, x), rows_y), :]

    def pack_y_flow(step, c):
        for up in (True, False):
            for i, (slot, row) in enumerate(flow_y[up]):
                ys[step, int(up), c, pl.ds((len(raw_y[up]) + i) * 8, 8), :] = vb[step][vb_pack(slot, c, row), :]

    def pack_corners(step, cxs):
        for d, (cx, cy) in enumerate(CORNERS):
            if cx in cxs:
                for i, (comp, x, y) in enumerate(corner[(cx, cy)]):
                    if comp in SLOT_X:
                        value = sx[step][pl.ds(sx_row(comp, x) + y, 1), :]
                    else:
                        value = sy[step][pl.ds(sy_row(comp, x) + y, 1), :]
                    ds[step, d, pl.ds(i, 1), :] = value

    def send_x(step, cores, ways):
        mine = iy % 2 == cores[0]
        for up in ways:

            @pl.when(to_x(up)[0] if len(cores) == 2 else jnp.logical_and(to_x(up)[0], mine))
            def _():
                x_copy(step, up).start()

    def send_y(step, cs, parts):
        for up in (True, False):

            @pl.when(to_y(up)[0])
            def _():
                for c in cs:
                    for part in parts:
                        y_copy(step, up, c, part).start()

    def send_corners(step, cxs):
        for d, (cx, cy) in enumerate(CORNERS):
            if cx in cxs:

                @pl.when(to_corner(cx, cy)[0])
                def _():
                    d_copy(step, d).start()

    weight = time_step / 24.0

    def flow_layer(step, x):
        scale = weight * of_cell(buo, x)
        for slot, force in enumerate(at.forces(step, x)):
            old = vel[pl.ds((slot * rows_x + x) * rows_y, rows_y), :] if step == 0 else at.own_v(step - 1, slot, x)
            vb[step][pl.ds(vb_row(slot, x), rows_y), :] = old + scale * force

    def stress_layer(step, x):
        s = at.stress(step, x)
        for comp in SLOT_X:
            sx[step + 1][pl.ds(sx_row(comp, x), rows_y), :] = s[comp]
        for comp in SLOT_Y:
            sy[step + 1][pl.ds(sy_row(comp, x), rows_y), :] = s[comp]
        zb[step + 1][pl.ds(x * rows_y, rows_y), :] = s[2]

    def of_cell(ref, x):
        return ref[pl.ds(x * rows_y, rows_y), :]

    def wait_x(step):
        for up in (True, False):

            @pl.when(to_x(not up)[0])
            def _():
                x_copy(step, up).wait_recv()

    def wait_y(step, cs):
        for up in (True, False):

            @pl.when(to_y(not up)[0])
            def _():
                for c in cs:
                    for part in y_parts(step):
                        y_copy(step, up, c, part).wait_recv()

    def wait_corners(step):
        for d, (cx, cy) in enumerate(CORNERS):

            @pl.when(to_corner(not cx, not cy)[0])
            def _():
                d_copy(step, d).wait_recv()

    def place(items, what):
        return [i for i, item in enumerate(items) if item == what][0]

    def take_corners(step):
        for d, (cx, cy) in enumerate(CORNERS):

            def raw(comp, x, y):
                return rd[step, d, pl.ds(place(corner[(cx, cy)], (comp, x, y)), 1), :]

            for k in range(3):
                comp, kind = FORCE_Y[k]
                ys_ = edge(kind, cy, rows_y)
                for x in edge(FLOW_X[k], cx, rows_x):
                    base = (int(cx) * 5 + place(flow_x[cx], (k, x))) * rows_y
                    for row, value in spread(kind, cy, rows_y, lambda i: raw(comp, x, ys_[i])):
                        xf[pl.ds(base + row, 1), :] = value
                comp, kind = FORCE_X[k]
                xs_ = edge(kind, cx, rows_x)
                for y in edge(FLOW_Y[k], cy, rows_y):
                    base = ((int(cy) * 5 + place(flow_y[cy], (k, y))) * 2 + int(cx)) * 8
                    for layer, value in spread(kind, cx, CH, lambda i: raw(comp, xs_[i], y)):
                        yf[pl.ds(base + layer, 1), :] = value

    def finish_x(step):
        for up in (True, False):
            side = int(up)
            for k, (comp, kind) in enumerate(FORCE_X):
                places = [place(raw_x[up], (comp, x)) for x in edge(kind, up, rows_x)]
                for x, value in spread(kind, up, rows_x, lambda i: rx[step, side, places[i]]):
                    where = pl.ds(vb_row(k, x), rows_y)
                    vb[step][where, :] = vb[step][where, :] + weight * of_cell(buo, x) * value
            for k, (comp, kind) in enumerate(FORCE_X):
                mine = edge(kind, not up, rows_x)
                adds = dict(spread(kind, not up, rows_x, lambda i: sx_tile(step, comp, mine[i])))
                for x in edge(FLOW_X[k], up, rows_x):
                    i = place(flow_x[up], (k, x))
                    add = adds[x] + xf[pl.ds((side * 5 + i) * rows_y, rows_y), :]
                    scale = weight * rx[0, side, len(raw_x[up]) + len(flow_x[up]) + place(buo_x[up], x)]
                    new = rx[step, side, len(raw_x[up]) + i] + scale * add
                    halo = x - rows_x if up else x + rows_x
                    vb[step][pl.ds(vb_row(k, halo), rows_y), :] = new

    def buo_halo_y(up, c, y):
        i = len(raw_y[up]) + len(flow_y[up]) + place(buo_y[up], y)
        return ry[0, int(up), c, pl.ds(i * 8, 8), :]

    def finish_y(step, c):
        for up in (True, False):
            side = int(up)

            def got(i):
                return ry[step, side, c, pl.ds(i * 8, 8), :]

            for k, (comp, kind) in enumerate(FORCE_Y):
                places = [place(raw_y[up], (comp, y)) for y in edge(kind, up, rows_y)]
                for y, value in spread(kind, up, rows_y, lambda i: got(places[i])):
                    where = vb_pack(k, c, y)
                    scale = weight * buo[pl.ds(c * CH * rows_y + y, CH, stride=rows_y), :]
                    vb[step][where, :] = vb[step][where, :] + scale * value
            for k, (comp, kind) in enumerate(FORCE_Y):
                mine = edge(kind, not up, rows_y)
                adds = dict(spread(kind, not up, rows_y, lambda i: sy_pack(step, comp, c, mine[i])))
                for y in edge(FLOW_Y[k], up, rows_y):
                    i = place(flow_y[up], (k, y))
                    scale = weight * buo_halo_y(up, c, y)
                    new = got(len(raw_y[up]) + i) + scale * adds[y]
                    halo = y - rows_y if up else y + rows_y
                    vb[step][vb_pack(k, c, halo), :] = new

    def finish_corners_y(step):
        for up in (True, False):
            for i, (k, y) in enumerate(flow_y[up]):
                halo = y - rows_y if up else y + rows_y
                for end, c in ((1, 0), (0, chunks - 1)):
                    add = yf[pl.ds(((int(up) * 5 + i) * 2 + end) * 8, 8), :]
                    where = vb_pack(k, c, halo)
                    vb[step][where, :] = vb[step][where, :] + weight * buo_halo_y(up, c, y) * add

    for copy in loads[:first]:
        copy.wait()

    def fill_y(i, carry):
        first_row = pl.multiple_of(i * rows_y, 8)
        for comp, value in (
            (3, sx0[pl.ds(sx_row(3, 0) + first_row, rows_y), :]),
            (1, stage[0, pl.ds(first_row, rows_y), :]),
            (5, stage[1, pl.ds(first_row, rows_y), :]),
        ):
            sy0[pl.ds(pl.multiple_of(sy_row(comp, 0) + i * R, 8), rows_y), :] = value
        return carry

    lax.fori_loop(0, rows_x, fill_y, 0, unroll=8)
    for copy in loads[first:second]:
        copy.wait()
    ends = [0] + ([chunks - 1] if chunks > 1 else [])
    middle = list(range(1, chunks - 1))
    for up in (True, False):
        pack_x_raw(0, up)
    pack_corners(0, (True, False))

    def flow_chunk(c):
        pack_y_raw(0, c)
        for i in range(CH):
            flow_layer(0, c * CH + i)
        pack_y_flow(0, c)

    for c in ends:
        flow_chunk(c)
    for up in (True, False):
        pack_x_flow(0, up)
    heard = sum(there.astype(jnp.int32) for there, _ in sides)
    pl.semaphore_wait(barrier, heard)
    for there, target in sides:

        @pl.when(there)
        def _():
            pl.semaphore_signal(ready, inc=1, device_id=target, device_id_type=MESH)

    send_x(0, (0,), (False, True))
    send_y(0, ends, (0,))
    for c in middle:
        flow_chunk(c)
        send_y(0, (c,), (0,))

    for copy in loads[second:sources]:
        copy.wait()
    cell = cell_ref[...]
    bits = depth.bit_length() - 1
    assert depth == 1 << bits
    plane_row = cell >> bits
    cell_z = cell & (depth - 1)
    row = lax.broadcasted_iota(jnp.int32, (rows_x * rows_y, cell.shape[1]), 0)
    row_bits = rows_y.bit_length() - 1
    assert rows_y == 1 << row_bits
    row = (ix * rows_x + (row >> row_bits)) * (ny * rows_y) + iy * rows_y + (row & (rows_y - 1))
    match = row == plane_row
    at_z = (lax.broadcasted_iota(jnp.int32, (depth, cell.shape[1]), 0) == cell_z).astype(jnp.float32)
    for comp in range(6):
        if comp == 4:
            pl.semaphore_wait(ready, heard)
            send_corners(0, (True, False))
            send_x(0, (1,), (False, True))
        moment = time_step * moment_ref[pl.ds(comp, 1), :]
        value = lax.dot_general(
            jnp.where(match, moment, 0.0),
            at_z,
            (((1,), (1,)), ((), ())),
            precision=lax.Precision.HIGHEST,
            preferred_element_type=jnp.float32,
        )
        inj[comp] = value.reshape(rows_x, rows_y, depth)

    for copy in loads[sources:third]:
        copy.wait()
    frictions, cohesions = [], []
    for which in range(coh_ref.shape[0]):
        f = jnp.full((rows_y, depth), fri_ref[which], jnp.float32)
        frictions.append(f)
        cohesions.append(coh_ref[which] * jnp.sqrt(1.0 - f * f))

    def table(x, carry):
        z = jnp.where(elig[x] == 1, zone[x], -1)
        c = jnp.full((rows_y, depth), 1e30, jnp.float32)
        f = jnp.zeros((rows_y, depth), jnp.float32)
        for which in range(coh_ref.shape[0]):
            hit = z == which
            c = jnp.where(hit, cohesions[which], c)
            f = jnp.where(hit, frictions[which], f)
        cc[x] = c
        cf[x] = f
        return carry

    lax.fori_loop(0, rows_x, table, 0, unroll=2)

    for copy in loads[third:]:
        copy.wait()

    def finish_sends(step):
        for up in (True, False):

            @pl.when(to_x(up)[0])
            def _():
                x_copy(step, up).wait_send()

            @pl.when(to_y(up)[0])
            def _():
                for c in range(chunks):
                    for part in y_parts(step):
                        y_copy(step, up, c, part).wait_send()

        for d, (cx, cy) in enumerate(CORNERS):

            @pl.when(to_corner(cx, cy)[0])
            def _():
                d_copy(step, d).wait_send()

    def flow_rest(step, c, done):
        for x in range(c * CH, (c + 1) * CH):
            if x not in done:
                flow_layer(step, x)
        pack_y_flow(step, c)
        send_y(step, (c,), (1,))

    for step in range(STEPS):
        nxt = step + 1
        wait_y(step, ends)
        for c in ends:
            finish_y(step, c)
        wait_corners(step)
        take_corners(step)
        finish_corners_y(step)
        wait_x(step)
        finish_x(step)
        if nxt == STEPS:
            for i, x in enumerate(rim_of(rows_x)):
                for comp, value in enumerate(at.stress(step, x)):
                    edge_out[comp, i] = value
        wait_y(step, middle)
        for c in middle:
            finish_y(step, c)
        if nxt == STEPS:
            break
        stressed = set()

        def stress_layers(layers):
            for x in layers:
                if x not in stressed:
                    stress_layer(step, x)
                    stressed.add(x)

        stress_layers(rim_of(rows_x))
        pack_corners(nxt, (False, True))
        send_corners(nxt, (False, True))
        flowed = (0, 1, rows_x - 2, rows_x - 1)
        for x in flowed:
            flow_layer(nxt, x)
        for up in (False, True):
            pack_x_raw(nxt, up)
            pack_x_flow(nxt, up)
        send_x(nxt, (0,), (False, True))
        for c in ends:
            stress_layers(range(c * CH, (c + 1) * CH))
            pack_y_raw(nxt, c)
            send_y(nxt, (c,), (0,))
        stress_layers((CH, CH + 1, rows_x - CH - 2, rows_x - CH - 1))
        for c in ends:
            flow_rest(nxt, c, flowed)
        send_x(nxt, (1,), (False, True))
        for c in middle:
            stress_layers(range(c * CH, (c + 1) * CH))
            pack_y_raw(nxt, c)
            send_y(nxt, (c,), (0,))
        for c in middle:
            flow_rest(nxt, c, ())
        for done in range(STEPS):
            finish_sends(done)


def on_device(nx, ny, velocity, stress, lame_first, modulus, buoyancy, zone, eligible, cohesion, friction, source_cell, source_moment):
    rows_x, rows_y, depth = zone.shape
    assert rows_y == 8 and rows_x % CH == 0 and rows_x >= 3 * CH
    chunks = rows_x // CH
    f32 = jnp.float32
    grid = (rows_x, rows_y, depth)
    plane = rows_x * rows_y
    any_spec = pl.BlockSpec(memory_space=pltpu.HBM)
    vmem = pl.BlockSpec(memory_space=pltpu.VMEM)
    dma = pltpu.SemaphoreType.DMA
    fields = [
        pltpu.VMEM((3 * (rows_x + 4) * rows_y, depth), f32),
        pltpu.VMEM((3 * R * (rows_x + 1) + R, depth), f32),
        pltpu.VMEM((plane, depth), f32),
        pltpu.VMEM((3 * (rows_x + 5) * R, depth), f32),
        pltpu.VMEM(grid, f32),
        pltpu.VMEM(grid, f32),
        pltpu.VMEM((6,) + grid, f32),
        pltpu.VMEM(grid, f32),
        pltpu.VMEM(grid, f32),
        pltpu.VMEM((6, len(rim_of(rows_x)), rows_y, depth), f32),
    ]
    held = pl.pallas_call(
        functools.partial(kernel, nx, ny),
        out_shape=fields,
        in_specs=[any_spec] * 11,
        out_specs=[vmem] * len(fields),
        scratch_shapes=fields[:4] + [
            pltpu.VMEM((2, plane, depth), f32),
            pltpu.VMEM((3 * plane, depth), f32),
            pltpu.VMEM((plane, depth), f32),
            pltpu.VMEM(grid, jnp.int32),
            pltpu.VMEM(grid, jnp.int32),
            pltpu.VMEM((STEPS, 2, 11, rows_y, depth), f32),
            pltpu.VMEM((STEPS, 2, 11, rows_y, depth), f32),
            pltpu.VMEM((STEPS, 2, chunks, 11 * 8, depth), f32),
            pltpu.VMEM((STEPS, 2, chunks, 11 * 8, depth), f32),
            pltpu.VMEM((STEPS, 4, 16, depth), f32),
            pltpu.VMEM((STEPS, 4, 16, depth), f32),
            pltpu.VMEM((2 * 5 * rows_y, depth), f32),
            pltpu.VMEM((2 * 5 * 2 * 8, depth), f32),
            pltpu.SMEM(cohesion.shape, f32),
            pltpu.SMEM(friction.shape, f32),
            pltpu.VMEM((1,) + source_cell.shape, jnp.int32),
            pltpu.VMEM(source_moment.shape, f32),
            dma((16,)),
            dma((STEPS, 2)),
            dma((STEPS, 2)),
            dma((STEPS, 2, chunks, 2)),
            dma((STEPS, 2, chunks, 2)),
            dma((STEPS, 4)),
            dma((STEPS, 4)),
            pltpu.SemaphoreType.REGULAR,
        ],
        compiler_params=pltpu.CompilerParams(collective_id=0, has_side_effects=True, vmem_limit_bytes=63_000_000),
    )(
        velocity.reshape(3 * plane, depth), stress.reshape(6 * plane, depth), lame_first, modulus,
        buoyancy.reshape(plane, depth), zone, eligible,
        cohesion, friction, source_cell.reshape(1, -1), source_moment,
    )
    return pl.pallas_call(
        finish_kernel,
        out_shape=(jax.ShapeDtypeStruct((3,) + grid, f32), jax.ShapeDtypeStruct((6,) + grid, f32)),
        in_specs=[vmem] * len(fields),
        out_specs=(any_spec, any_spec),
        scratch_shapes=[pltpu.VMEM((3,) + grid, f32), pltpu.VMEM((6,) + grid, f32), dma((2 + 2 * chunks,))],
        compiler_params=pltpu.CompilerParams(vmem_limit_bytes=24 * 2**20),
    )(*held)


def solution(mesh):
    field = P(None, "gx", "gy", None)
    cells = P("gx", "gy", None)
    return jax.shard_map(
        functools.partial(on_device, mesh.shape["gx"], mesh.shape["gy"]),
        mesh=mesh,
        in_specs=(field, field, cells, cells, cells, cells, cells, P(), P(), P(), P()),
        out_specs=(field, field),
        check_vma=False,
    )
```

```python
import functools

import jax
import jax.numpy as jnp
from jax import lax
from jax.experimental import pallas as pl
from jax.experimental.pallas import tpu as pltpu
from jax.sharding import PartitionSpec as P

STEPS = 2
time_step = 0.1
shear_floor = 0.25
MESH = pl.DeviceIdType.MESH
CH = 8
R = 16

BACK = {"F": 1, "B": 2}
AHEAD = {"F": 2, "B": 1}
FORCE_X = ((0, "F"), (3, "B"), (4, "B"))
FORCE_Y = ((3, "B"), (1, "F"), (5, "B"))
FLOW_X = ("B", "F", "F")
FLOW_Y = ("F", "B", "F")
SLOT_X = {0: 0, 3: 1, 4: 2}
SLOT_Y = {3: 0, 1: 1, 5: 2}


def edge(kind, up, n):
    return list(range(n - BACK[kind], n)) if up else list(range(AHEAD[kind]))


def spread(kind, up, n, get):
    if up and kind == "B":
        return [(0, get(0) - 27.0 * get(1)), (1, get(1))]
    if up:
        return [(0, get(0))]
    if kind == "B":
        return [(n - 1, -get(0))]
    return [(n - 1, 27.0 * get(0) - get(1)), (n - 2, -get(0))]


def raw_list(force, up, n):
    return [(comp, i) for comp, kind in force for i in edge(kind, up, n)]


def flow_list(flow, up, n):
    return [(slot, i) for slot, kind in enumerate(flow) for i in edge(kind, up, n)]


def corner_list(sx, sy, nx, ny):
    found = []
    for k in range(3):
        comp, kind = FORCE_Y[k]
        found += [(comp, x, y) for x in edge(FLOW_X[k], sx, nx) for y in edge(kind, sy, ny)]
        comp, kind = FORCE_X[k]
        found += [(comp, x, y) for x in edge(kind, sx, nx) for y in edge(FLOW_Y[k], sy, ny)]
    return list(dict.fromkeys(found))


CORNERS = [(False, True), (False, False), (True, True), (True, False)]


class Fields:
    def __init__(self, sx, sy, zb, vb, lam, mod, inj, cc, cf):
        self.sx, self.sy, self.zb, self.vb = sx, sy, zb, vb
        self.lam, self.mod, self.inj, self.cc, self.cf = lam, mod, inj, cc, cf
        self.rows_x, self.rows_y, self.depth = lam.shape
        lane = lax.broadcasted_iota(jnp.int32, (self.rows_y, self.depth), 1)
        self.keep = {1: lane < self.depth - 1, 2: lane < self.depth - 2, -1: lane >= 1, -2: lane >= 2}

    def sx_row(self, comp, x):
        return (SLOT_X[comp] * (self.rows_x + 4) + x + 2) * self.rows_y

    def sy_row(self, comp, x):
        return SLOT_Y[comp] * R * (self.rows_x + 1) + R * (x + 1)

    def vb_row(self, slot, x):
        return (slot * (self.rows_x + 5) + x + 3) * R

    def sx_tile(self, step, comp, x):
        return self.sx[step][pl.ds(self.sx_row(comp, x), self.rows_y), :]

    def own_sy(self, step, comp, x):
        return self.sy[step][pl.ds(self.sy_row(comp, x), self.rows_y), :]

    def own_zb(self, step, x):
        return self.zb[step][pl.ds(x * self.rows_y, self.rows_y), :]

    def own_v(self, step, slot, x):
        return self.vb[step][pl.ds(self.vb_row(slot, x), self.rows_y), :]

    def along_z(self, value, offset):
        if offset == 0:
            return value
        return jnp.where(self.keep[offset], pltpu.roll(value, (-offset) % self.depth, 1), 0.0)

    def derivative(self, get, forward):
        a, b, c, d = (get(1), get(0), get(2), get(-1)) if forward else (get(0), get(-1), get(1), get(-2))
        return 27.0 * (a - b) - (c - d)

    def s_dx(self, step, comp, x, forward):
        return self.derivative(lambda o: self.sx_tile(step, comp, x + o), forward)

    def s_dy(self, step, comp, x, forward):
        row = self.sy_row(comp, x)
        return self.derivative(lambda o: self.sy[step][pl.ds(row + o, self.rows_y), :], forward)

    def v_dx(self, step, slot, x, forward):
        return self.derivative(lambda o: self.own_v(step, slot, x + o), forward)

    def v_dy(self, step, slot, x, forward):
        row = self.vb_row(slot, x)
        return self.derivative(lambda o: self.vb[step][pl.ds(row + o, self.rows_y), :], forward)

    def dz(self, value, forward):
        return self.derivative(lambda o: self.along_z(value, o), forward)

    def forces(self, step, x):
        xz, yz, zz = self.sx_tile(step, 4, x), self.own_sy(step, 5, x), self.own_zb(step, x)
        return (
            self.s_dx(step, 0, x, True) + self.s_dy(step, 3, x, False) + self.dz(xz, False),
            self.s_dx(step, 3, x, False) + self.s_dy(step, 1, x, True) + self.dz(yz, False),
            self.s_dx(step, 4, x, False) + self.s_dy(step, 5, x, False) + self.dz(zz, True),
        )

    def stress(self, step, x):
        vx, vy, vz = (self.own_v(step, slot, x) for slot in range(3))
        ex = self.v_dx(step, 0, x, False)
        ey = self.v_dy(step, 1, x, False)
        ez = self.dz(vz, False)
        xy = self.v_dy(step, 0, x, True) + self.v_dx(step, 1, x, True)
        xz = self.dz(vx, True) + self.v_dx(step, 2, x, True)
        yz = self.dz(vy, True) + self.v_dy(step, 2, x, True)
        weight = time_step / 24.0
        inj = self.inj
        m = weight * self.mod[x]
        grow = weight * self.lam[x] * (ex + ey + ez)
        m2 = m + m
        s0, s3, s4 = (self.sx_tile(step, comp, x) for comp in (0, 3, 4))
        s1, s5 = self.own_sy(step, 1, x), self.own_sy(step, 5, x)
        s2 = self.own_zb(step, x)
        s0 = s0 + (grow + m2 * ex) + inj[0, x]
        s1 = s1 + (grow + m2 * ey) + inj[1, x]
        s2 = s2 + (grow + m2 * ez) + inj[2, x]
        s3 = s3 + m * xy + inj[3, x]
        s4 = s4 + m * xz + inj[4, x]
        s5 = s5 + m * yz + inj[5, x]
        pressure = (s0 + s1 + s2) * (1.0 / 3.0)
        d0, d1, d2 = s0 - pressure, s1 - pressure, s2 - pressure
        second = 0.5 * (d0 * d0 + d1 * d1 + d2 * d2) + (s3 * s3 + s4 * s4 + s5 * s5)
        strength = jnp.maximum(self.cc[x] - pressure * self.cf[x], 0.0)
        factor = jnp.minimum(1.0, strength * lax.rsqrt(jnp.maximum(second, shear_floor * shear_floor)))
        s0, s1, s2 = pressure + factor * d0, pressure + factor * d1, pressure + factor * d2
        return s0, s1, s2, factor * s3, factor * s4, factor * s5


def rim_of(rows_x):
    return [*range(4), *range(rows_x - 4, rows_x)]


def finish_kernel(sx, sy, zb, vb, lam, mod, inj, cc, cf, edge_out, vout_hbm, sout_hbm, vout, sout, sem):
    at = Fields((None, sx), (None, sy), (None, zb), (None, vb), lam, mod, inj, cc, cf)
    copies = []

    def put(src, dst):
        copy = pltpu.make_async_copy(src, dst, sem.at[len(copies)])
        copy.start()
        copies.append(copy)

    for i, x in ((0, 0), (4, at.rows_x - 4)):
        put(edge_out.at[:, pl.ds(i, 4)], sout_hbm.at[:, pl.ds(x, 4)])
    for start in range(4, at.rows_x - 4, CH):
        stop = min(start + CH, at.rows_x - 4)
        low, high = (0 if start == 4 else start), (at.rows_x if stop == at.rows_x - 4 else stop)
        for x in range(low, high):
            for slot in range(3):
                vout[slot, x] = at.own_v(STEPS - 1, slot, x)
        put(vout.at[:, pl.ds(low, high - low)], vout_hbm.at[:, pl.ds(low, high - low)])
        for x in range(start, stop):
            for comp, value in enumerate(at.stress(STEPS - 1, x)):
                sout[comp, x] = value
        put(sout.at[:, pl.ds(start, stop - start)], sout_hbm.at[:, pl.ds(start, stop - start)])
    for copy in copies:
        copy.wait()


def kernel(
    nx,
    ny,
    vel_hbm, str_hbm, lam_hbm, mod_hbm, buo_hbm, zone_hbm, elig_hbm,
    coh_hbm, fri_hbm, cell_hbm, moment_hbm,
    sx1, sy1, zb1, vb1, lam, mod, inj, cc, cf, edge_out,
    sx0, sy0, zb0, vb0, stage, vel, buo, zone, elig,
    xs, rx, ys, ry, ds, rd, xf, yf, coh_ref, fri_ref, cell_ref, moment_ref,
    load_sem, xsend, xrecv, ysend, yrecv, dsend, drecv, ready,
):
    rows_x = lam.shape[0]
    rows_y = lam.shape[1]
    depth = lam.shape[2]
    chunks = rows_x // CH
    sx, sy, zb, vb = (sx0, sx1), (sy0, sy1), (zb0, zb1), (vb0, vb1)
    at = Fields(sx, sy, zb, vb, lam, mod, inj, cc, cf)
    sx_row, sy_row, vb_row, sx_tile = at.sx_row, at.sy_row, at.vb_row, at.sx_tile
    ix = lax.axis_index("gx")
    iy = lax.axis_index("gy")
    x_lo, x_hi, y_lo, y_hi = ix > 0, ix < nx - 1, iy > 0, iy < ny - 1

    def to_x(up):
        return (x_hi, (ix + 1, iy)) if up else (x_lo, (ix - 1, iy))

    def to_y(up):
        return (y_hi, (ix, iy + 1)) if up else (y_lo, (ix, iy - 1))

    def to_corner(cx, cy):
        there = jnp.logical_and(to_x(cx)[0], to_y(cy)[0])
        return there, (to_x(cx)[1][0], to_y(cy)[1][1])

    sides = [to_x(True), to_x(False), to_y(True), to_y(False)]
    odd = iy % 2 == 1
    even = jnp.logical_not(odd)
    greeted = sides + [(jnp.logical_and(there, odd), target) for there, target in (to_corner(*c) for c in CORNERS)]
    expected = sides + [(jnp.logical_and(to_corner(*c)[0], even), None) for c in CORNERS]
    barrier = pltpu.get_barrier_semaphore()
    for there, target in greeted:

        @pl.when(there)
        def _():
            pl.semaphore_signal(barrier, inc=1, device_id=target, device_id_type=MESH)

    raw_x = {up: raw_list(FORCE_X, up, rows_x) for up in (True, False)}
    raw_y = {up: raw_list(FORCE_Y, up, rows_y) for up in (True, False)}
    flow_x = {up: flow_list(FLOW_X, up, rows_x) for up in (True, False)}
    flow_y = {up: flow_list(FLOW_Y, up, rows_y) for up in (True, False)}
    buo_x = {True: [rows_x - 2, rows_x - 1], False: [0, 1]}
    buo_y = {True: [rows_y - 2, rows_y - 1], False: [0, 1]}
    corner = {c: corner_list(c[0], c[1], rows_x, rows_y) for c in CORNERS}

    loads = []

    def load(src, dst):
        copy = pltpu.make_async_copy(src, dst, load_sem.at[len(loads)])
        copy.start()
        loads.append(copy)

    plane = rows_x * rows_y
    load(str_hbm.at[pl.ds(3 * plane, plane)], sx0.at[pl.ds(sx_row(3, 0), plane)])
    load(str_hbm.at[pl.ds(1 * plane, plane)], stage.at[0])
    load(str_hbm.at[pl.ds(5 * plane, plane)], stage.at[1])
    load(buo_hbm, buo)
    load(str_hbm.at[pl.ds(0 * plane, plane)], sx0.at[pl.ds(sx_row(0, 0), plane)])
    load(str_hbm.at[pl.ds(4 * plane, plane)], sx0.at[pl.ds(sx_row(4, 0), plane)])
    first = len(loads)
    load(str_hbm.at[pl.ds(2 * plane, plane)], zb0)
    load(vel_hbm, vel)
    second = len(loads)
    load(cell_hbm, cell_ref)
    load(moment_hbm, moment_ref)
    sources = len(loads)
    load(coh_hbm, coh_ref)
    load(fri_hbm, fri_ref)
    load(zone_hbm, zone)
    load(elig_hbm, elig)
    third = len(loads)
    load(lam_hbm, lam)
    load(mod_hbm, mod)

    tile = jnp.zeros((rows_y, depth), jnp.float32)

    for step in range(STEPS):
        for comp in SLOT_X:
            for layer in (-2, -1, rows_x, rows_x + 1):
                sx[step][pl.ds(sx_row(comp, layer), rows_y), :] = tile
    for ref in (xf, yf):
        for i in range(ref.shape[0] // rows_y):
            ref[pl.ds(i * rows_y, rows_y), :] = tile

    def clear(i, carry):
        for ref in sy:
            ref[pl.ds(pl.multiple_of(i * R + rows_y, 8), R - rows_y), :] = jnp.zeros((R - rows_y, depth), jnp.float32)
        return carry

    lax.fori_loop(0, sy0.shape[0] // R, clear, 0, unroll=4)

    for up in (True, False):

        @pl.when(jnp.logical_not(to_x(not up)[0]))
        def _():
            for step in range(STEPS):
                for i in range(rx.shape[2]):
                    rx[step, int(up), i] = tile

        @pl.when(jnp.logical_not(to_y(not up)[0]))
        def _():
            for step in range(STEPS):

                def wipe(c, carry):
                    for i in range(ry.shape[3] // 8):
                        ry[step, int(up), c, pl.ds(i * 8, 8), :] = tile
                    return carry

                lax.fori_loop(0, chunks, wipe, 0)

    for d, (cx, cy) in enumerate(CORNERS):

        @pl.when(jnp.logical_not(to_corner(not cx, not cy)[0]))
        def _():
            for step in range(STEPS):
                for i in range(rd.shape[2] // 8):
                    rd[step, d, pl.ds(i * 8, 8), :] = tile

    def x_copy(step, up):
        count = len(raw_x[up]) + len(flow_x[up]) + (2 if step == 0 else 0)
        return pltpu.make_async_remote_copy(
            src_ref=xs.at[step, int(up), pl.ds(0, count)],
            dst_ref=rx.at[step, int(up), pl.ds(0, count)],
            send_sem=xsend.at[step, int(up)],
            recv_sem=xrecv.at[step, int(up)],
            device_id=to_x(up)[1],
            device_id_type=MESH,
        )

    def y_parts(step):
        return (0,) if step == 0 else (0, 1)

    def y_copy(step, up, c, part):
        raw, flow = len(raw_y[up]), len(flow_y[up])
        start, count = (0, raw + flow + 2) if step == 0 else ((0, raw), (raw, flow))[part]
        return pltpu.make_async_remote_copy(
            src_ref=ys.at[step, int(up), c, pl.ds(start * 8, count * 8)],
            dst_ref=ry.at[step, int(up), c, pl.ds(start * 8, count * 8)],
            send_sem=ysend.at[step, int(up), c, part],
            recv_sem=yrecv.at[step, int(up), c, part],
            device_id=to_y(up)[1],
            device_id_type=MESH,
        )

    def d_copy(step, d):
        return pltpu.make_async_remote_copy(
            src_ref=ds.at[step, d, pl.ds(0, len(corner[CORNERS[d]]))],
            dst_ref=rd.at[step, d, pl.ds(0, len(corner[CORNERS[d]]))],
            send_sem=dsend.at[step, d],
            recv_sem=drecv.at[step, d],
            device_id=to_corner(*CORNERS[d])[1],
            device_id_type=MESH,
        )

    def sy_pack(step, comp, c, row):
        return sy[step][pl.ds(sy_row(comp, c * CH) + row, CH, stride=R), :]

    def vb_pack(slot, c, row):
        return pl.ds(vb_row(slot, c * CH) + row, CH, stride=R)

    def pack_x_raw(step, up):
        for i, (comp, x) in enumerate(raw_x[up]):
            xs[step, int(up), i] = sx_tile(step, comp, x)
        if step == 0:
            for i, x in enumerate(buo_x[up]):
                xs[step, int(up), len(raw_x[up]) + len(flow_x[up]) + i] = buo[pl.ds(x * rows_y, rows_y), :]

    def pack_y_raw(step, c):
        for up in (True, False):
            for i, (comp, row) in enumerate(raw_y[up]):
                ys[step, int(up), c, pl.ds(i * 8, 8), :] = sy_pack(step, comp, c, row)
            if step == 0:
                for i, row in enumerate(buo_y[up]):
                    value = buo[pl.ds(c * CH * rows_y + row, CH, stride=rows_y), :]
                    ys[step, int(up), c, pl.ds((len(raw_y[up]) + len(flow_y[up]) + i) * 8, 8), :] = value

    def pack_x_flow(step, up):
        for i, (slot, x) in enumerate(flow_x[up]):
            xs[step, int(up), len(raw_x[up]) + i] = vb[step][pl.ds(vb_row(slot, x), rows_y), :]

    def pack_y_flow(step, c):
        for up in (True, False):
            for i, (slot, row) in enumerate(flow_y[up]):
                ys[step, int(up), c, pl.ds((len(raw_y[up]) + i) * 8, 8), :] = vb[step][vb_pack(slot, c, row), :]

    def pack_corners(step, cxs):
        for d, (cx, cy) in enumerate(CORNERS):
            if cx in cxs:
                for i, (comp, x, y) in enumerate(corner[(cx, cy)]):
                    if comp in SLOT_X:
                        value = sx[step][pl.ds(sx_row(comp, x) + y, 1), :]
                    else:
                        value = sy[step][pl.ds(sy_row(comp, x) + y, 1), :]
                    ds[step, d, pl.ds(i, 1), :] = value

    def send_x(step, cores, ways):
        mine = iy % 2 == cores[0]
        for up in ways:

            @pl.when(to_x(up)[0] if len(cores) == 2 else jnp.logical_and(to_x(up)[0], mine))
            def _():
                x_copy(step, up).start()

    def send_y(step, cs, parts):
        for up in (True, False):

            @pl.when(to_y(up)[0])
            def _():
                for c in cs:
                    for part in parts:
                        y_copy(step, up, c, part).start()

    def send_corners(step, cxs, when=None):
        for d, (cx, cy) in enumerate(CORNERS):
            if cx in cxs:

                there = to_corner(cx, cy)[0]

                @pl.when(there if when is None else jnp.logical_and(there, when))
                def _():
                    d_copy(step, d).start()

    weight = time_step / 24.0

    def flow_layer(step, x):
        scale = weight * of_cell(buo, x)
        for slot, force in enumerate(at.forces(step, x)):
            old = vel[pl.ds((slot * rows_x + x) * rows_y, rows_y), :] if step == 0 else at.own_v(step - 1, slot, x)
            vb[step][pl.ds(vb_row(slot, x), rows_y), :] = old + scale * force

    def stress_layer(step, x):
        s = at.stress(step, x)
        for comp in SLOT_X:
            sx[step + 1][pl.ds(sx_row(comp, x), rows_y), :] = s[comp]
        for comp in SLOT_Y:
            sy[step + 1][pl.ds(sy_row(comp, x), rows_y), :] = s[comp]
        zb[step + 1][pl.ds(x * rows_y, rows_y), :] = s[2]

    def of_cell(ref, x):
        return ref[pl.ds(x * rows_y, rows_y), :]

    def wait_x(step):
        for up in (True, False):

            @pl.when(to_x(not up)[0])
            def _():
                x_copy(step, up).wait_recv()

    def wait_y(step, cs):
        for up in (True, False):

            @pl.when(to_y(not up)[0])
            def _():
                for c in cs:
                    for part in y_parts(step):
                        y_copy(step, up, c, part).wait_recv()

    def wait_corners(step):
        for d, (cx, cy) in enumerate(CORNERS):

            @pl.when(to_corner(not cx, not cy)[0])
            def _():
                d_copy(step, d).wait_recv()

    def place(items, what):
        return [i for i, item in enumerate(items) if item == what][0]

    def take_corners(step):
        for d, (cx, cy) in enumerate(CORNERS):

            def raw(comp, x, y):
                return rd[step, d, pl.ds(place(corner[(cx, cy)], (comp, x, y)), 1), :]

            for k in range(3):
                comp, kind = FORCE_Y[k]
                ys_ = edge(kind, cy, rows_y)
                for x in edge(FLOW_X[k], cx, rows_x):
                    base = (int(cx) * 5 + place(flow_x[cx], (k, x))) * rows_y
                    for row, value in spread(kind, cy, rows_y, lambda i: raw(comp, x, ys_[i])):
                        xf[pl.ds(base + row, 1), :] = value
                comp, kind = FORCE_X[k]
                xs_ = edge(kind, cx, rows_x)
                for y in edge(FLOW_Y[k], cy, rows_y):
                    base = ((int(cy) * 5 + place(flow_y[cy], (k, y))) * 2 + int(cx)) * 8
                    for layer, value in spread(kind, cx, CH, lambda i: raw(comp, xs_[i], y)):
                        yf[pl.ds(base + layer, 1), :] = value

    def finish_x(step):
        for up in (True, False):
            side = int(up)
            for k, (comp, kind) in enumerate(FORCE_X):
                places = [place(raw_x[up], (comp, x)) for x in edge(kind, up, rows_x)]
                for x, value in spread(kind, up, rows_x, lambda i: rx[step, side, places[i]]):
                    where = pl.ds(vb_row(k, x), rows_y)
                    vb[step][where, :] = vb[step][where, :] + weight * of_cell(buo, x) * value
            for k, (comp, kind) in enumerate(FORCE_X):
                mine = edge(kind, not up, rows_x)
                adds = dict(spread(kind, not up, rows_x, lambda i: sx_tile(step, comp, mine[i])))
                for x in edge(FLOW_X[k], up, rows_x):
                    i = place(flow_x[up], (k, x))
                    add = adds[x] + xf[pl.ds((side * 5 + i) * rows_y, rows_y), :]
                    scale = weight * rx[0, side, len(raw_x[up]) + len(flow_x[up]) + place(buo_x[up], x)]
                    new = rx[step, side, len(raw_x[up]) + i] + scale * add
                    halo = x - rows_x if up else x + rows_x
                    vb[step][pl.ds(vb_row(k, halo), rows_y), :] = new

    def buo_halo_y(up, c, y):
        i = len(raw_y[up]) + len(flow_y[up]) + place(buo_y[up], y)
        return ry[0, int(up), c, pl.ds(i * 8, 8), :]

    def finish_y(step, c):
        for up in (True, False):
            side = int(up)

            def got(i):
                return ry[step, side, c, pl.ds(i * 8, 8), :]

            for k, (comp, kind) in enumerate(FORCE_Y):
                places = [place(raw_y[up], (comp, y)) for y in edge(kind, up, rows_y)]
                for y, value in spread(kind, up, rows_y, lambda i: got(places[i])):
                    where = vb_pack(k, c, y)
                    scale = weight * buo[pl.ds(c * CH * rows_y + y, CH, stride=rows_y), :]
                    vb[step][where, :] = vb[step][where, :] + scale * value
            for k, (comp, kind) in enumerate(FORCE_Y):
                mine = edge(kind, not up, rows_y)
                adds = dict(spread(kind, not up, rows_y, lambda i: sy_pack(step, comp, c, mine[i])))
                for y in edge(FLOW_Y[k], up, rows_y):
                    i = place(flow_y[up], (k, y))
                    scale = weight * buo_halo_y(up, c, y)
                    new = got(len(raw_y[up]) + i) + scale * adds[y]
                    halo = y - rows_y if up else y + rows_y
                    vb[step][vb_pack(k, c, halo), :] = new

    def finish_corners_y(step):
        for up in (True, False):
            for i, (k, y) in enumerate(flow_y[up]):
                halo = y - rows_y if up else y + rows_y
                for end, c in ((1, 0), (0, chunks - 1)):
                    add = yf[pl.ds(((int(up) * 5 + i) * 2 + end) * 8, 8), :]
                    where = vb_pack(k, c, halo)
                    vb[step][where, :] = vb[step][where, :] + weight * buo_halo_y(up, c, y) * add

    for copy in loads[:first]:
        copy.wait()

    def fill_y(i, carry):
        first_row = pl.multiple_of(i * rows_y, 8)
        for comp, value in (
            (3, sx0[pl.ds(sx_row(3, 0) + first_row, rows_y), :]),
            (1, stage[0, pl.ds(first_row, rows_y), :]),
            (5, stage[1, pl.ds(first_row, rows_y), :]),
        ):
            sy0[pl.ds(pl.multiple_of(sy_row(comp, 0) + i * R, 8), rows_y), :] = value
        return carry

    lax.fori_loop(0, rows_x, fill_y, 0, unroll=8)
    for copy in loads[first:second]:
        copy.wait()
    ends = [0] + ([chunks - 1] if chunks > 1 else [])
    middle = list(range(1, chunks - 1))
    for up in (True, False):
        pack_x_raw(0, up)
    pack_corners(0, (True, False))

    def flow_chunk(c):
        pack_y_raw(0, c)
        for i in range(CH):
            flow_layer(0, c * CH + i)
        pack_y_flow(0, c)

    for c in ends:
        flow_chunk(c)
    for up in (True, False):
        pack_x_flow(0, up)
    pl.semaphore_wait(barrier, sum(there.astype(jnp.int32) for there, _ in expected))
    for i, (there, target) in enumerate(sides):

        @pl.when(jnp.logical_and(there, odd if i < 2 else even))
        def _():
            pl.semaphore_signal(ready, inc=1, device_id=target, device_id_type=MESH)

    send_corners(0, (True, False), even)
    send_x(0, (0,), (False, True))
    send_y(0, ends, (0,))
    for c in middle:
        flow_chunk(c)
        send_y(0, (c,), (0,))

    for copy in loads[second:sources]:
        copy.wait()
    cell = cell_ref[...]
    bits = depth.bit_length() - 1
    assert depth == 1 << bits
    plane_row = cell >> bits
    cell_z = cell & (depth - 1)
    row = lax.broadcasted_iota(jnp.int32, (rows_x * rows_y, cell.shape[1]), 0)
    row_bits = rows_y.bit_length() - 1
    assert rows_y == 1 << row_bits
    row = (ix * rows_x + (row >> row_bits)) * (ny * rows_y) + iy * rows_y + (row & (rows_y - 1))
    match = row == plane_row
    at_z = (lax.broadcasted_iota(jnp.int32, (depth, cell.shape[1]), 0) == cell_z).astype(jnp.float32)
    for comp in range(6):
        if comp == 4:
            send_x(0, (1,), (False, True))

            @pl.when(odd)
            def _():
                pl.semaphore_wait(ready, sum(there.astype(jnp.int32) for there, _ in sides))

            send_corners(0, (True, False), odd)
        moment = time_step * moment_ref[pl.ds(comp, 1), :]
        value = lax.dot_general(
            jnp.where(match, moment, 0.0),
            at_z,
            (((1,), (1,)), ((), ())),
            precision=lax.Precision.HIGHEST,
            preferred_element_type=jnp.float32,
        )
        inj[comp] = value.reshape(rows_x, rows_y, depth)

    for copy in loads[sources:third]:
        copy.wait()
    frictions, cohesions = [], []
    for which in range(coh_ref.shape[0]):
        f = jnp.full((rows_y, depth), fri_ref[which], jnp.float32)
        frictions.append(f)
        cohesions.append(coh_ref[which] * jnp.sqrt(1.0 - f * f))

    def table(x, carry):
        z = jnp.where(elig[x] == 1, zone[x], -1)
        c = jnp.full((rows_y, depth), 1e30, jnp.float32)
        f = jnp.zeros((rows_y, depth), jnp.float32)
        for which in range(coh_ref.shape[0]):
            hit = z == which
            c = jnp.where(hit, cohesions[which], c)
            f = jnp.where(hit, frictions[which], f)
        cc[x] = c
        cf[x] = f
        return carry

    lax.fori_loop(0, rows_x, table, 0, unroll=2)

    for copy in loads[third:]:
        copy.wait()

    def finish_sends(step):
        for up in (True, False):

            @pl.when(to_x(up)[0])
            def _():
                x_copy(step, up).wait_send()

            @pl.when(to_y(up)[0])
            def _():
                for c in range(chunks):
                    for part in y_parts(step):
                        y_copy(step, up, c, part).wait_send()

        for d, (cx, cy) in enumerate(CORNERS):

            @pl.when(to_corner(cx, cy)[0])
            def _():
                d_copy(step, d).wait_send()

    def flow_rest(step, c, done):
        for x in range(c * CH, (c + 1) * CH):
            if x not in done:
                flow_layer(step, x)
        pack_y_flow(step, c)
        send_y(step, (c,), (1,))

    for step in range(STEPS):
        nxt = step + 1
        wait_y(step, ends)
        for c in ends:
            finish_y(step, c)
        wait_corners(step)
        take_corners(step)
        finish_corners_y(step)
        wait_x(step)
        finish_x(step)
        if nxt == STEPS:
            for i, x in enumerate(rim_of(rows_x)):
                for comp, value in enumerate(at.stress(step, x)):
                    edge_out[comp, i] = value
        wait_y(step, middle)
        for c in middle:
            finish_y(step, c)
        if nxt == STEPS:
            break
        stressed = set()

        def stress_layers(layers):
            for x in layers:
                if x not in stressed:
                    stress_layer(step, x)
                    stressed.add(x)

        stress_layers(rim_of(rows_x))
        pack_corners(nxt, (False, True))
        send_corners(nxt, (False, True))
        flowed = (0, 1, rows_x - 2, rows_x - 1)
        for x in flowed:
            flow_layer(nxt, x)
        for up in (False, True):
            pack_x_raw(nxt, up)
            pack_x_flow(nxt, up)
        send_x(nxt, (0,), (False, True))
        for c in ends:
            stress_layers(range(c * CH, (c + 1) * CH))
            pack_y_raw(nxt, c)
            send_y(nxt, (c,), (0,))
        stress_layers((CH, CH + 1, rows_x - CH - 2, rows_x - CH - 1))
        for c in ends:
            flow_rest(nxt, c, flowed)
        send_x(nxt, (1,), (False, True))
        for c in middle:
            stress_layers(range(c * CH, (c + 1) * CH))
            pack_y_raw(nxt, c)
            send_y(nxt, (c,), (0,))
        for c in middle:
            flow_rest(nxt, c, ())
        for done in range(STEPS):
            finish_sends(done)


def on_device(nx, ny, velocity, stress, lame_first, modulus, buoyancy, zone, eligible, cohesion, friction, source_cell, source_moment):
    rows_x, rows_y, depth = zone.shape
    assert rows_y == 8 and rows_x % CH == 0 and rows_x >= 3 * CH
    chunks = rows_x // CH
    f32 = jnp.float32
    grid = (rows_x, rows_y, depth)
    plane = rows_x * rows_y
    any_spec = pl.BlockSpec(memory_space=pltpu.HBM)
    vmem = pl.BlockSpec(memory_space=pltpu.VMEM)
    dma = pltpu.SemaphoreType.DMA
    fields = [
        pltpu.VMEM((3 * (rows_x + 4) * rows_y, depth), f32),
        pltpu.VMEM((3 * R * (rows_x + 1) + R, depth), f32),
        pltpu.VMEM((plane, depth), f32),
        pltpu.VMEM((3 * (rows_x + 5) * R, depth), f32),
        pltpu.VMEM(grid, f32),
        pltpu.VMEM(grid, f32),
        pltpu.VMEM((6,) + grid, f32),
        pltpu.VMEM(grid, f32),
        pltpu.VMEM(grid, f32),
        pltpu.VMEM((6, len(rim_of(rows_x)), rows_y, depth), f32),
    ]
    held = pl.pallas_call(
        functools.partial(kernel, nx, ny),
        out_shape=fields,
        in_specs=[any_spec] * 11,
        out_specs=[vmem] * len(fields),
        scratch_shapes=fields[:4] + [
            pltpu.VMEM((2, plane, depth), f32),
            pltpu.VMEM((3 * plane, depth), f32),
            pltpu.VMEM((plane, depth), f32),
            pltpu.VMEM(grid, jnp.int32),
            pltpu.VMEM(grid, jnp.int32),
            pltpu.VMEM((STEPS, 2, 11, rows_y, depth), f32),
            pltpu.VMEM((STEPS, 2, 11, rows_y, depth), f32),
            pltpu.VMEM((STEPS, 2, chunks, 11 * 8, depth), f32),
            pltpu.VMEM((STEPS, 2, chunks, 11 * 8, depth), f32),
            pltpu.VMEM((STEPS, 4, 16, depth), f32),
            pltpu.VMEM((STEPS, 4, 16, depth), f32),
            pltpu.VMEM((2 * 5 * rows_y, depth), f32),
            pltpu.VMEM((2 * 5 * 2 * 8, depth), f32),
            pltpu.SMEM(cohesion.shape, f32),
            pltpu.SMEM(friction.shape, f32),
            pltpu.VMEM((1,) + source_cell.shape, jnp.int32),
            pltpu.VMEM(source_moment.shape, f32),
            dma((16,)),
            dma((STEPS, 2)),
            dma((STEPS, 2)),
            dma((STEPS, 2, chunks, 2)),
            dma((STEPS, 2, chunks, 2)),
            dma((STEPS, 4)),
            dma((STEPS, 4)),
            pltpu.SemaphoreType.REGULAR,
        ],
        compiler_params=pltpu.CompilerParams(collective_id=0, has_side_effects=True, vmem_limit_bytes=63_000_000),
    )(
        velocity.reshape(3 * plane, depth), stress.reshape(6 * plane, depth), lame_first, modulus,
        buoyancy.reshape(plane, depth), zone, eligible,
        cohesion, friction, source_cell.reshape(1, -1), source_moment,
    )
    return pl.pallas_call(
        finish_kernel,
        out_shape=(jax.ShapeDtypeStruct((3,) + grid, f32), jax.ShapeDtypeStruct((6,) + grid, f32)),
        in_specs=[vmem] * len(fields),
        out_specs=(any_spec, any_spec),
        scratch_shapes=[pltpu.VMEM((3,) + grid, f32), pltpu.VMEM((6,) + grid, f32), dma((2 + 2 * chunks,))],
        compiler_params=pltpu.CompilerParams(vmem_limit_bytes=24 * 2**20),
    )(*held)


def solution(mesh):
    field = P(None, "gx", "gy", None)
    cells = P("gx", "gy", None)
    return jax.shard_map(
        functools.partial(on_device, mesh.shape["gx"], mesh.shape["gy"]),
        mesh=mesh,
        in_specs=(field, field, cells, cells, cells, cells, cells, P(), P(), P(), P()),
        out_specs=(field, field),
        check_vma=False,
    )
```

```python
import functools

import jax
import jax.numpy as jnp
from jax import lax
from jax.experimental import pallas as pl
from jax.experimental.pallas import tpu as pltpu
from jax.sharding import PartitionSpec as P

STEPS = 2
time_step = 0.1
shear_floor = 0.25
MESH = pl.DeviceIdType.MESH
CH = 8
R = 16

BACK = {"F": 1, "B": 2}
AHEAD = {"F": 2, "B": 1}
FORCE_X = ((0, "F"), (3, "B"), (4, "B"))
FORCE_Y = ((3, "B"), (1, "F"), (5, "B"))
FLOW_X = ("B", "F", "F")
FLOW_Y = ("F", "B", "F")
SLOT_X = {0: 0, 3: 1, 4: 2}
SLOT_Y = {3: 0, 1: 1, 5: 2}


def edge(kind, up, n):
    return list(range(n - BACK[kind], n)) if up else list(range(AHEAD[kind]))


def spread(kind, up, n, get):
    if up and kind == "B":
        return [(0, get(0) - 27.0 * get(1)), (1, get(1))]
    if up:
        return [(0, get(0))]
    if kind == "B":
        return [(n - 1, -get(0))]
    return [(n - 1, 27.0 * get(0) - get(1)), (n - 2, -get(0))]


def raw_list(force, up, n):
    return [(comp, i) for comp, kind in force for i in edge(kind, up, n)]


def flow_list(flow, up, n):
    return [(slot, i) for slot, kind in enumerate(flow) for i in edge(kind, up, n)]


def corner_list(sx, sy, nx, ny):
    found = []
    for k in range(3):
        comp, kind = FORCE_Y[k]
        found += [(comp, x, y) for x in edge(FLOW_X[k], sx, nx) for y in edge(kind, sy, ny)]
        comp, kind = FORCE_X[k]
        found += [(comp, x, y) for x in edge(kind, sx, nx) for y in edge(FLOW_Y[k], sy, ny)]
    return list(dict.fromkeys(found))


CORNERS = [(False, True), (False, False), (True, True), (True, False)]


class Fields:
    def __init__(self, sx, sy, zb, vb, lam, mod, inj, cc, cf):
        self.sx, self.sy, self.zb, self.vb = sx, sy, zb, vb
        self.lam, self.mod, self.inj, self.cc, self.cf = lam, mod, inj, cc, cf
        self.rows_x, self.rows_y, self.depth = lam.shape
        lane = lax.broadcasted_iota(jnp.int32, (self.rows_y, self.depth), 1)
        self.keep = {1: lane < self.depth - 1, 2: lane < self.depth - 2, -1: lane >= 1, -2: lane >= 2}

    def sx_row(self, comp, x):
        return (SLOT_X[comp] * (self.rows_x + 4) + x + 2) * self.rows_y

    def sy_row(self, comp, x):
        return SLOT_Y[comp] * R * (self.rows_x + 1) + R * (x + 1)

    def vb_row(self, slot, x):
        return (slot * (self.rows_x + 5) + x + 3) * R

    def sx_tile(self, step, comp, x):
        return self.sx[step][pl.ds(self.sx_row(comp, x), self.rows_y), :]

    def own_sy(self, step, comp, x):
        return self.sy[step][pl.ds(self.sy_row(comp, x), self.rows_y), :]

    def own_zb(self, step, x):
        return self.zb[step][pl.ds(x * self.rows_y, self.rows_y), :]

    def own_v(self, step, slot, x):
        return self.vb[step][pl.ds(self.vb_row(slot, x), self.rows_y), :]

    def along_z(self, value, offset):
        if offset == 0:
            return value
        return jnp.where(self.keep[offset], pltpu.roll(value, (-offset) % self.depth, 1), 0.0)

    def derivative(self, get, forward):
        a, b, c, d = (get(1), get(0), get(2), get(-1)) if forward else (get(0), get(-1), get(1), get(-2))
        return 27.0 * (a - b) - (c - d)

    def s_dx(self, step, comp, x, forward):
        return self.derivative(lambda o: self.sx_tile(step, comp, x + o), forward)

    def s_dy(self, step, comp, x, forward):
        row = self.sy_row(comp, x)
        return self.derivative(lambda o: self.sy[step][pl.ds(row + o, self.rows_y), :], forward)

    def v_dx(self, step, slot, x, forward):
        return self.derivative(lambda o: self.own_v(step, slot, x + o), forward)

    def v_dy(self, step, slot, x, forward):
        row = self.vb_row(slot, x)
        return self.derivative(lambda o: self.vb[step][pl.ds(row + o, self.rows_y), :], forward)

    def dz(self, value, forward):
        return self.derivative(lambda o: self.along_z(value, o), forward)

    def forces(self, step, x):
        xz, yz, zz = self.sx_tile(step, 4, x), self.own_sy(step, 5, x), self.own_zb(step, x)
        return (
            self.s_dx(step, 0, x, True) + self.s_dy(step, 3, x, False) + self.dz(xz, False),
            self.s_dx(step, 3, x, False) + self.s_dy(step, 1, x, True) + self.dz(yz, False),
            self.s_dx(step, 4, x, False) + self.s_dy(step, 5, x, False) + self.dz(zz, True),
        )

    def stress(self, step, x):
        vx, vy, vz = (self.own_v(step, slot, x) for slot in range(3))
        ex = self.v_dx(step, 0, x, False)
        ey = self.v_dy(step, 1, x, False)
        ez = self.dz(vz, False)
        xy = self.v_dy(step, 0, x, True) + self.v_dx(step, 1, x, True)
        xz = self.dz(vx, True) + self.v_dx(step, 2, x, True)
        yz = self.dz(vy, True) + self.v_dy(step, 2, x, True)
        weight = time_step / 24.0
        inj = self.inj
        m = weight * self.mod[x]
        grow = weight * self.lam[x] * (ex + ey + ez)
        m2 = m + m
        s0, s3, s4 = (self.sx_tile(step, comp, x) for comp in (0, 3, 4))
        s1, s5 = self.own_sy(step, 1, x), self.own_sy(step, 5, x)
        s2 = self.own_zb(step, x)
        s0 = s0 + (grow + m2 * ex) + inj[0, x]
        s1 = s1 + (grow + m2 * ey) + inj[1, x]
        s2 = s2 + (grow + m2 * ez) + inj[2, x]
        s3 = s3 + m * xy + inj[3, x]
        s4 = s4 + m * xz + inj[4, x]
        s5 = s5 + m * yz + inj[5, x]
        pressure = (s0 + s1 + s2) * (1.0 / 3.0)
        d0, d1, d2 = s0 - pressure, s1 - pressure, s2 - pressure
        second = 0.5 * (d0 * d0 + d1 * d1 + d2 * d2) + (s3 * s3 + s4 * s4 + s5 * s5)
        strength = jnp.maximum(self.cc[x] - pressure * self.cf[x], 0.0)
        factor = jnp.minimum(1.0, strength * lax.rsqrt(jnp.maximum(second, shear_floor * shear_floor)))
        s0, s1, s2 = pressure + factor * d0, pressure + factor * d1, pressure + factor * d2
        return s0, s1, s2, factor * s3, factor * s4, factor * s5


def rim_of(rows_x):
    return [*range(4), *range(rows_x - 4, rows_x)]


def finish_kernel(sx, sy, zb, vb, lam, mod, inj, cc, cf, edge_out, vout_hbm, sout_hbm, vout, sout, sem):
    at = Fields((None, sx), (None, sy), (None, zb), (None, vb), lam, mod, inj, cc, cf)
    copies = []

    def put(src, dst):
        copy = pltpu.make_async_copy(src, dst, sem.at[len(copies)])
        copy.start()
        copies.append(copy)

    for i, x in ((0, 0), (4, at.rows_x - 4)):
        put(edge_out.at[:, pl.ds(i, 4)], sout_hbm.at[:, pl.ds(x, 4)])
    for start in range(4, at.rows_x - 4, CH):
        stop = min(start + CH, at.rows_x - 4)
        low, high = (0 if start == 4 else start), (at.rows_x if stop == at.rows_x - 4 else stop)
        for x in range(low, high):
            for slot in range(3):
                vout[slot, x] = at.own_v(STEPS - 1, slot, x)
        put(vout.at[:, pl.ds(low, high - low)], vout_hbm.at[:, pl.ds(low, high - low)])
        for x in range(start, stop):
            for comp, value in enumerate(at.stress(STEPS - 1, x)):
                sout[comp, x] = value
        put(sout.at[:, pl.ds(start, stop - start)], sout_hbm.at[:, pl.ds(start, stop - start)])
    for copy in copies:
        copy.wait()


def kernel(
    nx,
    ny,
    vel_hbm, str_hbm, lam_hbm, mod_hbm, buo_hbm, zone_hbm, elig_hbm,
    coh_hbm, fri_hbm, cell_hbm, moment_hbm,
    sx1, sy1, zb1, vb1, lam, mod, inj, cc, cf, edge_out,
    sx0, sy0, zb0, vb0, stage, vel, buo, zone, elig,
    xs, rx, ys, ry, ds, rd, xf, yf, coh_ref, fri_ref, cell_ref, moment_ref,
    load_sem, xsend, xrecv, ysend, yrecv, dsend, drecv,
):
    rows_x = lam.shape[0]
    rows_y = lam.shape[1]
    depth = lam.shape[2]
    chunks = rows_x // CH
    sx, sy, zb, vb = (sx0, sx1), (sy0, sy1), (zb0, zb1), (vb0, vb1)
    at = Fields(sx, sy, zb, vb, lam, mod, inj, cc, cf)
    sx_row, sy_row, vb_row, sx_tile = at.sx_row, at.sy_row, at.vb_row, at.sx_tile
    ix = lax.axis_index("gx")
    iy = lax.axis_index("gy")
    x_lo, x_hi, y_lo, y_hi = ix > 0, ix < nx - 1, iy > 0, iy < ny - 1

    def to_x(up):
        return (x_hi, (ix + 1, iy)) if up else (x_lo, (ix - 1, iy))

    def to_y(up):
        return (y_hi, (ix, iy + 1)) if up else (y_lo, (ix, iy - 1))

    def to_corner(cx, cy):
        there = jnp.logical_and(to_x(cx)[0], to_y(cy)[0])
        return there, (to_x(cx)[1][0], to_y(cy)[1][1])

    sides = [to_x(True), to_x(False), to_y(True), to_y(False)] + [to_corner(*c) for c in CORNERS]
    barrier = pltpu.get_barrier_semaphore()
    for there, target in sides:

        @pl.when(there)
        def _():
            pl.semaphore_signal(barrier, inc=1, device_id=target, device_id_type=MESH)

    raw_x = {up: raw_list(FORCE_X, up, rows_x) for up in (True, False)}
    raw_y = {up: raw_list(FORCE_Y, up, rows_y) for up in (True, False)}
    flow_x = {up: flow_list(FLOW_X, up, rows_x) for up in (True, False)}
    flow_y = {up: flow_list(FLOW_Y, up, rows_y) for up in (True, False)}
    buo_x = {True: [rows_x - 2, rows_x - 1], False: [0, 1]}
    buo_y = {True: [rows_y - 2, rows_y - 1], False: [0, 1]}
    corner = {c: corner_list(c[0], c[1], rows_x, rows_y) for c in CORNERS}

    loads = []

    def load(src, dst):
        copy = pltpu.make_async_copy(src, dst, load_sem.at[len(loads)])
        copy.start()
        loads.append(copy)

    plane = rows_x * rows_y
    load(str_hbm.at[pl.ds(3 * plane, plane)], sx0.at[pl.ds(sx_row(3, 0), plane)])
    load(str_hbm.at[pl.ds(1 * plane, plane)], stage.at[0])
    load(str_hbm.at[pl.ds(5 * plane, plane)], stage.at[1])
    load(buo_hbm, buo)
    load(str_hbm.at[pl.ds(0 * plane, plane)], sx0.at[pl.ds(sx_row(0, 0), plane)])
    load(str_hbm.at[pl.ds(4 * plane, plane)], sx0.at[pl.ds(sx_row(4, 0), plane)])
    first = len(loads)
    load(str_hbm.at[pl.ds(2 * plane, plane)], zb0)
    load(vel_hbm, vel)
    second = len(loads)
    load(cell_hbm, cell_ref)
    load(moment_hbm, moment_ref)
    sources = len(loads)
    load(coh_hbm, coh_ref)
    load(fri_hbm, fri_ref)
    load(zone_hbm, zone)
    load(elig_hbm, elig)
    third = len(loads)
    load(lam_hbm, lam)
    load(mod_hbm, mod)

    tile = jnp.zeros((rows_y, depth), jnp.float32)

    for step in range(STEPS):
        for comp in SLOT_X:
            for layer in (-2, -1, rows_x, rows_x + 1):
                sx[step][pl.ds(sx_row(comp, layer), rows_y), :] = tile
    for ref in (xf, yf):
        for i in range(ref.shape[0] // rows_y):
            ref[pl.ds(i * rows_y, rows_y), :] = tile

    def clear(i, carry):
        for ref in sy:
            ref[pl.ds(pl.multiple_of(i * R + rows_y, 8), R - rows_y), :] = jnp.zeros((R - rows_y, depth), jnp.float32)
        return carry

    lax.fori_loop(0, sy0.shape[0] // R, clear, 0, unroll=4)

    for up in (True, False):

        @pl.when(jnp.logical_not(to_x(not up)[0]))
        def _():
            for step in range(STEPS):
                for i in range(rx.shape[2]):
                    rx[step, int(up), i] = tile

        @pl.when(jnp.logical_not(to_y(not up)[0]))
        def _():
            for step in range(STEPS):

                def wipe(c, carry):
                    for i in range(ry.shape[3] // 8):
                        ry[step, int(up), c, pl.ds(i * 8, 8), :] = tile
                    return carry

                lax.fori_loop(0, chunks, wipe, 0)

    for d, (cx, cy) in enumerate(CORNERS):

        @pl.when(jnp.logical_not(to_corner(not cx, not cy)[0]))
        def _():
            for step in range(STEPS):
                for i in range(rd.shape[2] // 8):
                    rd[step, d, pl.ds(i * 8, 8), :] = tile

    def x_copy(step, up):
        count = len(raw_x[up]) + len(flow_x[up]) + (2 if step == 0 else 0)
        return pltpu.make_async_remote_copy(
            src_ref=xs.at[step, int(up), pl.ds(0, count)],
            dst_ref=rx.at[step, int(up), pl.ds(0, count)],
            send_sem=xsend.at[step, int(up)],
            recv_sem=xrecv.at[step, int(up)],
            device_id=to_x(up)[1],
            device_id_type=MESH,
        )

    def y_parts(step):
        return (0,) if step == 0 else (0, 1)

    def y_copy(step, up, c, part):
        raw, flow = len(raw_y[up]), len(flow_y[up])
        start, count = (0, raw + flow + 2) if step == 0 else ((0, raw), (raw, flow))[part]
        return pltpu.make_async_remote_copy(
            src_ref=ys.at[step, int(up), c, pl.ds(start * 8, count * 8)],
            dst_ref=ry.at[step, int(up), c, pl.ds(start * 8, count * 8)],
            send_sem=ysend.at[step, int(up), c, part],
            recv_sem=yrecv.at[step, int(up), c, part],
            device_id=to_y(up)[1],
            device_id_type=MESH,
        )

    def d_copy(step, d):
        return pltpu.make_async_remote_copy(
            src_ref=ds.at[step, d, pl.ds(0, len(corner[CORNERS[d]]))],
            dst_ref=rd.at[step, d, pl.ds(0, len(corner[CORNERS[d]]))],
            send_sem=dsend.at[step, d],
            recv_sem=drecv.at[step, d],
            device_id=to_corner(*CORNERS[d])[1],
            device_id_type=MESH,
        )

    def sy_pack(step, comp, c, row):
        return sy[step][pl.ds(sy_row(comp, c * CH) + row, CH, stride=R), :]

    def vb_pack(slot, c, row):
        return pl.ds(vb_row(slot, c * CH) + row, CH, stride=R)

    def pack_x_raw(step, up):
        for i, (comp, x) in enumerate(raw_x[up]):
            xs[step, int(up), i] = sx_tile(step, comp, x)
        if step == 0:
            for i, x in enumerate(buo_x[up]):
                xs[step, int(up), len(raw_x[up]) + len(flow_x[up]) + i] = buo[pl.ds(x * rows_y, rows_y), :]

    def pack_y_raw(step, c):
        for up in (True, False):
            for i, (comp, row) in enumerate(raw_y[up]):
                ys[step, int(up), c, pl.ds(i * 8, 8), :] = sy_pack(step, comp, c, row)
            if step == 0:
                for i, row in enumerate(buo_y[up]):
                    value = buo[pl.ds(c * CH * rows_y + row, CH, stride=rows_y), :]
                    ys[step, int(up), c, pl.ds((len(raw_y[up]) + len(flow_y[up]) + i) * 8, 8), :] = value

    def pack_x_flow(step, up):
        for i, (slot, x) in enumerate(flow_x[up]):
            xs[step, int(up), len(raw_x[up]) + i] = vb[step][pl.ds(vb_row(slot, x), rows_y), :]

    def pack_y_flow(step, c):
        for up in (True, False):
            for i, (slot, row) in enumerate(flow_y[up]):
                ys[step, int(up), c, pl.ds((len(raw_y[up]) + i) * 8, 8), :] = vb[step][vb_pack(slot, c, row), :]

    def pack_corners(step, cxs):
        for d, (cx, cy) in enumerate(CORNERS):
            if cx in cxs:
                for i, (comp, x, y) in enumerate(corner[(cx, cy)]):
                    if comp in SLOT_X:
                        value = sx[step][pl.ds(sx_row(comp, x) + y, 1), :]
                    else:
                        value = sy[step][pl.ds(sy_row(comp, x) + y, 1), :]
                    ds[step, d, pl.ds(i, 1), :] = value

    def send_x(step, cores, ways):
        mine = iy % 2 == cores[0]
        for up in ways:

            @pl.when(to_x(up)[0] if len(cores) == 2 else jnp.logical_and(to_x(up)[0], mine))
            def _():
                x_copy(step, up).start()

    def send_y(step, cs, parts):
        for up in (True, False):

            @pl.when(to_y(up)[0])
            def _():
                for c in cs:
                    for part in parts:
                        y_copy(step, up, c, part).start()

    def send_corners(step, cxs):
        for d, (cx, cy) in enumerate(CORNERS):
            if cx in cxs:

                @pl.when(to_corner(cx, cy)[0])
                def _():
                    d_copy(step, d).start()

    weight = time_step / 24.0

    def flow_layer(step, x):
        scale = weight * of_cell(buo, x)
        for slot, force in enumerate(at.forces(step, x)):
            old = vel[pl.ds((slot * rows_x + x) * rows_y, rows_y), :] if step == 0 else at.own_v(step - 1, slot, x)
            vb[step][pl.ds(vb_row(slot, x), rows_y), :] = old + scale * force

    def stress_layer(step, x):
        s = at.stress(step, x)
        for comp in SLOT_X:
            sx[step + 1][pl.ds(sx_row(comp, x), rows_y), :] = s[comp]
        for comp in SLOT_Y:
            sy[step + 1][pl.ds(sy_row(comp, x), rows_y), :] = s[comp]
        zb[step + 1][pl.ds(x * rows_y, rows_y), :] = s[2]

    def of_cell(ref, x):
        return ref[pl.ds(x * rows_y, rows_y), :]

    def wait_x(step):
        for up in (True, False):

            @pl.when(to_x(not up)[0])
            def _():
                x_copy(step, up).wait_recv()

    def wait_y(step, cs):
        for up in (True, False):

            @pl.when(to_y(not up)[0])
            def _():
                for c in cs:
                    for part in y_parts(step):
                        y_copy(step, up, c, part).wait_recv()

    def wait_corners(step):
        for d, (cx, cy) in enumerate(CORNERS):

            @pl.when(to_corner(not cx, not cy)[0])
            def _():
                d_copy(step, d).wait_recv()

    def place(items, what):
        return [i for i, item in enumerate(items) if item == what][0]

    def take_corners(step):
        for d, (cx, cy) in enumerate(CORNERS):

            def raw(comp, x, y):
                return rd[step, d, pl.ds(place(corner[(cx, cy)], (comp, x, y)), 1), :]

            for k in range(3):
                comp, kind = FORCE_Y[k]
                ys_ = edge(kind, cy, rows_y)
                for x in edge(FLOW_X[k], cx, rows_x):
                    base = (int(cx) * 5 + place(flow_x[cx], (k, x))) * rows_y
                    for row, value in spread(kind, cy, rows_y, lambda i: raw(comp, x, ys_[i])):
                        xf[pl.ds(base + row, 1), :] = value
                comp, kind = FORCE_X[k]
                xs_ = edge(kind, cx, rows_x)
                for y in edge(FLOW_Y[k], cy, rows_y):
                    base = ((int(cy) * 5 + place(flow_y[cy], (k, y))) * 2 + int(cx)) * 8
                    for layer, value in spread(kind, cx, CH, lambda i: raw(comp, xs_[i], y)):
                        yf[pl.ds(base + layer, 1), :] = value

    def finish_x(step):
        for up in (True, False):
            side = int(up)
            for k, (comp, kind) in enumerate(FORCE_X):
                places = [place(raw_x[up], (comp, x)) for x in edge(kind, up, rows_x)]
                for x, value in spread(kind, up, rows_x, lambda i: rx[step, side, places[i]]):
                    where = pl.ds(vb_row(k, x), rows_y)
                    vb[step][where, :] = vb[step][where, :] + weight * of_cell(buo, x) * value
            for k, (comp, kind) in enumerate(FORCE_X):
                mine = edge(kind, not up, rows_x)
                adds = dict(spread(kind, not up, rows_x, lambda i: sx_tile(step, comp, mine[i])))
                for x in edge(FLOW_X[k], up, rows_x):
                    i = place(flow_x[up], (k, x))
                    add = adds[x] + xf[pl.ds((side * 5 + i) * rows_y, rows_y), :]
                    scale = weight * rx[0, side, len(raw_x[up]) + len(flow_x[up]) + place(buo_x[up], x)]
                    new = rx[step, side, len(raw_x[up]) + i] + scale * add
                    halo = x - rows_x if up else x + rows_x
                    vb[step][pl.ds(vb_row(k, halo), rows_y), :] = new

    def buo_halo_y(up, c, y):
        i = len(raw_y[up]) + len(flow_y[up]) + place(buo_y[up], y)
        return ry[0, int(up), c, pl.ds(i * 8, 8), :]

    def finish_y(step, c):
        for up in (True, False):
            side = int(up)

            def got(i):
                return ry[step, side, c, pl.ds(i * 8, 8), :]

            for k, (comp, kind) in enumerate(FORCE_Y):
                places = [place(raw_y[up], (comp, y)) for y in edge(kind, up, rows_y)]
                for y, value in spread(kind, up, rows_y, lambda i: got(places[i])):
                    where = vb_pack(k, c, y)
                    scale = weight * buo[pl.ds(c * CH * rows_y + y, CH, stride=rows_y), :]
                    vb[step][where, :] = vb[step][where, :] + scale * value
            for k, (comp, kind) in enumerate(FORCE_Y):
                mine = edge(kind, not up, rows_y)
                adds = dict(spread(kind, not up, rows_y, lambda i: sy_pack(step, comp, c, mine[i])))
                for y in edge(FLOW_Y[k], up, rows_y):
                    i = place(flow_y[up], (k, y))
                    scale = weight * buo_halo_y(up, c, y)
                    new = got(len(raw_y[up]) + i) + scale * adds[y]
                    halo = y - rows_y if up else y + rows_y
                    vb[step][vb_pack(k, c, halo), :] = new

    def finish_corners_y(step):
        for up in (True, False):
            for i, (k, y) in enumerate(flow_y[up]):
                halo = y - rows_y if up else y + rows_y
                for end, c in ((1, 0), (0, chunks - 1)):
                    add = yf[pl.ds(((int(up) * 5 + i) * 2 + end) * 8, 8), :]
                    where = vb_pack(k, c, halo)
                    vb[step][where, :] = vb[step][where, :] + weight * buo_halo_y(up, c, y) * add

    for copy in loads[:first]:
        copy.wait()

    def fill_y(i, carry):
        first_row = pl.multiple_of(i * rows_y, 8)
        for comp, value in (
            (3, sx0[pl.ds(sx_row(3, 0) + first_row, rows_y), :]),
            (1, stage[0, pl.ds(first_row, rows_y), :]),
            (5, stage[1, pl.ds(first_row, rows_y), :]),
        ):
            sy0[pl.ds(pl.multiple_of(sy_row(comp, 0) + i * R, 8), rows_y), :] = value
        return carry

    lax.fori_loop(0, rows_x, fill_y, 0, unroll=8)
    for copy in loads[first:second]:
        copy.wait()
    ends = [0] + ([chunks - 1] if chunks > 1 else [])
    middle = list(range(1, chunks - 1))
    for up in (True, False):
        pack_x_raw(0, up)
    pack_corners(0, (True, False))

    def flow_chunk(c):
        pack_y_raw(0, c)
        for i in range(CH):
            flow_layer(0, c * CH + i)
        pack_y_flow(0, c)

    for c in ends:
        flow_chunk(c)
    for up in (True, False):
        pack_x_flow(0, up)
    heard = sum(there.astype(jnp.int32) for there, _ in sides)
    pl.semaphore_wait(barrier, heard)
    send_corners(0, (True, False))
    send_x(0, (0,), (False, True))
    send_y(0, ends, (0,))
    for c in middle:
        flow_chunk(c)
        send_y(0, (c,), (0,))

    for copy in loads[second:sources]:
        copy.wait()
    cell = cell_ref[...]
    bits = depth.bit_length() - 1
    assert depth == 1 << bits
    plane_row = cell >> bits
    cell_z = cell & (depth - 1)
    row = lax.broadcasted_iota(jnp.int32, (rows_x * rows_y, cell.shape[1]), 0)
    row_bits = rows_y.bit_length() - 1
    assert rows_y == 1 << row_bits
    row = (ix * rows_x + (row >> row_bits)) * (ny * rows_y) + iy * rows_y + (row & (rows_y - 1))
    match = row == plane_row
    at_z = (lax.broadcasted_iota(jnp.int32, (depth, cell.shape[1]), 0) == cell_z).astype(jnp.float32)
    for comp in range(6):
        moment = time_step * moment_ref[pl.ds(comp, 1), :]
        value = lax.dot_general(
            jnp.where(match, moment, 0.0),
            at_z,
            (((1,), (1,)), ((), ())),
            precision=lax.Precision.HIGHEST,
            preferred_element_type=jnp.float32,
        )
        inj[comp] = value.reshape(rows_x, rows_y, depth)

    send_x(0, (1,), (False, True))
    for copy in loads[sources:third]:
        copy.wait()
    frictions, cohesions = [], []
    for which in range(coh_ref.shape[0]):
        f = jnp.full((rows_y, depth), fri_ref[which], jnp.float32)
        frictions.append(f)
        cohesions.append(coh_ref[which] * jnp.sqrt(1.0 - f * f))

    def table(x, carry):
        z = jnp.where(elig[x] == 1, zone[x], -1)
        c = jnp.full((rows_y, depth), 1e30, jnp.float32)
        f = jnp.zeros((rows_y, depth), jnp.float32)
        for which in range(coh_ref.shape[0]):
            hit = z == which
            c = jnp.where(hit, cohesions[which], c)
            f = jnp.where(hit, frictions[which], f)
        cc[x] = c
        cf[x] = f
        return carry

    lax.fori_loop(0, rows_x, table, 0, unroll=2)

    for copy in loads[third:]:
        copy.wait()

    def finish_sends(step):
        for up in (True, False):

            @pl.when(to_x(up)[0])
            def _():
                x_copy(step, up).wait_send()

            @pl.when(to_y(up)[0])
            def _():
                for c in range(chunks):
                    for part in y_parts(step):
                        y_copy(step, up, c, part).wait_send()

        for d, (cx, cy) in enumerate(CORNERS):

            @pl.when(to_corner(cx, cy)[0])
            def _():
                d_copy(step, d).wait_send()

    def flow_rest(step, c, done):
        for x in range(c * CH, (c + 1) * CH):
            if x not in done:
                flow_layer(step, x)
        pack_y_flow(step, c)
        send_y(step, (c,), (1,))

    for step in range(STEPS):
        nxt = step + 1
        wait_y(step, ends)
        for c in ends:
            finish_y(step, c)
        wait_corners(step)
        take_corners(step)
        finish_corners_y(step)
        wait_x(step)
        finish_x(step)
        if nxt == STEPS:
            for i, x in enumerate(rim_of(rows_x)):
                for comp, value in enumerate(at.stress(step, x)):
                    edge_out[comp, i] = value
        wait_y(step, middle)
        for c in middle:
            finish_y(step, c)
        if nxt == STEPS:
            break
        stressed = set()

        def stress_layers(layers):
            for x in layers:
                if x not in stressed:
                    stress_layer(step, x)
                    stressed.add(x)

        stress_layers(rim_of(rows_x))
        pack_corners(nxt, (False, True))
        send_corners(nxt, (False, True))
        flowed = (0, 1, rows_x - 2, rows_x - 1)
        for x in flowed:
            flow_layer(nxt, x)
        for up in (False, True):
            pack_x_raw(nxt, up)
            pack_x_flow(nxt, up)
        send_x(nxt, (0,), (False, True))
        for c in ends:
            stress_layers(range(c * CH, (c + 1) * CH))
            pack_y_raw(nxt, c)
            send_y(nxt, (c,), (0,))
        stress_layers((CH, CH + 1, rows_x - CH - 2, rows_x - CH - 1))
        for c in ends:
            flow_rest(nxt, c, flowed)
        send_x(nxt, (1,), (False, True))
        for c in middle:
            stress_layers(range(c * CH, (c + 1) * CH))
            pack_y_raw(nxt, c)
            send_y(nxt, (c,), (0,))
        for c in middle:
            flow_rest(nxt, c, ())
        for done in range(STEPS):
            finish_sends(done)


def on_device(nx, ny, velocity, stress, lame_first, modulus, buoyancy, zone, eligible, cohesion, friction, source_cell, source_moment):
    rows_x, rows_y, depth = zone.shape
    assert rows_y == 8 and rows_x % CH == 0 and rows_x >= 3 * CH
    chunks = rows_x // CH
    f32 = jnp.float32
    grid = (rows_x, rows_y, depth)
    plane = rows_x * rows_y
    any_spec = pl.BlockSpec(memory_space=pltpu.HBM)
    vmem = pl.BlockSpec(memory_space=pltpu.VMEM)
    dma = pltpu.SemaphoreType.DMA
    fields = [
        pltpu.VMEM((3 * (rows_x + 4) * rows_y, depth), f32),
        pltpu.VMEM((3 * R * (rows_x + 1) + R, depth), f32),
        pltpu.VMEM((plane, depth), f32),
        pltpu.VMEM((3 * (rows_x + 5) * R, depth), f32),
        pltpu.VMEM(grid, f32),
        pltpu.VMEM(grid, f32),
        pltpu.VMEM((6,) + grid, f32),
        pltpu.VMEM(grid, f32),
        pltpu.VMEM(grid, f32),
        pltpu.VMEM((6, len(rim_of(rows_x)), rows_y, depth), f32),
    ]
    held = pl.pallas_call(
        functools.partial(kernel, nx, ny),
        out_shape=fields,
        in_specs=[any_spec] * 11,
        out_specs=[vmem] * len(fields),
        scratch_shapes=fields[:4] + [
            pltpu.VMEM((2, plane, depth), f32),
            pltpu.VMEM((3 * plane, depth), f32),
            pltpu.VMEM((plane, depth), f32),
            pltpu.VMEM(grid, jnp.int32),
            pltpu.VMEM(grid, jnp.int32),
            pltpu.VMEM((STEPS, 2, 11, rows_y, depth), f32),
            pltpu.VMEM((STEPS, 2, 11, rows_y, depth), f32),
            pltpu.VMEM((STEPS, 2, chunks, 11 * 8, depth), f32),
            pltpu.VMEM((STEPS, 2, chunks, 11 * 8, depth), f32),
            pltpu.VMEM((STEPS, 4, 16, depth), f32),
            pltpu.VMEM((STEPS, 4, 16, depth), f32),
            pltpu.VMEM((2 * 5 * rows_y, depth), f32),
            pltpu.VMEM((2 * 5 * 2 * 8, depth), f32),
            pltpu.SMEM(cohesion.shape, f32),
            pltpu.SMEM(friction.shape, f32),
            pltpu.VMEM((1,) + source_cell.shape, jnp.int32),
            pltpu.VMEM(source_moment.shape, f32),
            dma((16,)),
            dma((STEPS, 2)),
            dma((STEPS, 2)),
            dma((STEPS, 2, chunks, 2)),
            dma((STEPS, 2, chunks, 2)),
            dma((STEPS, 4)),
            dma((STEPS, 4)),
        ],
        compiler_params=pltpu.CompilerParams(collective_id=0, has_side_effects=True, vmem_limit_bytes=63_000_000),
    )(
        velocity.reshape(3 * plane, depth), stress.reshape(6 * plane, depth), lame_first, modulus,
        buoyancy.reshape(plane, depth), zone, eligible,
        cohesion, friction, source_cell.reshape(1, -1), source_moment,
    )
    return pl.pallas_call(
        finish_kernel,
        out_shape=(jax.ShapeDtypeStruct((3,) + grid, f32), jax.ShapeDtypeStruct((6,) + grid, f32)),
        in_specs=[vmem] * len(fields),
        out_specs=(any_spec, any_spec),
        scratch_shapes=[pltpu.VMEM((3,) + grid, f32), pltpu.VMEM((6,) + grid, f32), dma((2 + 2 * chunks,))],
        compiler_params=pltpu.CompilerParams(vmem_limit_bytes=24 * 2**20),
    )(*held)


def solution(mesh):
    field = P(None, "gx", "gy", None)
    cells = P("gx", "gy", None)
    return jax.shard_map(
        functools.partial(on_device, mesh.shape["gx"], mesh.shape["gy"]),
        mesh=mesh,
        in_specs=(field, field, cells, cells, cells, cells, cells, P(), P(), P(), P()),
        out_specs=(field, field),
        check_vma=False,
    )
```
